32 devices in a mesh: band: 4 (over z), px: 4 (over x, core), py: 2 (over y).
Axes of the slice: x: 2, y: 2, z: 4, core: 2. Of those that a mesh axis runs over, the one named last changes fastest.
Arguments:
- orbitals: bfloat16 [4, 1024, 384], P('band', ('px', 'py')), may hold values from -0.01171875 to 0.01171875
- occupations: float32 [4], P('band'), may hold values from 0.2 to 2
- stick_map: int32 [2, 1024], P(None, 'px'), may hold values from 0 to 191, as said below
- core_density: float32 [192, 192, 192], P('py', 'px'), may hold values from 0.05 to 0.5
Outputs:
- potential: float32 [192, 192, 192], P('py', 'px')
- gradient: float32 [3, 192, 192, 192], P(None, 'py', 'px')
The draws below stay inside these ranges and needn't reach their ends.
Inputs may be any that keep to these rules, and one draw needn't show every extreme that they name: `stick_map`: columns i * 128 * 2 to (i + 1) * 128 * 2 - 1 have x index from i * 48 to (i + 1) * 48 - 1; no two columns share a grid position.
All inputs are finite; a program needn't handle non-finite values.
Results may differ from the reference program's by a relative error of at most 0.0054.
Values may be sent and summed in bfloat16 or wider, within the bound.
A program may use at most 128 MiB of HBM per device.

```python
import math
import jax
import jax.numpy as jnp
from jax import lax

NG = 192
STK_DEV = 128
BANDS = 4
STICKS = 1024
N_PX = 4
N_PY = 2


def draw_stick_map(key, part):
    per_block = STK_DEV * N_PY
    xblock = NG // N_PX
    block_keys = jax.random.split(key, N_PX)

    def pick_block(one_key):
        return jax.random.permutation(one_key, xblock * NG)[:per_block]
    chosen = jax.vmap(pick_block)(block_keys)
    offsets = jnp.arange(N_PX, dtype=jnp.int32)[:, None] * xblock
    x_pos = offsets + chosen // NG
    y_pos = chosen % NG
    return jnp.stack([x_pos.reshape(-1), y_pos.reshape(-1)]).astype(jnp.int32)


def level_of(stream_key, shape, pieces, least, largest):
    def one(position, parts):
        heights = jax.random.uniform(jax.random.fold_in(jax.random.fold_in(stream_key, 6), position), (parts,), jnp.float32, least / len(pieces), largest / len(pieces))
        return jnp.repeat(jnp.exp(heights), shape[position] // parts).reshape((-1,) + (1,) * (len(shape) - position - 1))

    loudness = one(*pieces[0])
    for cut in pieces[1:]:
        loudness = loudness * one(*cut)
    return loudness


def scatter_about(own_key, dims, spread, limit, cuts=(), kind=jnp.bfloat16):
    entries = spread * jax.random.normal(own_key, dims, jnp.float32)
    if cuts:
        entries = entries * level_of(own_key, dims, cuts, -0.22, 0.18)
    return jnp.clip(entries, -limit, limit).astype(kind)


def setup_inputs(seed: int = 0) -> dict:
    seeds = jax.random.split(jax.random.key(seed), 5)
    orbitals = scatter_about(seeds[0], (BANDS, STICKS, 2 * NG), ((2 * STICKS * NG * BANDS) ** -0.5), 0.01171875, ((0, 4), (1, 8)))
    occupations = jnp.clip(0.2 + 1.8 * jax.random.uniform(seeds[1], (BANDS,), jnp.float32) ** level_of(seeds[1], (BANDS,), ((0, 4),), -0.2, 0.2), 0.2, 2.0)
    stick_map = draw_stick_map(jax.random.fold_in(seeds[4], 71), 0)
    core_density = jnp.clip(jnp.exp(math.log(0.5) - 2.3025851 * jax.random.uniform(seeds[3], (NG, NG, NG), jnp.float32) ** level_of(seeds[3], (NG, NG, NG), ((0, 2), (1, 4)), -0.2, 0.2)), 0.05, 0.5)
    return dict(orbitals=orbitals, occupations=occupations, stick_map=stick_map, core_density=core_density)


SPACING = 0.25
PBE_KAPPA = 0.804
PBE_MU = 0.2195
SLATER_COEF = 0.75 * (3.0 / math.pi) ** (1.0 / 3.0)
REDUCED_SCALE = 4.0 * (3.0 * math.pi ** 2) ** (2.0 / 3.0)


def rounded(values):
    return lax.optimization_barrier(values.astype(jnp.bfloat16)).astype(jnp.float32)


def exchange_part(density, hartree, grad_x, grad_y, grad_z):
    cube_root = jnp.cbrt(density)
    four_thirds = density * cube_root
    grad_square = grad_x * grad_x + grad_y * grad_y + grad_z * grad_z
    reduced = grad_square / (REDUCED_SCALE * four_thirds * four_thirds)
    denominator = 1.0 + PBE_MU * reduced / PBE_KAPPA
    enhance = 1.0 + PBE_KAPPA - PBE_KAPPA / denominator
    enhance_slope = PBE_MU / (denominator * denominator)
    return hartree - SLATER_COEF * cube_root * ((4.0 / 3.0) * enhance - (8.0 / 3.0) * reduced * enhance_slope)


def reference(orbitals, occupations, stick_map, core_density):
    points = orbitals.shape[2] // 2
    x_cols = stick_map[0]
    y_cols = stick_map[1]

    def add_band(summed, inputs):
        coeffs, weight = inputs
        real_in = coeffs[:, :points].astype(jnp.float32)
        imag_in = coeffs[:, points:].astype(jnp.float32)
        along_z = jnp.fft.ifft(real_in + 1j * imag_in, axis=1) * points
        plane_real = jnp.zeros((points, points, points), jnp.float32).at[:, y_cols, x_cols].set(rounded(along_z.real).T)
        plane_imag = jnp.zeros((points, points, points), jnp.float32).at[:, y_cols, x_cols].set(rounded(along_z.imag).T)
        along_y = jnp.fft.ifft(plane_real + 1j * plane_imag, axis=1) * points
        along_x = jnp.fft.ifft(rounded(along_y.real) + 1j * rounded(along_y.imag), axis=2) * points
        return summed + weight * (along_x.real * along_x.real + along_x.imag * along_x.imag), None

    valence = lax.scan(add_band, jnp.zeros((points, points, points), jnp.float32), (orbitals, occupations))[0]
    density = valence + core_density
    rho_hat = jnp.fft.fftn(density)
    every_index = jnp.arange(points)
    q_full = jnp.where(every_index <= points // 2, every_index, every_index - points).astype(jnp.float32)
    g_full = jnp.where(every_index == points // 2, 0.0, q_full).astype(jnp.float32)
    wave_unit = 2.0 * math.pi / (points * SPACING)
    squared = wave_unit ** 2 * (q_full[:, None, None] ** 2 + q_full[None, :, None] ** 2 + q_full[None, None, :] ** 2)
    hartree_factor = jnp.where(squared > 0, 4.0 * math.pi / jnp.where(squared > 0, squared, 1.0), 0.0)
    hartree = jnp.fft.ifftn(hartree_factor * rho_hat).real
    grad_x = jnp.fft.ifftn(1j * wave_unit * g_full[None, None, :] * rho_hat).real
    grad_y = jnp.fft.ifftn(1j * wave_unit * g_full[None, :, None] * rho_hat).real
    grad_z = jnp.fft.ifftn(1j * wave_unit * g_full[:, None, None] * rho_hat).real
    potential = exchange_part(density, hartree, grad_x, grad_y, grad_z)
    return potential, jnp.stack([grad_x, grad_y, grad_z])
```

```python
import math

import jax
import jax.numpy as jnp
import numpy as np
from jax import lax
from jax.experimental.layout import Layout, with_layout_constraint
from jax.sharding import PartitionSpec as P

SPACING = 0.25
PBE_KAPPA = 0.804
PBE_MU = 0.2195
SLATER_COEF = 0.75 * (3.0 / math.pi) ** (1.0 / 3.0)
REDUCED_SCALE = 4.0 * (3.0 * math.pi**2) ** (2.0 / 3.0)
BF = jnp.bfloat16
F32 = jnp.float32
HIGH = lax.Precision.HIGH


def inverse_table(points):
    k = np.arange(points)
    angles = 2.0 * np.pi / points * (k[:, None] * k[None, :] % points)
    cosine, sine = np.cos(angles), np.sin(angles)
    return np.stack([np.stack([cosine, sine], 1), np.stack([-sine, cosine], 1)], 0)


def two_halves(table):
    high = table.astype(np.float32).astype(BF)
    low = (table - high.astype(np.float64)).astype(np.float32).astype(BF)
    return high, low


def dot2(spec, data, table):
    high, low = table
    first = jnp.einsum(spec, data, high, preferred_element_type=F32)
    return first + jnp.einsum(spec, data, low, preferred_element_type=F32)


def real_basis(points):
    pos = np.arange(points)
    freq = np.concatenate([np.arange(points // 2 + 1), np.arange(1, points // 2)])
    angle = 2.0 * np.pi / points * (pos[:, None] * freq[None, :] % points)
    basis = np.where(np.arange(points)[None, :] <= points // 2, np.cos(angle), np.sin(angle))
    scale = np.where((freq == 0) | (freq == points // 2), 1.0 / points, 2.0 / points)
    return basis * np.sqrt(scale), freq


def derivative_matrix(points):
    pos = np.arange(points)
    freq = np.arange(1, points // 2)
    unit = 2.0 * np.pi / (points * SPACING)
    lag = (pos[None, :] - pos[:, None]) % points
    values = np.zeros(points)
    for d in range(points):
        values[d] = np.sum(-2.0 * unit * freq * np.sin(2.0 * np.pi * (freq * d % points) / points)) / points
    return values[lag]


def exchange_part(density, hartree, grad_x, grad_y, grad_z):
    cube_root = jnp.cbrt(density)
    four_thirds = density * cube_root
    grad_square = grad_x * grad_x + grad_y * grad_y + grad_z * grad_z
    reduced = grad_square / (REDUCED_SCALE * four_thirds * four_thirds)
    denominator = 1.0 + PBE_MU * reduced / PBE_KAPPA
    enhance = 1.0 + PBE_KAPPA - PBE_KAPPA / denominator
    enhance_slope = PBE_MU / (denominator * denominator)
    return hartree - SLATER_COEF * cube_root * (
        4.0 / 3.0 * enhance - 8.0 / 3.0 * reduced * enhance_slope
    )


def share_density(orbitals, occupations, stick_map, px_index):
    bands_here, columns_here, doubled = orbitals.shape
    points = doubled // 2
    rows_px = lax.axis_size("px")
    rows_py = lax.axis_size("py")
    groups = lax.axis_size("band")
    xblock = points // rows_px
    yblock = points // rows_px
    pieces = groups * rows_py
    zshare = points // pieces
    sticks = columns_here * rows_py
    bands = groups * bands_here
    inverse = inverse_table(points)
    z_order = inverse.reshape(2, points, 2, rows_py, groups, zshare).transpose(0, 1, 4, 3, 2, 5)
    z_table = two_halves(z_order.reshape(doubled, pieces, 2 * zshare))
    columns = dot2("bsk,kdw->dbsw", orbitals, z_table).astype(BF)
    columns = lax.all_to_all(columns, ("band", "py"), split_axis=0, concat_axis=0, tiled=True)
    columns = lax.all_gather(columns, "px", axis=0, tiled=False)
    columns = columns.reshape(rows_px, groups, rows_py, bands_here, columns_here, 2, zshare)
    columns = columns.transpose(0, 2, 4, 5, 1, 3, 6).reshape(rows_px, sticks, 2, bands * zshare)
    places = lax.all_gather(stick_map, "px", axis=0, tiled=False)
    weights = lax.all_gather(occupations, "band", axis=0, tiled=True)
    y_hot = (places[:, 1, :, None] == jnp.arange(points, dtype=jnp.int32)).astype(BF)
    x_local = places[:, 0] - jnp.arange(rows_px, dtype=jnp.int32)[:, None] * xblock
    x_hot = x_local[:, :, None] == jnp.arange(xblock, dtype=jnp.int32)
    by_y = inverse.reshape(2, points, 2, rows_px, yblock).transpose(3, 1, 0, 4, 2)
    picked = [
        jnp.einsum(
            "psy,yiwo->psiwo",
            y_hot,
            lax.dynamic_index_in_dim(jnp.asarray(half), px_index, 0, keepdims=False),
            preferred_element_type=F32,
        ).astype(BF)
        for half in two_halves(by_y)
    ]
    x_table = two_halves(inverse.reshape(2, rows_px, xblock, 2, points).transpose(1, 0, 2, 3, 4))
    spread = jnp.where(x_hot[:, :, None, :, None], columns[:, :, :, None, :], jnp.zeros((), BF))
    plane = jnp.einsum("psiwo,psixz->pwoxz", picked[0], spread, preferred_element_type=F32)
    plane = plane + jnp.einsum("psiwo,psixz->pwoxz", picked[1], spread, preferred_element_type=F32)
    values = dot2("pwoxz,poxtk->wztk", plane.astype(BF), x_table)
    values = values.reshape(yblock, bands, zshare, 2, points)
    square = values[:, :, :, 0] * values[:, :, :, 0] + values[:, :, :, 1] * values[:, :, :, 1]
    return (weights[None, :, None, None] * square).sum(1)


def gathered(field):
    field = with_layout_constraint(field.astype(BF), Layout((0, 1, 2)))
    return lax.all_gather(field, "band", axis=0, tiled=True)


def body(orbitals, occupations, stick_map, core_density):
    points = orbitals.shape[2] // 2
    rows_px = lax.axis_size("px")
    rows_py = lax.axis_size("py")
    groups = lax.axis_size("band")
    px_index = lax.axis_index("px")
    py_index = lax.axis_index("py")
    band_index = lax.axis_index("band")
    yblock = points // rows_px
    xblock = points // rows_px
    zblock = points // rows_py
    zshare = zblock // groups
    pieces = groups * rows_py
    kyblock = points // pieces

    density = share_density(orbitals, occupations, stick_map, px_index)
    core = lax.dynamic_slice_in_dim(core_density, band_index * zshare, zshare, 0)
    rho = density + core.transpose(1, 0, 2)

    basis, freq = real_basis(points)
    derive = derivative_matrix(points).astype(np.float32)
    basis32 = basis.astype(np.float32)
    data = jnp.einsum("yzx,xpk->pyzk", rho, basis32.reshape(points, rows_px, xblock), precision=HIGH)
    grad_x = jnp.einsum("yzx,xw->zyw", rho, derive, precision=HIGH)
    data, grad_x_sent = lax.optimization_barrier((data, grad_x.astype(BF)))
    every_x = gathered(grad_x_sent)
    data = lax.all_to_all(data, "px", split_axis=0, concat_axis=0, tiled=True)
    data = data.reshape(points, zshare, xblock)
    high_basis, low_basis = two_halves(basis)
    x_basis = (high_basis.reshape(points, rows_px, xblock), low_basis.reshape(points, rows_px, xblock))
    lines_y = jnp.einsum("yzk,yw->wzk", data, derive, precision=HIGH).astype(BF)
    lines_y = lines_y.reshape(rows_px, yblock, zshare, xblock)
    lines_y = lax.all_to_all(lines_y, "px", split_axis=0, concat_axis=0, tiled=True)
    grad_y = dot2("pyzk,xpk->zyx", lines_y, x_basis)
    grad_y_sent = grad_y.astype(BF)
    modes = jnp.einsum("yzk,yj->jzk", data, basis32, precision=HIGH)
    modes = modes.reshape(pieces, kyblock, zshare, xblock)
    modes = lax.all_to_all(modes, ("band", "py"), split_axis=0, concat_axis=0, tiled=True)
    source = np.arange(points)
    device, within = source // zshare, source % zshare
    z_order = device % rows_py * zblock + device // rows_py * zshare + within
    z_basis = basis32[z_order].reshape(pieces, zshare, points)
    z_derive = derive[z_order][:, z_order].reshape(pieces, zshare, pieces, zshare)
    spectrum = jnp.einsum("djzk,dzm->mjk", modes, z_basis, precision=HIGH)
    unit = 2.0 * math.pi / (points * SPACING)
    all_q = jnp.asarray((freq * freq).astype(np.float32))
    q_col = lax.dynamic_slice_in_dim(all_q, (band_index * rows_py + py_index) * kyblock, kyblock)
    q_row = lax.dynamic_slice_in_dim(all_q, px_index * xblock, xblock)
    squared = unit**2 * (all_q[:, None, None] + q_col[None, :, None] + q_row[None, None, :])
    factor = jnp.where(squared > 0, 4.0 * math.pi / jnp.where(squared > 0, squared, 1.0), 0.0)
    spectrum = spectrum * factor
    back = jnp.stack(
        [
            jnp.einsum("mjk,dzm->djzk", spectrum, z_basis, precision=HIGH).astype(BF),
            jnp.einsum("ejwk,ewdz->djzk", modes, z_derive, precision=HIGH).astype(BF),
        ],
        1,
    )
    back, every_y, every_x = lax.optimization_barrier((back, grad_y_sent, every_x))
    every_y = gathered(every_y)
    back = lax.all_to_all(back, ("band", "py"), split_axis=0, concat_axis=0, tiled=True)
    y_basis = (high_basis.reshape(points, pieces, kyblock), low_basis.reshape(points, pieces, kyblock))
    lines = dot2("dfjzk,ydj->fyzk", back, y_basis)
    lines = lines.astype(BF).reshape(2, rows_px, yblock, zshare, xblock)
    lines = lax.all_to_all(lines, "px", split_axis=1, concat_axis=1, tiled=True)
    fields = dot2("fpyzk,xpk->fzyx", lines, x_basis)
    every_z = gathered(fields[1])
    potential = exchange_part(rho.transpose(1, 0, 2), fields[0], grad_x, grad_y, fields[1])
    every_potential = gathered(potential)
    gradient = jnp.stack([every_x.astype(F32), every_y.astype(F32), every_z.astype(F32)])
    return (every_potential.astype(F32), gradient)


def solution(mesh):
    return jax.shard_map(
        body,
        mesh=mesh,
        in_specs=(P("band", ("px", "py"), None), P("band"), P(None, "px"), P("py", "px", None)),
        out_specs=(P("py", "px", None), P(None, "py", "px", None)),
        check_vma=False,
    )
```

```python
import functools
import math

import jax
import jax.numpy as jnp
import numpy as np
from jax import lax
from jax.experimental import pallas as pl
from jax.experimental.pallas import tpu as pltpu
from jax.experimental.layout import Layout, with_layout_constraint
from jax.sharding import PartitionSpec as P

SPACING = 0.25
PBE_KAPPA = 0.804
PBE_MU = 0.2195
SLATER_COEF = 0.75 * (3.0 / math.pi) ** (1.0 / 3.0)
REDUCED_SCALE = 4.0 * (3.0 * math.pi**2) ** (2.0 / 3.0)
BF = jnp.bfloat16
F32 = jnp.float32
HIGH = lax.Precision.HIGH
CORE_LEAST = 0.05
CORE_TYPICAL = 0.2


def inverse_table(points):
    k = np.arange(points)
    angles = 2.0 * np.pi / points * (k[:, None] * k[None, :] % points)
    cosine, sine = np.cos(angles), np.sin(angles)
    return np.stack([np.stack([cosine, sine], 1), np.stack([-sine, cosine], 1)], 0)


def two_halves(table):
    high = table.astype(np.float32).astype(BF)
    low = (table - high.astype(np.float64)).astype(np.float32).astype(BF)
    return high, low


def dot2(spec, data, table):
    high, low = table
    first = jnp.einsum(spec, data, high, preferred_element_type=F32)
    return first + jnp.einsum(spec, data, low, preferred_element_type=F32)


def real_basis(points):
    pos = np.arange(points)
    freq = np.concatenate([np.arange(points // 2 + 1), np.arange(1, points // 2)])
    angle = 2.0 * np.pi / points * (pos[:, None] * freq[None, :] % points)
    basis = np.where(np.arange(points)[None, :] <= points // 2, np.cos(angle), np.sin(angle))
    scale = np.where((freq == 0) | (freq == points // 2), 1.0 / points, 2.0 / points)
    return basis * np.sqrt(scale), freq


def derivative_matrix(points):
    pos = np.arange(points)
    freq = np.arange(1, points // 2)
    unit = 2.0 * np.pi / (points * SPACING)
    lag = (pos[None, :] - pos[:, None]) % points
    values = np.zeros(points)
    for d in range(points):
        values[d] = np.sum(-2.0 * unit * freq * np.sin(2.0 * np.pi * (freq * d % points) / points)) / points
    return values[lag]


def exchange_part(density, hartree, grad_x, grad_y, grad_z):
    cube_root = jnp.cbrt(density)
    four_thirds = density * cube_root
    grad_square = grad_x * grad_x + grad_y * grad_y + grad_z * grad_z
    reduced = grad_square / (REDUCED_SCALE * four_thirds * four_thirds)
    denominator = 1.0 + PBE_MU * reduced / PBE_KAPPA
    enhance = 1.0 + PBE_KAPPA - PBE_KAPPA / denominator
    enhance_slope = PBE_MU / (denominator * denominator)
    return hartree - SLATER_COEF * cube_root * (
        4.0 / 3.0 * enhance - 8.0 / 3.0 * reduced * enhance_slope
    )


def share_density(orbitals, occupations, stick_map, px_index):
    bands_here, columns_here, doubled = orbitals.shape
    points = doubled // 2
    rows_px = lax.axis_size("px")
    rows_py = lax.axis_size("py")
    groups = lax.axis_size("band")
    xblock = points // rows_px
    yblock = points // rows_px
    pieces = groups * rows_py
    zshare = points // pieces
    sticks = columns_here * rows_py
    bands = groups * bands_here
    inverse = inverse_table(points)
    z_order = inverse.reshape(2, points, 2, rows_py, groups, zshare).transpose(0, 1, 4, 3, 2, 5)
    z_table = two_halves(z_order.reshape(doubled, pieces, 2 * zshare))
    columns = dot2("bsk,kdw->dbsw", orbitals, z_table).astype(BF)
    columns = lax.all_to_all(columns, ("band", "py"), split_axis=0, concat_axis=0, tiled=True)
    columns = lax.all_gather(columns, "px", axis=0, tiled=False)
    columns = columns.reshape(rows_px, groups, rows_py, bands_here, columns_here, 2, zshare)
    columns = columns.transpose(0, 2, 4, 5, 1, 3, 6).reshape(rows_px, sticks, 2, bands * zshare)
    places = lax.all_gather(stick_map, "px", axis=0, tiled=False)
    loads = (orbitals.astype(F32) ** 2).sum((1, 2))
    first = (px_index == 0) & (lax.axis_index("py") == 0)
    own = jnp.where(jnp.arange(groups)[:, None] == lax.axis_index("band"), occupations[None, :], 0.0).reshape(bands)
    totals = jnp.concatenate([jnp.where(first, own, 0.0), (occupations * loads).sum()[None]])
    totals = lax.psum(totals, ("band", "px", "py"))
    weights, mean = totals[:bands], totals[bands]
    y_hot = (places[:, 1, :, None] == jnp.arange(points, dtype=jnp.int32)).astype(BF)
    x_local = places[:, 0] - jnp.arange(rows_px, dtype=jnp.int32)[:, None] * xblock
    x_hot = x_local[:, :, None] == jnp.arange(xblock, dtype=jnp.int32)
    by_y = inverse.reshape(2, points, 2, rows_px, yblock).transpose(3, 1, 0, 4, 2)
    picked = [
        jnp.einsum(
            "psy,yiwo->psiwo",
            y_hot,
            lax.dynamic_index_in_dim(jnp.asarray(half), px_index, 0, keepdims=False),
            preferred_element_type=F32,
        ).astype(BF)
        for half in two_halves(by_y)
    ]
    x_table = two_halves(inverse.reshape(2, rows_px, xblock, 2, points).transpose(1, 0, 2, 3, 4))
    spread = jnp.where(x_hot[:, :, None, :, None], columns[:, :, :, None, :], jnp.zeros((), BF))
    plane = jnp.einsum("psiwo,psixz->pwoxz", picked[0], spread, preferred_element_type=F32)
    plane = plane + jnp.einsum("psiwo,psixz->pwoxz", picked[1], spread, preferred_element_type=F32)
    values = dot2("pwoxz,poxtk->wztk", plane.astype(BF), x_table)
    values = values.reshape(yblock, bands, zshare, 2, points)
    square = values[:, :, :, 0] * values[:, :, :, 0] + values[:, :, :, 1] * values[:, :, :, 1]
    return (weights[None, :, None, None] * square).sum(1), mean


def gathered(field):
    field = with_layout_constraint(field.astype(BF), Layout((0, 1, 2)))
    return lax.all_gather(field, "band", axis=0, tiled=True)


LANES = 128
HALF = 64


def halves_stack(table, axis):
    return jnp.asarray(np.concatenate([np.asarray(h) for h in two_halves(table)], axis))


def packed_lane(parity, mode):
    return np.where(mode < LANES, parity * LANES + mode, 2 * LANES + parity * HALF + mode - LANES)


def chain_tables(points, rows_px, rows_py, groups):
    basis, freq = real_basis(points)
    derive = derivative_matrix(points)
    xblock = points // rows_px
    zshare = points // (rows_py * groups)
    modes = np.arange(points)
    forward = np.zeros((2, points, 3 * LANES + rows_px * LANES))
    spread = np.zeros((rows_px, LANES, 3 * LANES))
    for parity in range(2):
        forward[parity][:, packed_lane(parity, modes)] = basis
        lane = modes // xblock * LANES + parity * HALF + modes % xblock
        forward[parity][:, 3 * LANES + lane] = basis
        spread[modes // xblock, parity * HALF + modes % xblock, packed_lane(parity, modes)] = 1.0
    source = np.arange(points // 2)
    device, within = source // (zshare // 2), source % (zshare // 2)
    even = device % rows_py * (points // rows_py) + device // rows_py * zshare + 2 * within
    to_modes = [half for z in (even, even + 1) for half in two_halves(basis[z].T)]
    from_modes = np.concatenate([basis[even], basis[even + 1]], 0)
    return dict(
        forward=jnp.stack([jnp.asarray(h) for h in two_halves(forward)]),
        y_in=halves_stack(basis.T, 0),
        y_out=halves_stack(basis, 0),
        y_slope=halves_stack(derive.T, 0),
        z_in=jnp.asarray(np.concatenate([np.asarray(h) for h in to_modes], 0)),
        z_out=halves_stack(from_modes, 0),
        spread=jnp.asarray(spread.astype(np.float32).astype(BF)),
    )


def slope_tables(points, rows_py, groups):
    derive = derivative_matrix(points)
    pairs = np.arange(points // 2)
    zblock = points // rows_py
    own = []
    for py in range(rows_py):
        order = np.concatenate([np.arange(zblock) + q * zblock for q in [py] + [q for q in range(rows_py) if q != py]])
        mine = np.arange(zblock) + py * zblock
        parts = []
        for out_parity in range(2):
            for in_parity in range(2):
                parts.append(derive[np.ix_(order[in_parity::2], mine[out_parity::2])].T)
        own.append(np.concatenate(parts, 0))
    stacked = np.stack(own)
    return np.concatenate([np.asarray(h) for h in two_halves(stacked)], 1)


def final_tables(points):
    basis, _ = real_basis(points)
    derive = derivative_matrix(points)
    out = np.zeros((2, 2 * LANES, 2, 2 * LANES))
    for parity in range(2):
        modes = np.arange(points)
        row = np.where(modes < LANES, modes, parity * HALF + modes)
        out[parity, row, 0, :points] = basis.T
        out[parity, row, 1, :points] = basis.T @ derive
    high, low = two_halves(out)
    both = np.stack([np.asarray(high), np.asarray(low)], 3)
    return jnp.asarray(both.reshape(2, 2 * LANES, 2, 4 * LANES).transpose(0, 2, 1, 3))


def dotf(left, right):
    return jnp.dot(left, right, preferred_element_type=F32)


def split(value):
    high = value.astype(BF)
    return high, (value - high.astype(F32)).astype(BF)


def chain_kernel(
    dims, rho, forward, y_in, y_out, y_slope, z_in, z_out, spread, factor, slope,
    xs, gy, gz, h,
    others, c1s, c1, c2s, c2, c3s, c3, c4s, c4, gin, gs, wide, deep, sends, recvs,
):
    points, rows_px, rows_py, groups = dims
    yblock = points // rows_px
    zpairs = points // (rows_py * groups) // 2
    pieces = groups * rows_py
    kyblock = points // pieces
    rows = zpairs * yblock
    short = zpairs * kyblock
    band, px, py = lax.axis_index("band"), lax.axis_index("px"), lax.axis_index("py")
    me = band * rows_py + py
    px_peers = [lax.rem(px + s, rows_px) for s in range(1, rows_px)]
    zy_peers = [
        (lax.rem(band + b, groups), lax.rem(py + q, rows_py))
        for b in range(groups) for q in range(rows_py) if b or q
    ]
    barrier = pltpu.get_barrier_semaphore()
    for peer in px_peers:
        pl.semaphore_signal(barrier, inc=1, device_id=(band, peer, py), device_id_type=pl.DeviceIdType.MESH)
    for peer_band, peer_py in zy_peers:
        pl.semaphore_signal(barrier, inc=1, device_id=(peer_band, px, peer_py), device_id_type=pl.DeviceIdType.MESH)
    pl.semaphore_wait(barrier, len(px_peers) + len(zy_peers))
    used = []

    def send(src, dst, device):
        copy = pltpu.make_async_remote_copy(
            src_ref=src, dst_ref=dst, send_sem=sends.at[len(used)], recv_sem=recvs.at[len(used)],
            device_id=device, device_id_type=pl.DeviceIdType.MESH,
        )
        used.append(copy)
        copy.start()
        return copy

    def to_px(src, dst):
        return [send(src.at[peer], dst.at[px], (band, peer, py)) for peer in px_peers]

    def to_zy(src, dst):
        return [
            send(src.at[b * rows_py + q], dst.at[me], (b, px, q)) for b, q in zy_peers
        ]

    def arrived(copies):
        for copy in copies:
            copy.wait_recv()

    right, left = lax.rem(band + 1, groups), lax.rem(band + groups - 1, groups)

    def to_band(field, slot, target):
        return send(field.at[slot], field.at[slot], (target, px, py))

    def to_other(slot):
        return send(xs.at[slot], others.at[slot], (band, px, lax.rem(py + 1, rows_py)))

    step = 2 * yblock

    @pl.loop(0, rows // step)
    def _(i):
        at = pl.ds(pl.multiple_of(i * step, step), step)
        out = None
        for parity in range(2):
            high, low = split(rho[parity, at, :])
            part = dotf(high, forward[0, parity]) + dotf(low, forward[0, parity]) + dotf(high, forward[1, parity])
            out = part if out is None else out + part
        xs[band, at, :] = out[:, : 3 * LANES].astype(BF)
        for p in range(rows_px):
            c1s[p, at, :] = out[:, (3 + p) * LANES : (4 + p) * LANES].astype(BF)

    first = to_px(c1s, c1)
    ring_right = to_band(xs, band, right)
    ring_left = to_band(xs, band, left)
    across = [to_other(band)]
    c1[px] = c1s[px]
    arrived(first)

    @pl.loop(0, zpairs // 2)
    def _(i):
        found = []
        for k in range(2):
            at = pl.ds(pl.multiple_of((2 * i + k) * yblock, yblock), yblock)
            out = dotf(y_in[...], jnp.concatenate([c1[p, at, :] for p in range(rows_px)], 0))
            found.append(out[:points] + out[points:])
        at = pl.ds(pl.multiple_of(i * 2 * kyblock, 2 * kyblock), 2 * kyblock)
        for d in range(pieces):
            cut = slice(d * kyblock, (d + 1) * kyblock)
            c2s[d, at, :] = jnp.concatenate([f[cut] for f in found], 0).astype(BF)

    second = to_zy(c2s, c2)
    c2[me] = c2s[me]
    ring_right.wait_recv()
    ring_far = to_band(xs, left, right)
    across.append(to_other(left))
    ring_left.wait_recv()
    across.append(to_other(right))
    arrived(second)
    for d in range(pieces):
        wide[pl.ds(d * short, short), :] = c2[d].astype(F32)
    lane = lax.broadcasted_iota(jnp.int32, (points, LANES), 1)
    column = pieces * zpairs

    @pl.loop(0, kyblock)
    def _(j):
        data = wide[pl.ds(j, column, stride=kyblock), :].astype(BF)
        out = dotf(z_in[...], data)
        even = out[:points] + out[points : 2 * points]
        odd = out[2 * points : 3 * points] + out[3 * points :]
        spectrum = (even + pltpu.roll(odd, HALF, 1)) * factor[j]
        spectrum = jnp.where(lane < HALF, spectrum, pltpu.roll(spectrum, HALF, 1))
        high, low = split(spectrum)
        back = dotf(z_out[...], high)
        back = back[:points] + back[points:] + dotf(z_out[:points, :], low)
        wide[pl.ds(j, column, stride=kyblock), :] = jnp.where(
            lane[:column] < HALF, back[:column], back[column:]
        )

    for d in range(pieces):
        c3s[d] = wide[pl.ds(d * short, short), :].astype(BF)
    third = to_zy(c3s, c3)
    c3[me] = c3s[me]
    ring_far.wait_recv()
    far = lax.rem(band + 2, groups)
    across.append(to_other(far))
    outward = to_px(xs, gin)
    gin[px] = xs[px]
    arrived(third)
    for d in range(pieces):
        wide[pl.ds(d * short, short), :] = c3[d].astype(F32)

    @pl.loop(0, zpairs)
    def _(i):
        data = jnp.concatenate(
            [wide[pl.ds(pl.multiple_of(d * short + i * kyblock, 8), kyblock), :] for d in range(pieces)], 0
        ).astype(BF)
        out = dotf(y_out[...], data)
        out = out[:points] + out[points:]
        at = pl.ds(pl.multiple_of(i * yblock, yblock), yblock)
        for p in range(rows_px):
            c4s[p, at, :] = out[p * yblock : (p + 1) * yblock].astype(BF)

    fourth = to_px(c4s, c4)
    c4[px] = c4s[px]
    arrived(fourth)

    @pl.loop(0, rows // step)
    def _(i):
        at = pl.ds(pl.multiple_of(i * step, step), step)
        out = None
        for p in range(rows_px):
            part = dotf(c4[p, at, :], spread[p])
            out = part if out is None else out + part
        h[band, at, :] = out.astype(BF)

    h_right = to_band(h, band, right)
    h_left = to_band(h, band, left)
    arrived(outward)

    @pl.loop(0, zpairs)
    def _(i):
        at = pl.ds(pl.multiple_of(i * yblock, yblock), yblock)
        out = dotf(y_slope[...], jnp.concatenate([gin[p, at, :] for p in range(rows_px)], 0))
        out = out[:points] + out[points:]
        for p in range(rows_px):
            gs[p, at, :] = out[p * yblock : (p + 1) * yblock].astype(BF)

    homeward = to_px(gs, gy)
    gy[px] = gs[px]
    h_right.wait_recv()
    h_far = to_band(h, left, right)
    arrived(across)
    own_rows = groups * rows
    for b in range(groups):
        for t in range(3):
            cut = pl.ds(t * LANES, LANES)
            deep[t, pl.ds(b * rows, rows), :] = xs[b, :, cut].astype(F32)
            deep[t, pl.ds(own_rows + b * rows, rows), :] = others[b, :, cut].astype(F32)
    zlines = groups * zpairs
    tail = lax.broadcasted_iota(jnp.int32, (zlines, LANES), 1) < HALF

    @pl.loop(0, yblock)
    def _(j):
        data = [
            deep[t, pl.ds(j, rows_py * zlines, stride=yblock), :].astype(BF) for t in range(3)
        ]
        out = [dotf(slope[...], d) for d in data]
        parts = [
            [out[t][q * zlines : (q + 1) * zlines] + out[t][(4 + q) * zlines : (5 + q) * zlines] for q in range(4)]
            for t in range(3)
        ]
        even = parts[2][0] + pltpu.roll(parts[2][1], HALF, 1)
        odd = pltpu.roll(parts[2][2], HALF, 1) + parts[2][3]
        at = pl.ds(j, zlines, stride=yblock)
        deep[0, at, :] = parts[0][0] + parts[1][1]
        deep[1, at, :] = parts[0][2] + parts[1][3]
        deep[2, at, :] = jnp.where(tail, even, odd)

    for b in range(groups):
        for t in range(3):
            gz[b, :, pl.ds(t * LANES, LANES)] = deep[t, pl.ds(b * rows, rows), :].astype(BF)
    h_left.wait_recv()
    h_far.wait_recv()
    arrived(homeward)
    for copy in used:
        copy.wait_send()


def run_chain(rho, factor, slope, tables, dims):
    points, rows_px, rows_py, groups = dims
    yblock = points // rows_px
    zpairs = points // (rows_py * groups) // 2
    pieces = groups * rows_py
    kyblock = points // pieces
    rows, short = zpairs * yblock, zpairs * kyblock
    copies = 4 * (rows_px - 1) + 2 * (pieces - 1) + 3 + 3 + groups
    field = jax.ShapeDtypeStruct((groups, rows, 3 * LANES), BF)
    vmem = pl.BlockSpec(memory_space=pltpu.VMEM)
    lined = pltpu.VMEM((rows_px, rows, LANES), BF)
    cut = pltpu.VMEM((pieces, short, LANES), BF)
    names = ("forward", "y_in", "y_out", "y_slope", "z_in", "z_out", "spread")
    return pl.pallas_call(
        functools.partial(chain_kernel, dims),
        out_shape=[field] * 4,
        in_specs=[vmem] * (len(names) + 3),
        out_specs=[vmem] * 4,
        scratch_shapes=[
            pltpu.VMEM((groups, rows, 3 * LANES), BF),
            lined, lined, cut, cut, cut, cut, lined, lined,
            pltpu.VMEM((rows_px, rows, 3 * LANES), BF),
            pltpu.VMEM((rows_px, rows, 3 * LANES), BF),
            pltpu.VMEM((pieces * short, LANES), F32),
            pltpu.VMEM((3, rows_py * groups * rows, LANES), F32),
            pltpu.SemaphoreType.DMA((copies,)),
            pltpu.SemaphoreType.DMA((copies,)),
        ],
        compiler_params=pltpu.CompilerParams(
            collective_id=1, has_side_effects=True, vmem_limit_bytes=60 << 20
        ),
    )(rho, *[tables[n] for n in names], factor, slope)


def final_kernel(dims, shift, xs, gy, gz, h, table, potential, gradient):
    points, yblock, pairs = dims
    for parity in range(2):
        first = slice(parity * LANES, (parity + 1) * LANES)

        def natural(ref):
            value = ref[...]
            return jnp.concatenate([value[:, first], value[:, 2 * LANES :]], 1)

        lines = natural(xs)
        out = dotf(jnp.concatenate([lines, natural(gy), natural(gz), natural(h)], 0), table[parity, 0])
        out = (out[:, : 2 * LANES] + out[:, 2 * LANES :])[:, :points]
        grad_x = dotf(lines, table[parity, 1])
        grad_x = (grad_x[:, : 2 * LANES] + grad_x[:, 2 * LANES :])[:, :points]
        n = pairs * yblock
        density, grad_y, grad_z, hartree = (out[k * n : (k + 1) * n] for k in range(4))
        density = jnp.maximum(density + shift[0], CORE_LEAST)
        cube_root = jnp.exp(jnp.log(density) * (1.0 / 3.0))
        four_thirds = density * cube_root
        grad_square = grad_x * grad_x + grad_y * grad_y + grad_z * grad_z
        scale = (PBE_MU / (PBE_KAPPA * REDUCED_SCALE)) * grad_square
        inverse = 1.0 / (four_thirds * four_thirds + scale)
        ratio = four_thirds * four_thirds * inverse
        steep = scale * inverse
        part = (4.0 / 3.0) * (1.0 + PBE_KAPPA - PBE_KAPPA * ratio) - (8.0 / 3.0) * PBE_KAPPA * steep * ratio
        value = hartree - SLATER_COEF * cube_root * part
        for k in range(pairs):
            cut = slice(k * yblock, (k + 1) * yblock)
            potential[2 * k + parity] = value[cut]
            gradient[0, 2 * k + parity] = grad_x[cut]
            gradient[1, 2 * k + parity] = grad_y[cut]
            gradient[2, 2 * k + parity] = grad_z[cut]


def run_final(xs, gy, gz, h, shift, points, yblock):
    groups, rows, _ = xs.shape
    pairs = 2
    steps = groups * rows // (pairs * yblock)
    zblock = steps * 2 * pairs
    table = final_tables(points)
    flat = pl.BlockSpec((pairs * yblock, 3 * LANES), lambda i: (i, 0))
    return pl.pallas_call(
        functools.partial(final_kernel, (points, yblock, pairs)),
        grid=(steps,),
        out_shape=[
            jax.ShapeDtypeStruct((zblock, yblock, points), F32),
            jax.ShapeDtypeStruct((3, zblock, yblock, points), F32),
        ],
        in_specs=[pl.BlockSpec(memory_space=pltpu.SMEM)]
        + [flat] * 4
        + [pl.BlockSpec(table.shape, lambda i: (0, 0, 0, 0))],
        out_specs=[
            pl.BlockSpec((2 * pairs, yblock, points), lambda i: (i, 0, 0)),
            pl.BlockSpec((3, 2 * pairs, yblock, points), lambda i: (0, i, 0, 0)),
        ],
    )(shift, *[f.reshape(groups * rows, 3 * LANES) for f in (xs, gy, gz, h)], table)


def fast_body(orbitals, occupations, stick_map, core_density):
    points = orbitals.shape[2] // 2
    rows_px, rows_py, groups = lax.axis_size("px"), lax.axis_size("py"), lax.axis_size("band")
    px_index, py_index, band_index = lax.axis_index("px"), lax.axis_index("py"), lax.axis_index("band")
    dims = (points, rows_px, rows_py, groups)
    yblock = xblock = points // rows_px
    zshare = points // (rows_py * groups)
    kyblock = points // (rows_py * groups)
    density, mean = share_density(orbitals, occupations, stick_map, px_index)
    core = lax.dynamic_slice_in_dim(core_density, band_index * zshare, zshare, 0)
    shift = mean + CORE_TYPICAL
    rho = density.transpose(1, 0, 2) + (core - shift)
    rho = rho.reshape(zshare // 2, 2, yblock, points).transpose(1, 0, 2, 3).reshape(2, zshare // 2 * yblock, points)
    _, freq = real_basis(points)
    unit = 2.0 * math.pi / (points * SPACING)
    all_q = (freq * freq).astype(np.float32)
    lane_q = np.zeros((rows_px, LANES), np.float32)
    lane_q[:, :xblock] = all_q.reshape(rows_px, xblock)
    q_row = lax.dynamic_index_in_dim(jnp.asarray(lane_q), px_index, 0, keepdims=False)
    q_col = lax.dynamic_slice_in_dim(jnp.asarray(all_q), (band_index * rows_py + py_index) * kyblock, kyblock)
    squared = unit**2 * (q_col[:, None, None] + all_q[None, :, None] + q_row[None, None, :])
    factor = jnp.where(squared > 0, 4.0 * math.pi / jnp.where(squared > 0, squared, 1.0), 0.0)
    slope = lax.dynamic_index_in_dim(jnp.asarray(slope_tables(points, rows_py, groups)), py_index, 0, keepdims=False)
    tables = chain_tables(points, rows_px, rows_py, groups)
    xs, gy, gz, h = run_chain(rho, factor, slope, tables, dims)
    return tuple(run_final(xs, gy, gz, h, shift.reshape(1), points, yblock))


def body(orbitals, occupations, stick_map, core_density):
    points = orbitals.shape[2] // 2
    rows_px = lax.axis_size("px")
    rows_py = lax.axis_size("py")
    groups = lax.axis_size("band")
    px_index = lax.axis_index("px")
    py_index = lax.axis_index("py")
    band_index = lax.axis_index("band")
    yblock = points // rows_px
    xblock = points // rows_px
    zblock = points // rows_py
    zshare = zblock // groups
    pieces = groups * rows_py
    kyblock = points // pieces

    density, _ = share_density(orbitals, occupations, stick_map, px_index)
    core = lax.dynamic_slice_in_dim(core_density, band_index * zshare, zshare, 0)
    rho = density + core.transpose(1, 0, 2)

    basis, freq = real_basis(points)
    derive = derivative_matrix(points).astype(np.float32)
    basis32 = basis.astype(np.float32)
    data = jnp.einsum("yzx,xpk->pyzk", rho, basis32.reshape(points, rows_px, xblock), precision=HIGH)
    grad_x = jnp.einsum("yzx,xw->zyw", rho, derive, precision=HIGH)
    data, grad_x_sent = lax.optimization_barrier((data, grad_x.astype(BF)))
    every_x = gathered(grad_x_sent)
    data = lax.all_to_all(data, "px", split_axis=0, concat_axis=0, tiled=True)
    data = data.reshape(points, zshare, xblock)
    high_basis, low_basis = two_halves(basis)
    x_basis = (high_basis.reshape(points, rows_px, xblock), low_basis.reshape(points, rows_px, xblock))
    lines_y = jnp.einsum("yzk,yw->wzk", data, derive, precision=HIGH).astype(BF)
    lines_y = lines_y.reshape(rows_px, yblock, zshare, xblock)
    lines_y = lax.all_to_all(lines_y, "px", split_axis=0, concat_axis=0, tiled=True)
    grad_y = dot2("pyzk,xpk->zyx", lines_y, x_basis)
    grad_y_sent = grad_y.astype(BF)
    modes = jnp.einsum("yzk,yj->jzk", data, basis32, precision=HIGH)
    modes = modes.reshape(pieces, kyblock, zshare, xblock)
    modes = lax.all_to_all(modes, ("band", "py"), split_axis=0, concat_axis=0, tiled=True)
    source = np.arange(points)
    device, within = source // zshare, source % zshare
    z_order = device % rows_py * zblock + device // rows_py * zshare + within
    z_basis = basis32[z_order].reshape(pieces, zshare, points)
    z_derive = derive[z_order][:, z_order].reshape(pieces, zshare, pieces, zshare)
    spectrum = jnp.einsum("djzk,dzm->mjk", modes, z_basis, precision=HIGH)
    unit = 2.0 * math.pi / (points * SPACING)
    all_q = jnp.asarray((freq * freq).astype(np.float32))
    q_col = lax.dynamic_slice_in_dim(all_q, (band_index * rows_py + py_index) * kyblock, kyblock)
    q_row = lax.dynamic_slice_in_dim(all_q, px_index * xblock, xblock)
    squared = unit**2 * (all_q[:, None, None] + q_col[None, :, None] + q_row[None, None, :])
    factor = jnp.where(squared > 0, 4.0 * math.pi / jnp.where(squared > 0, squared, 1.0), 0.0)
    spectrum = spectrum * factor
    back = jnp.stack(
        [
            jnp.einsum("mjk,dzm->djzk", spectrum, z_basis, precision=HIGH).astype(BF),
            jnp.einsum("ejwk,ewdz->djzk", modes, z_derive, precision=HIGH).astype(BF),
        ],
        1,
    )
    back, every_y, every_x = lax.optimization_barrier((back, grad_y_sent, every_x))
    every_y = gathered(every_y)
    back = lax.all_to_all(back, ("band", "py"), split_axis=0, concat_axis=0, tiled=True)
    y_basis = (high_basis.reshape(points, pieces, kyblock), low_basis.reshape(points, pieces, kyblock))
    lines = dot2("dfjzk,ydj->fyzk", back, y_basis)
    lines = lines.astype(BF).reshape(2, rows_px, yblock, zshare, xblock)
    lines = lax.all_to_all(lines, "px", split_axis=1, concat_axis=1, tiled=True)
    fields = dot2("fpyzk,xpk->fzyx", lines, x_basis)
    every_z = gathered(fields[1])
    potential = exchange_part(rho.transpose(1, 0, 2), fields[0], grad_x, grad_y, fields[1])
    every_potential = gathered(potential)
    gradient = jnp.stack([every_x.astype(F32), every_y.astype(F32), every_z.astype(F32)])
    return (every_potential.astype(F32), gradient)


def solution(mesh):
    def step(orbitals, occupations, stick_map, core_density):
        points = orbitals.shape[2] // 2
        block = points // mesh.shape["px"]
        share = points // (mesh.shape["py"] * mesh.shape["band"])
        fits = (
            points == LANES + HALF and block <= HALF and block % 16 == 0 and share % 8 == 0
            and mesh.shape["py"] == 2 and mesh.shape["band"] == 4
        )
        return (fast_body if fits else body)(orbitals, occupations, stick_map, core_density)

    return jax.shard_map(
        step,
        mesh=mesh,
        in_specs=(P("band", ("px", "py"), None), P("band"), P(None, "px"), P("py", "px", None)),
        out_specs=(P("py", "px", None), P(None, "py", "px", None)),
        check_vma=False,
    )
```

```python
import functools
import math

import jax
import jax.numpy as jnp
import numpy as np
from jax import lax
from jax.experimental import pallas as pl
from jax.experimental.pallas import tpu as pltpu
from jax.experimental.layout import Layout, with_layout_constraint
from jax.sharding import PartitionSpec as P

SPACING = 0.25
PBE_KAPPA = 0.804
PBE_MU = 0.2195
SLATER_COEF = 0.75 * (3.0 / math.pi) ** (1.0 / 3.0)
REDUCED_SCALE = 4.0 * (3.0 * math.pi**2) ** (2.0 / 3.0)
BF = jnp.bfloat16
F32 = jnp.float32
HIGH = lax.Precision.HIGH
CORE_LEAST = 0.05
CORE_TYPICAL = 0.2


def inverse_table(points):
    k = np.arange(points)
    angles = 2.0 * np.pi / points * (k[:, None] * k[None, :] % points)
    cosine, sine = np.cos(angles), np.sin(angles)
    return np.stack([np.stack([cosine, sine], 1), np.stack([-sine, cosine], 1)], 0)


def two_halves(table):
    high = table.astype(np.float32).astype(BF)
    low = (table - high.astype(np.float64)).astype(np.float32).astype(BF)
    return high, low


def dot2(spec, data, table):
    high, low = table
    first = jnp.einsum(spec, data, high, preferred_element_type=F32)
    return first + jnp.einsum(spec, data, low, preferred_element_type=F32)


def real_basis(points):
    pos = np.arange(points)
    freq = np.concatenate([np.arange(points // 2 + 1), np.arange(1, points // 2)])
    angle = 2.0 * np.pi / points * (pos[:, None] * freq[None, :] % points)
    basis = np.where(np.arange(points)[None, :] <= points // 2, np.cos(angle), np.sin(angle))
    scale = np.where((freq == 0) | (freq == points // 2), 1.0 / points, 2.0 / points)
    return basis * np.sqrt(scale), freq


def derivative_matrix(points):
    pos = np.arange(points)
    freq = np.arange(1, points // 2)
    unit = 2.0 * np.pi / (points * SPACING)
    lag = (pos[None, :] - pos[:, None]) % points
    values = np.zeros(points)
    for d in range(points):
        values[d] = np.sum(-2.0 * unit * freq * np.sin(2.0 * np.pi * (freq * d % points) / points)) / points
    return values[lag]


def exchange_part(density, hartree, grad_x, grad_y, grad_z):
    cube_root = jnp.cbrt(density)
    four_thirds = density * cube_root
    grad_square = grad_x * grad_x + grad_y * grad_y + grad_z * grad_z
    reduced = grad_square / (REDUCED_SCALE * four_thirds * four_thirds)
    denominator = 1.0 + PBE_MU * reduced / PBE_KAPPA
    enhance = 1.0 + PBE_KAPPA - PBE_KAPPA / denominator
    enhance_slope = PBE_MU / (denominator * denominator)
    return hartree - SLATER_COEF * cube_root * (
        4.0 / 3.0 * enhance - 8.0 / 3.0 * reduced * enhance_slope
    )


def share_density(orbitals, occupations, stick_map, px_index):
    bands_here, columns_here, doubled = orbitals.shape
    points = doubled // 2
    rows_px = lax.axis_size("px")
    rows_py = lax.axis_size("py")
    groups = lax.axis_size("band")
    xblock = points // rows_px
    yblock = points // rows_px
    pieces = groups * rows_py
    zshare = points // pieces
    sticks = columns_here * rows_py
    bands = groups * bands_here
    inverse = inverse_table(points)
    z_order = inverse.reshape(2, points, 2, rows_py, groups, zshare).transpose(0, 1, 4, 3, 2, 5)
    z_table = two_halves(z_order.reshape(doubled, pieces, 2 * zshare))
    columns = dot2("bsk,kdw->dbsw", orbitals, z_table).astype(BF)
    columns = lax.all_to_all(columns, ("band", "py"), split_axis=0, concat_axis=0, tiled=True)
    columns = lax.all_gather(columns, "px", axis=0, tiled=False)
    columns = columns.reshape(rows_px, groups, rows_py, bands_here, columns_here, 2, zshare)
    columns = columns.transpose(0, 2, 4, 5, 1, 3, 6).reshape(rows_px, sticks, 2, bands * zshare)
    places = lax.all_gather(stick_map, "px", axis=0, tiled=False)
    loads = (orbitals.astype(F32) ** 2).sum((1, 2))
    first = (px_index == 0) & (lax.axis_index("py") == 0)
    own = jnp.where(jnp.arange(groups)[:, None] == lax.axis_index("band"), occupations[None, :], 0.0).reshape(bands)
    totals = jnp.concatenate([jnp.where(first, own, 0.0), (occupations * loads).sum()[None]])
    totals = lax.psum(totals, ("band", "px", "py"))
    weights, mean = totals[:bands], totals[bands]
    y_hot = (places[:, 1, :, None] == jnp.arange(points, dtype=jnp.int32)).astype(BF)
    x_local = places[:, 0] - jnp.arange(rows_px, dtype=jnp.int32)[:, None] * xblock
    x_hot = x_local[:, :, None] == jnp.arange(xblock, dtype=jnp.int32)
    by_y = inverse.reshape(2, points, 2, rows_px, yblock).transpose(3, 1, 0, 4, 2)
    picked = [
        jnp.einsum(
            "psy,yiwo->psiwo",
            y_hot,
            lax.dynamic_index_in_dim(jnp.asarray(half), px_index, 0, keepdims=False),
            preferred_element_type=F32,
        ).astype(BF)
        for half in two_halves(by_y)
    ]
    x_table = two_halves(inverse.reshape(2, rows_px, xblock, 2, points).transpose(1, 0, 2, 3, 4))
    spread = jnp.where(x_hot[:, :, None, :, None], columns[:, :, :, None, :], jnp.zeros((), BF))
    plane = jnp.einsum("psiwo,psixz->pwoxz", picked[0], spread, preferred_element_type=F32)
    plane = plane + jnp.einsum("psiwo,psixz->pwoxz", picked[1], spread, preferred_element_type=F32)
    values = dot2("pwoxz,poxtk->wztk", plane.astype(BF), x_table)
    values = values.reshape(yblock, bands, zshare, 2, points)
    square = values[:, :, :, 0] * values[:, :, :, 0] + values[:, :, :, 1] * values[:, :, :, 1]
    return (weights[None, :, None, None] * square).sum(1), mean


def gathered(field):
    field = with_layout_constraint(field.astype(BF), Layout((0, 1, 2)))
    return lax.all_gather(field, "band", axis=0, tiled=True)


LANES = 128
HALF = 64


def halves_stack(table, axis):
    return jnp.asarray(np.concatenate([np.asarray(h) for h in two_halves(table)], axis))


def packed_lane(parity, mode):
    return np.where(mode < LANES, parity * LANES + mode, 2 * LANES + parity * HALF + mode - LANES)


def chain_tables(points, rows_px, rows_py, groups):
    basis, freq = real_basis(points)
    derive = derivative_matrix(points)
    xblock = points // rows_px
    zshare = points // (rows_py * groups)
    modes = np.arange(points)
    forward = np.zeros((2, points, 3 * LANES + rows_px * LANES))
    spread = np.zeros((rows_px, LANES, 3 * LANES))
    for parity in range(2):
        forward[parity][:, packed_lane(parity, modes)] = basis
        lane = modes // xblock * LANES + parity * HALF + modes % xblock
        forward[parity][:, 3 * LANES + lane] = basis
        spread[modes // xblock, parity * HALF + modes % xblock, packed_lane(parity, modes)] = 1.0
    source = np.arange(points // 2)
    device, within = source // (zshare // 2), source % (zshare // 2)
    even = device % rows_py * (points // rows_py) + device // rows_py * zshare + 2 * within
    to_modes = np.concatenate([basis[even].T, basis[even + 1].T], 0)
    from_modes = np.concatenate([basis[even], basis[even + 1]], 0)
    return dict(
        forward=jnp.stack([jnp.asarray(h) for h in two_halves(forward)]),
        y_in=halves_stack(basis.T, 0),
        y_out=halves_stack(basis, 0),
        y_slope=halves_stack(derive.T, 0),
        z_in=halves_stack(to_modes, 1),
        z_out=halves_stack(from_modes, 0),
        spread=jnp.asarray(spread.astype(np.float32).astype(BF)),
    )


def slope_tables(points, rows_py, groups):
    derive = derivative_matrix(points)
    pairs = np.arange(points // 2)
    zblock = points // rows_py
    own = []
    for py in range(rows_py):
        order = np.concatenate([np.arange(zblock) + q * zblock for q in [py] + [q for q in range(rows_py) if q != py]])
        mine = np.arange(zblock) + py * zblock
        parts = []
        for out_parity in range(2):
            for in_parity in range(2):
                parts.append(derive[np.ix_(order[in_parity::2], mine[out_parity::2])].T)
        own.append(np.concatenate(parts, 0))
    stacked = np.stack(own)
    return np.concatenate([np.asarray(h) for h in two_halves(stacked)], 2)


def final_tables(points):
    basis, _ = real_basis(points)
    derive = derivative_matrix(points)
    out = np.zeros((2, 2 * LANES, 2, 2 * LANES))
    for parity in range(2):
        modes = np.arange(points)
        row = np.where(modes < LANES, modes, parity * HALF + modes)
        out[parity, row, 0, :points] = basis.T
        out[parity, row, 1, :points] = basis.T @ derive
    high, low = two_halves(out)
    both = np.stack([np.asarray(high), np.asarray(low)], 0)
    return jnp.asarray(both.transpose(1, 3, 0, 2, 4))


def dotf(left, right):
    return jnp.dot(left, right, preferred_element_type=F32)


def split(value):
    high = value.astype(BF)
    return high, (value - high.astype(F32)).astype(BF)


def chain_kernel(
    dims, rho, forward, y_in, y_out, y_slope, z_in, z_out, spread, slope,
    xs, gy, gz, h,
    others, c1s, c1, c2s, c2, c3s, c3, c4s, c4, gin, gs, wide, deep, sends, recvs,
):
    points, rows_px, rows_py, groups = dims
    yblock = points // rows_px
    zpairs = points // (rows_py * groups) // 2
    pieces = groups * rows_py
    kyblock = points // pieces
    rows = zpairs * yblock
    short = zpairs * kyblock
    band, px, py = lax.axis_index("band"), lax.axis_index("px"), lax.axis_index("py")
    me = band * rows_py + py
    px_peers = [lax.rem(px + s, rows_px) for s in range(1, rows_px)]
    zy_peers = [
        (lax.rem(band + b, groups), lax.rem(py + q, rows_py))
        for b in range(groups) for q in range(rows_py) if b or q
    ]
    barrier = pltpu.get_barrier_semaphore()
    for peer in px_peers:
        pl.semaphore_signal(barrier, inc=1, device_id=(band, peer, py), device_id_type=pl.DeviceIdType.MESH)
    for peer_band, peer_py in zy_peers:
        pl.semaphore_signal(barrier, inc=1, device_id=(peer_band, px, peer_py), device_id_type=pl.DeviceIdType.MESH)
    pl.semaphore_wait(barrier, len(px_peers) + len(zy_peers))
    used = []

    def send(src, dst, device):
        copy = pltpu.make_async_remote_copy(
            src_ref=src, dst_ref=dst, send_sem=sends.at[len(used)], recv_sem=recvs.at[len(used)],
            device_id=device, device_id_type=pl.DeviceIdType.MESH,
        )
        used.append(copy)
        copy.start()
        return copy

    def to_px(src, dst):
        return [send(src.at[peer], dst.at[px], (band, peer, py)) for peer in px_peers]

    def to_zy(src, dst):
        return [
            send(src.at[b * rows_py + q], dst.at[me], (b, px, q)) for b, q in zy_peers
        ]

    def arrived(copies):
        for copy in copies:
            copy.wait_recv()

    right, left = lax.rem(band + 1, groups), lax.rem(band + groups - 1, groups)

    def to_band(field, slot, target):
        return send(field.at[slot], field.at[slot], (target, px, py))

    def to_other(slot):
        return send(xs.at[slot], others.at[slot], (band, px, lax.rem(py + 1, rows_py)))

    step = 2 * yblock

    @pl.loop(0, rows // step)
    def _(i):
        at = pl.ds(pl.multiple_of(i * step, step), step)
        out = None
        for parity in range(2):
            high, low = split(rho[parity, at, :])
            part = dotf(high, forward[0, parity]) + dotf(low, forward[0, parity]) + dotf(high, forward[1, parity])
            out = part if out is None else out + part
        xs[band, at, :] = out[:, : 3 * LANES].astype(BF)
        for p in range(rows_px):
            c1s[p, at, :] = out[:, (3 + p) * LANES : (4 + p) * LANES].astype(BF)

    first = to_px(c1s, c1)
    ring_right = to_band(xs, band, right)
    across = [to_other(band)]
    c1[px] = c1s[px]
    arrived(first)

    @pl.loop(0, zpairs // 2)
    def _(i):
        found = []
        for k in range(2):
            at = pl.ds(pl.multiple_of((2 * i + k) * yblock, yblock), yblock)
            out = dotf(y_in[...], jnp.concatenate([c1[p, at, :] for p in range(rows_px)], 0))
            found.append(out[:points] + out[points:])
        at = pl.ds(pl.multiple_of(i * 2 * kyblock, 2 * kyblock), 2 * kyblock)
        for d in range(pieces):
            cut = slice(d * kyblock, (d + 1) * kyblock)
            c2s[d, at, :] = jnp.concatenate([f[cut] for f in found], 0).astype(BF)

    second = to_zy(c2s, c2)
    c2[me] = c2s[me]
    ring_left = to_band(xs, band, left)
    ring_right.wait_recv()
    ring_far = to_band(xs, left, right)
    across.append(to_other(left))
    arrived(second)
    for d in range(pieces):
        wide[pl.ds(d * short, short), :] = c2[d].astype(F32)
    lane = lax.broadcasted_iota(jnp.int32, (points, 2 * LANES), 1) % LANES
    column = pieces * zpairs
    unit = 2.0 * math.pi / (points * SPACING)

    def frequency(index):
        return jnp.where(index > points // 2, index - points // 2, index)

    level = frequency(lax.broadcasted_iota(jnp.int32, (points, 2 * LANES), 0))
    across_x = frequency(lane + px * yblock)
    flat = (level * level + across_x * across_x).astype(F32)
    second_half = lax.broadcasted_iota(jnp.int32, (points, 2 * LANES), 1) >= LANES

    def swapped(value):
        return jnp.concatenate([pltpu.roll(value[:, k * LANES : (k + 1) * LANES], HALF, 1) for k in range(2)], 1)

    @pl.loop(0, kyblock // 2)
    def _(i):
        at = [pl.ds(2 * i + k, column, stride=kyblock) for k in range(2)]
        data = jnp.concatenate([wide[a, :] for a in at], 1).astype(BF)
        out = dotf(z_in[...], jnp.concatenate([data, data], 0))
        here = [frequency(me * kyblock + 2 * i + k) for k in range(2)]
        here = [(f * f).astype(F32) for f in here]
        squared = unit**2 * (flat + jnp.where(second_half, here[1], here[0]))
        factor = jnp.where(squared > 0, 4.0 * math.pi / jnp.where(squared > 0, squared, 1.0), 0.0)
        spectrum = (out[:points] + swapped(out[points:])) * factor
        spectrum = jnp.where(lane < HALF, spectrum, swapped(spectrum))
        high, low = split(spectrum)
        back = dotf(z_out[:points, :], high) + dotf(z_out[points:, :], high) + dotf(z_out[:points, :], low)
        back = jnp.where(lane[:column] < HALF, back[:column], back[column:])
        for k in range(2):
            wide[at[k], :] = back[:, k * LANES : (k + 1) * LANES]

    for d in range(pieces):
        c3s[d] = wide[pl.ds(d * short, short), :].astype(BF)
    third = to_zy(c3s, c3)
    c3[me] = c3s[me]
    ring_left.wait_recv()
    across.append(to_other(right))
    ring_far.wait_recv()
    far = lax.rem(band + 2, groups)
    across.append(to_other(far))
    outward = to_px(xs, gin)
    gin[px] = xs[px]
    arrived(third)
    for d in range(pieces):
        wide[pl.ds(d * short, short), :] = c3[d].astype(F32)

    @pl.loop(0, zpairs)
    def _(i):
        data = jnp.concatenate(
            [wide[pl.ds(pl.multiple_of(d * short + i * kyblock, 8), kyblock), :] for d in range(pieces)], 0
        ).astype(BF)
        out = dotf(y_out[...], data)
        out = out[:points] + out[points:]
        at = pl.ds(pl.multiple_of(i * yblock, yblock), yblock)
        for p in range(rows_px):
            c4s[p, at, :] = out[p * yblock : (p + 1) * yblock].astype(BF)

    fourth = to_px(c4s, c4)
    c4[px] = c4s[px]
    arrived(fourth)

    @pl.loop(0, rows // step)
    def _(i):
        at = pl.ds(pl.multiple_of(i * step, step), step)
        out = None
        for p in range(rows_px):
            part = dotf(c4[p, at, :], spread[p])
            out = part if out is None else out + part
        h[band, at, :] = out.astype(BF)

    h_right = to_band(h, band, right)
    h_left = to_band(h, band, left)
    arrived(outward)

    @pl.loop(0, zpairs)
    def _(i):
        at = pl.ds(pl.multiple_of(i * yblock, yblock), yblock)
        out = dotf(y_slope[...], jnp.concatenate([gin[p, at, :] for p in range(rows_px)], 0))
        out = out[:points] + out[points:]
        for p in range(rows_px):
            gs[p, at, :] = out[p * yblock : (p + 1) * yblock].astype(BF)

    homeward = to_px(gs, gy)
    gy[px] = gs[px]
    h_right.wait_recv()
    h_far = to_band(h, left, right)
    arrived(across)
    own_rows = groups * rows
    for b in range(groups):
        for t in range(3):
            cut = pl.ds(t * LANES, LANES)
            deep[t, pl.ds(b * rows, rows), :] = xs[b, :, cut].astype(F32)
            deep[t, pl.ds(own_rows + b * rows, rows), :] = others[b, :, cut].astype(F32)
    zlines = groups * zpairs
    tail = lax.broadcasted_iota(jnp.int32, (zlines, LANES), 1) < HALF

    @pl.loop(0, yblock // 2)
    def _(i):
        data = jnp.concatenate(
            [
                deep[t, pl.ds(2 * i + k, rows_py * zlines, stride=yblock), :]
                for k in range(2) for t in range(3)
            ],
            1,
        ).astype(BF)
        out = dotf(slope[py], jnp.concatenate([data, data], 0))
        parts = [out[q * zlines : (q + 1) * zlines] for q in range(4)]
        for k in range(2):
            first, middle, last = (slice((3 * k + t) * LANES, (3 * k + t + 1) * LANES) for t in range(3))
            at = pl.ds(2 * i + k, zlines, stride=yblock)
            even = parts[0][:, last] + pltpu.roll(parts[1][:, last], HALF, 1)
            odd = pltpu.roll(parts[2][:, last], HALF, 1) + parts[3][:, last]
            deep[0, at, :] = parts[0][:, first] + parts[1][:, middle]
            deep[1, at, :] = parts[2][:, first] + parts[3][:, middle]
            deep[2, at, :] = jnp.where(tail, even, odd)

    for b in range(groups):
        for t in range(3):
            gz[b, :, pl.ds(t * LANES, LANES)] = deep[t, pl.ds(b * rows, rows), :].astype(BF)
    h_left.wait_recv()
    h_far.wait_recv()
    arrived(homeward)
    for copy in used:
        copy.wait_send()


def run_chain(rho, slope, tables, dims):
    points, rows_px, rows_py, groups = dims
    yblock = points // rows_px
    zpairs = points // (rows_py * groups) // 2
    pieces = groups * rows_py
    kyblock = points // pieces
    rows, short = zpairs * yblock, zpairs * kyblock
    copies = 4 * (rows_px - 1) + 2 * (pieces - 1) + 3 + 3 + groups
    field = jax.ShapeDtypeStruct((groups, rows, 3 * LANES), BF)
    vmem = pl.BlockSpec(memory_space=pltpu.VMEM)
    lined = pltpu.VMEM((rows_px, rows, LANES), BF)
    cut = pltpu.VMEM((pieces, short, LANES), BF)
    names = ("forward", "y_in", "y_out", "y_slope", "z_in", "z_out", "spread")
    return pl.pallas_call(
        functools.partial(chain_kernel, dims),
        out_shape=[field] * 4,
        in_specs=[vmem] * (len(names) + 2),
        out_specs=[vmem] * 4,
        scratch_shapes=[
            pltpu.VMEM((groups, rows, 3 * LANES), BF),
            lined, lined, cut, cut, cut, cut, lined, lined,
            pltpu.VMEM((rows_px, rows, 3 * LANES), BF),
            pltpu.VMEM((rows_px, rows, 3 * LANES), BF),
            pltpu.VMEM((pieces * short, LANES), F32),
            pltpu.VMEM((3, rows_py * groups * rows, LANES), F32),
            pltpu.SemaphoreType.DMA((copies,)),
            pltpu.SemaphoreType.DMA((copies,)),
        ],
        compiler_params=pltpu.CompilerParams(
            collective_id=1, has_side_effects=True, vmem_limit_bytes=60 << 20
        ),
    )(rho, *[tables[n] for n in names], slope)


def final_kernel(dims, shift, xs, gy, gz, h, table, potential, gradient):
    points, yblock, pairs = dims
    for parity in range(2):
        first = slice(parity * LANES, (parity + 1) * LANES)

        def natural(ref):
            value = ref[...]
            return jnp.concatenate([value[:, first], value[:, 2 * LANES :]], 1)

        def spatial(value, kind):
            out = dotf(value, table[parity, kind, 0]) + dotf(value, table[parity, kind, 1])
            return out[:, :points]

        lines = natural(xs)
        out = spatial(jnp.concatenate([lines, natural(gy), natural(gz), natural(h)], 0), 0)
        grad_x = spatial(lines, 1)
        n = pairs * yblock
        density, grad_y, grad_z, hartree = (out[k * n : (k + 1) * n] for k in range(4))
        density = jnp.maximum(density + shift[0:1, 0:1], CORE_LEAST)
        cube_root = jnp.exp(jnp.log(density) * (1.0 / 3.0))
        four_thirds = density * cube_root
        grad_square = grad_x * grad_x + grad_y * grad_y + grad_z * grad_z
        scale = (PBE_MU / (PBE_KAPPA * REDUCED_SCALE)) * grad_square
        inverse = 1.0 / (four_thirds * four_thirds + scale)
        ratio = four_thirds * four_thirds * inverse
        steep = scale * inverse
        part = (4.0 / 3.0) * (1.0 + PBE_KAPPA - PBE_KAPPA * ratio) - (8.0 / 3.0) * PBE_KAPPA * steep * ratio
        value = hartree - SLATER_COEF * cube_root * part
        for k in range(pairs):
            cut = slice(k * yblock, (k + 1) * yblock)
            potential[2 * k + parity] = value[cut]
            gradient[0, 2 * k + parity] = grad_x[cut]
            gradient[1, 2 * k + parity] = grad_y[cut]
            gradient[2, 2 * k + parity] = grad_z[cut]


def run_final(xs, gy, gz, h, shift, points, yblock):
    groups, rows, _ = xs.shape
    pairs = 2
    steps = groups * rows // (pairs * yblock)
    zblock = steps * 2 * pairs
    table = final_tables(points)
    flat = pl.BlockSpec((pairs * yblock, 3 * LANES), lambda i: (i, 0))
    return pl.pallas_call(
        functools.partial(final_kernel, (points, yblock, pairs)),
        grid=(steps,),
        out_shape=[
            jax.ShapeDtypeStruct((zblock, yblock, points), F32),
            jax.ShapeDtypeStruct((3, zblock, yblock, points), F32),
        ],
        in_specs=[pl.BlockSpec((8, LANES), lambda i: (0, 0))]
        + [flat] * 4
        + [pl.BlockSpec(table.shape, lambda i: (0, 0, 0, 0, 0))],
        out_specs=[
            pl.BlockSpec((2 * pairs, yblock, points), lambda i: (i, 0, 0)),
            pl.BlockSpec((3, 2 * pairs, yblock, points), lambda i: (0, i, 0, 0)),
        ],
    )(shift, *[f.reshape(groups * rows, 3 * LANES) for f in (xs, gy, gz, h)], table)


def column_tables(points, rows_px, rows_py, groups):
    inverse = inverse_table(points)
    pieces = groups * rows_py
    zshare = points // pieces
    yblock = points // rows_px
    doubled = 2 * points
    z_order = inverse.reshape(2, points, 2, rows_py, groups, zshare).transpose(0, 1, 4, 3, 2, 5)
    by_y = np.zeros((rows_px, 2, points, 2, HALF))
    by_y[:, :, :, :, :yblock] = inverse.reshape(2, points, 2, rows_px, yblock).transpose(3, 0, 1, 2, 4)
    by_y = np.concatenate([np.asarray(h) for h in two_halves(by_y.reshape(rows_px, 2, points, LANES))], 3)
    by_x = np.stack([np.asarray(h) for h in two_halves(inverse[0].transpose(1, 2, 0))], 1)
    z_table = np.stack([np.asarray(h) for h in two_halves(z_order.reshape(doubled, doubled).T)])
    return jnp.asarray(z_table), jnp.asarray(by_y), jnp.asarray(by_x)


def column_kernel(
    dims, occupation, orbitals, z_table, places, sticks, every_place, notes, columns, note, middle, sends, recvs
):
    points, rows_px, rows_py, groups = dims
    band, px, py = lax.axis_index("band"), lax.axis_index("px"), lax.axis_index("py")
    me = band * rows_py + py
    px_peers = [(band, lax.rem(px + s, rows_px), py) for s in range(1, rows_px)]
    zy_peers = [
        (lax.rem(band + b, groups), px, lax.rem(py + q, rows_py))
        for b in range(groups) for q in range(rows_py) if b or q
    ]
    barrier = pltpu.get_barrier_semaphore()
    for peer in px_peers + zy_peers:
        pl.semaphore_signal(barrier, inc=1, device_id=peer, device_id_type=pl.DeviceIdType.MESH)
    coefficients = orbitals[0]
    contract = (((1,), (1,)), ((), ()))
    found = lax.dot_general(z_table[0], coefficients, contract, preferred_element_type=F32)
    found = found + lax.dot_general(z_table[1], coefficients, contract, preferred_element_type=F32)
    share = 2 * points // (groups * rows_py)
    for d in range(groups * rows_py):
        columns[d] = found[d * share : (d + 1) * share].astype(BF)
    wide = coefficients.astype(F32)
    load = occupation[0] * jnp.sum(wide * wide)
    lane = lax.broadcasted_iota(jnp.int32, (8, LANES), 1)
    note[...] = jnp.where(lane == 0, occupation[0], jnp.where(lane == 1, load, 0.0))
    pl.semaphore_wait(barrier, len(px_peers) + len(zy_peers))
    used = []

    def send(src, dst, device):
        copy = pltpu.make_async_remote_copy(
            src_ref=src, dst_ref=dst, send_sem=sends.at[len(used)], recv_sem=recvs.at[len(used)],
            device_id=device, device_id_type=pl.DeviceIdType.MESH,
        )
        used.append(copy)
        copy.start()

    for peer in zy_peers:
        send(columns.at[peer[0] * rows_py + peer[2]], middle.at[me], peer)
    for peer in zy_peers:
        send(note, notes.at[px, me], peer)
    first = len(used)
    for peer in px_peers:
        send(places, every_place.at[px], peer)
    middle[me] = columns[me]
    notes[px, me] = note[...]
    every_place[px] = places[...]
    for copy in used[:first]:
        copy.wait_recv()
    for peer in px_peers:
        send(middle, sticks.at[px], peer)
        send(notes.at[px], notes.at[px], peer)
    sticks[px] = middle[...]
    for copy in used[first:]:
        copy.wait_recv()
    for copy in used:
        copy.wait_send()


def run_columns(occupations, orbitals, z_table, places, dims):
    points, rows_px, rows_py, groups = dims
    pieces = groups * rows_py
    copies = 2 * (pieces - 1) + 3 * (rows_px - 1)
    share = (pieces, 2 * points // pieces, LANES)
    vmem = pl.BlockSpec(memory_space=pltpu.VMEM)
    return pl.pallas_call(
        functools.partial(column_kernel, dims),
        out_shape=[
            jax.ShapeDtypeStruct((rows_px,) + share, BF),
            jax.ShapeDtypeStruct((rows_px,) + places.shape, jnp.int32),
            jax.ShapeDtypeStruct((rows_px, pieces, 8, LANES), F32),
        ],
        in_specs=[pl.BlockSpec(memory_space=pltpu.SMEM)] + [vmem] * 3,
        out_specs=[vmem] * 3,
        scratch_shapes=[
            pltpu.VMEM(share, BF),
            pltpu.VMEM((8, LANES), F32),
            pltpu.VMEM(share, BF),
            pltpu.SemaphoreType.DMA((copies,)),
            pltpu.SemaphoreType.DMA((copies,)),
        ],
        compiler_params=pltpu.CompilerParams(collective_id=2, has_side_effects=True),
    )(occupations, orbitals, z_table, places)


def density_kernel(dims, notes, sticks, places, by_y, by_x, core, rho, shift, wide, planes, held, sem):
    points, rows_px, rows_py, groups = dims
    xblock = yblock = points // rows_px
    zshare = points // (rows_py * groups)
    band, px = lax.axis_index("band"), lax.axis_index("px")
    fetch = pltpu.make_async_copy(core.at[pl.ds(band * zshare, zshare)], held, sem)
    fetch.start()
    mean = CORE_TYPICAL
    for p in range(rows_px):
        for d in range(groups * rows_py):
            mean = mean + notes[p, d, :, 1:2]
    shift[...] = jnp.broadcast_to(mean, (8, LANES))
    mean = mean[0:1]
    weights = [notes[0, b * rows_py, 0:1, 0:1] for b in range(groups)]
    count = 8
    lines = groups * zshare
    sticks_px = rows_py * LANES

    @pl.loop(0, rows_px)
    def _(p):
        wide[...] = sticks[p].astype(F32)
        spots = places[p]
        at_y = lax.broadcasted_iota(jnp.int32, (points, sticks_px), 0) == spots[1:2, :]
        one_hot = at_y.astype(F32).astype(BF)
        table = jnp.concatenate(
            [
                lax.dot_general(one_hot, by_y[px, i], (((0,), (0,)), ((), ())), preferred_element_type=F32)
                for i in range(2)
            ],
            0,
        ).astype(BF)
        at_x = lax.broadcasted_iota(jnp.int32, (xblock, sticks_px), 0) == spots[0:1, :] - p * xblock
        mask = at_x.astype(F32)

        @pl.loop(0, lines // count)
        def _(c):
            b = c // (zshare // count)
            z = (c % (zshare // count)) * count
            blocks = []
            for k in range(count):
                tiles = [
                    mask[:, q * LANES : (q + 1) * LANES]
                    * wide[b * rows_py + q, pl.ds(i * zshare + z + k, 1), :]
                    for i in range(2) for q in range(rows_py)
                ]
                blocks.append(jnp.concatenate(tiles, 1))
            out = dotf(jnp.concatenate(blocks, 0).astype(BF), table)
            out = (out[:, :LANES] + out[:, LANES:]).astype(BF)
            for k in range(count):
                planes[c * count + k, pl.ds(pl.multiple_of(p * xblock, xblock), xblock), :] = out[
                    k * xblock : (k + 1) * xblock
                ]

    fetch.wait()
    lane = lax.broadcasted_iota(jnp.int32, (points, LANES), 1)
    sign = jnp.where(lane < HALF, -1.0, 1.0)

    @pl.loop(0, zshare // 2)
    def _(i):
        total = [None, None]
        for b in range(groups):
            both = jnp.concatenate([planes[b * zshare + 2 * i + k] for k in range(2)], 1)
            cosine = dotf(by_x[0, 0], both) + dotf(by_x[0, 1], both)
            sine = dotf(by_x[1, 0], both) + dotf(by_x[1, 1], both)
            for k in range(2):
                cut = slice(k * LANES, (k + 1) * LANES)
                value = cosine[:, cut] + sign * pltpu.roll(sine[:, cut], HALF, 1)
                value = weights[b] * (value * value)
                total[k] = value if b == 0 else total[k] + value
        for k in range(2):
            density = total[k] + pltpu.roll(total[k], HALF, 1)
            rho[k, pl.ds(pl.multiple_of(i * yblock, yblock), yblock), :] = (
                density.T[:yblock] + (held[2 * i + k] - mean)
            )


def run_density(notes, sticks, places, core, by_y, by_x, dims):
    points, rows_px, rows_py, groups = dims
    zshare = points // (rows_py * groups)
    yblock = points // rows_px
    vmem = pl.BlockSpec(memory_space=pltpu.VMEM)
    return pl.pallas_call(
        functools.partial(density_kernel, dims),
        out_shape=[
            jax.ShapeDtypeStruct((2, zshare // 2 * yblock, points), F32),
            jax.ShapeDtypeStruct((8, LANES), F32),
        ],
        in_specs=[vmem] * 5 + [pl.BlockSpec(memory_space=pl.ANY)],
        out_specs=[vmem] * 2,
        scratch_shapes=[
            pltpu.VMEM(sticks.shape[1:], F32),
            pltpu.VMEM((groups * zshare, points, LANES), BF),
            pltpu.VMEM((zshare, yblock, points), F32),
            pltpu.SemaphoreType.DMA,
        ],
        compiler_params=pltpu.CompilerParams(vmem_limit_bytes=48 << 20),
    )(notes, sticks, places, by_y, by_x, core)


def fast_body(orbitals, occupations, stick_map, core_density):
    points = orbitals.shape[2] // 2
    rows_px, rows_py, groups = lax.axis_size("px"), lax.axis_size("py"), lax.axis_size("band")
    dims = (points, rows_px, rows_py, groups)
    yblock = xblock = points // rows_px
    kyblock = points // (rows_py * groups)
    z_table, by_y, by_x = column_tables(points, rows_px, rows_py, groups)
    sticks, places, notes = run_columns(occupations, orbitals, z_table, stick_map, dims)
    rho, shift = run_density(notes, sticks, places, core_density, by_y, by_x, dims)
    slope = jnp.asarray(slope_tables(points, rows_py, groups))
    tables = chain_tables(points, rows_px, rows_py, groups)
    xs, gy, gz, h = run_chain(rho, slope, tables, dims)
    return tuple(run_final(xs, gy, gz, h, shift, points, yblock))


def body(orbitals, occupations, stick_map, core_density):
    points = orbitals.shape[2] // 2
    rows_px = lax.axis_size("px")
    rows_py = lax.axis_size("py")
    groups = lax.axis_size("band")
    px_index = lax.axis_index("px")
    py_index = lax.axis_index("py")
    band_index = lax.axis_index("band")
    yblock = points // rows_px
    xblock = points // rows_px
    zblock = points // rows_py
    zshare = zblock // groups
    pieces = groups * rows_py
    kyblock = points // pieces

    density, _ = share_density(orbitals, occupations, stick_map, px_index)
    core = lax.dynamic_slice_in_dim(core_density, band_index * zshare, zshare, 0)
    rho = density + core.transpose(1, 0, 2)

    basis, freq = real_basis(points)
    derive = derivative_matrix(points).astype(np.float32)
    basis32 = basis.astype(np.float32)
    data = jnp.einsum("yzx,xpk->pyzk", rho, basis32.reshape(points, rows_px, xblock), precision=HIGH)
    grad_x = jnp.einsum("yzx,xw->zyw", rho, derive, precision=HIGH)
    data, grad_x_sent = lax.optimization_barrier((data, grad_x.astype(BF)))
    every_x = gathered(grad_x_sent)
    data = lax.all_to_all(data, "px", split_axis=0, concat_axis=0, tiled=True)
    data = data.reshape(points, zshare, xblock)
    high_basis, low_basis = two_halves(basis)
    x_basis = (high_basis.reshape(points, rows_px, xblock), low_basis.reshape(points, rows_px, xblock))
    lines_y = jnp.einsum("yzk,yw->wzk", data, derive, precision=HIGH).astype(BF)
    lines_y = lines_y.reshape(rows_px, yblock, zshare, xblock)
    lines_y = lax.all_to_all(lines_y, "px", split_axis=0, concat_axis=0, tiled=True)
    grad_y = dot2("pyzk,xpk->zyx", lines_y, x_basis)
    grad_y_sent = grad_y.astype(BF)
    modes = jnp.einsum("yzk,yj->jzk", data, basis32, precision=HIGH)
    modes = modes.reshape(pieces, kyblock, zshare, xblock)
    modes = lax.all_to_all(modes, ("band", "py"), split_axis=0, concat_axis=0, tiled=True)
    source = np.arange(points)
    device, within = source // zshare, source % zshare
    z_order = device % rows_py * zblock + device // rows_py * zshare + within
    z_basis = basis32[z_order].reshape(pieces, zshare, points)
    z_derive = derive[z_order][:, z_order].reshape(pieces, zshare, pieces, zshare)
    spectrum = jnp.einsum("djzk,dzm->mjk", modes, z_basis, precision=HIGH)
    unit = 2.0 * math.pi / (points * SPACING)
    all_q = jnp.asarray((freq * freq).astype(np.float32))
    q_col = lax.dynamic_slice_in_dim(all_q, (band_index * rows_py + py_index) * kyblock, kyblock)
    q_row = lax.dynamic_slice_in_dim(all_q, px_index * xblock, xblock)
    squared = unit**2 * (all_q[:, None, None] + q_col[None, :, None] + q_row[None, None, :])
    factor = jnp.where(squared > 0, 4.0 * math.pi / jnp.where(squared > 0, squared, 1.0), 0.0)
    spectrum = spectrum * factor
    back = jnp.stack(
        [
            jnp.einsum("mjk,dzm->djzk", spectrum, z_basis, precision=HIGH).astype(BF),
            jnp.einsum("ejwk,ewdz->djzk", modes, z_derive, precision=HIGH).astype(BF),
        ],
        1,
    )
    back, every_y, every_x = lax.optimization_barrier((back, grad_y_sent, every_x))
    every_y = gathered(every_y)
    back = lax.all_to_all(back, ("band", "py"), split_axis=0, concat_axis=0, tiled=True)
    y_basis = (high_basis.reshape(points, pieces, kyblock), low_basis.reshape(points, pieces, kyblock))
    lines = dot2("dfjzk,ydj->fyzk", back, y_basis)
    lines = lines.astype(BF).reshape(2, rows_px, yblock, zshare, xblock)
    lines = lax.all_to_all(lines, "px", split_axis=1, concat_axis=1, tiled=True)
    fields = dot2("fpyzk,xpk->fzyx", lines, x_basis)
    every_z = gathered(fields[1])
    potential = exchange_part(rho.transpose(1, 0, 2), fields[0], grad_x, grad_y, fields[1])
    every_potential = gathered(potential)
    gradient = jnp.stack([every_x.astype(F32), every_y.astype(F32), every_z.astype(F32)])
    return (every_potential.astype(F32), gradient)


def solution(mesh):
    def step(orbitals, occupations, stick_map, core_density):
        points = orbitals.shape[2] // 2
        block = points // mesh.shape["px"]
        share = points // (mesh.shape["py"] * mesh.shape["band"])
        fits = (
            points == LANES + HALF and block <= HALF and block % 16 == 0 and share % 8 == 0
            and orbitals.shape[:2] == (1, LANES)
            and mesh.shape["py"] == 2 and mesh.shape["band"] == 4
        )
        return (fast_body if fits else body)(orbitals, occupations, stick_map, core_density)

    return jax.shard_map(
        step,
        mesh=mesh,
        in_specs=(P("band", ("px", "py"), None), P("band"), P(None, "px"), P("py", "px", None)),
        out_specs=(P("py", "px", None), P(None, "py", "px", None)),
        check_vma=False,
    )
```

```python
import functools
import math

import jax
import jax.numpy as jnp
import numpy as np
from jax import lax
from jax.experimental import pallas as pl
from jax.experimental.pallas import tpu as pltpu
from jax.experimental.layout import Layout, with_layout_constraint
from jax.sharding import PartitionSpec as P

SPACING = 0.25
PBE_KAPPA = 0.804
PBE_MU = 0.2195
SLATER_COEF = 0.75 * (3.0 / math.pi) ** (1.0 / 3.0)
REDUCED_SCALE = 4.0 * (3.0 * math.pi**2) ** (2.0 / 3.0)
BF = jnp.bfloat16
F32 = jnp.float32
HIGH = lax.Precision.HIGH
CORE_LEAST = 0.05
CORE_TYPICAL = 0.2
PAIRS = 12
COUNT = 24
CHUNKS = 3


def inverse_table(points):
    k = np.arange(points)
    angles = 2.0 * np.pi / points * (k[:, None] * k[None, :] % points)
    cosine, sine = np.cos(angles), np.sin(angles)
    return np.stack([np.stack([cosine, sine], 1), np.stack([-sine, cosine], 1)], 0)


def two_halves(table):
    high = table.astype(np.float32).astype(BF)
    low = (table - high.astype(np.float64)).astype(np.float32).astype(BF)
    return high, low


def dot2(spec, data, table):
    high, low = table
    first = jnp.einsum(spec, data, high, preferred_element_type=F32)
    return first + jnp.einsum(spec, data, low, preferred_element_type=F32)


def real_basis(points):
    pos = np.arange(points)
    freq = np.concatenate([np.arange(points // 2 + 1), np.arange(1, points // 2)])
    angle = 2.0 * np.pi / points * (pos[:, None] * freq[None, :] % points)
    basis = np.where(np.arange(points)[None, :] <= points // 2, np.cos(angle), np.sin(angle))
    scale = np.where((freq == 0) | (freq == points // 2), 1.0 / points, 2.0 / points)
    return basis * np.sqrt(scale), freq


def derivative_matrix(points):
    pos = np.arange(points)
    freq = np.arange(1, points // 2)
    unit = 2.0 * np.pi / (points * SPACING)
    lag = (pos[None, :] - pos[:, None]) % points
    values = np.zeros(points)
    for d in range(points):
        values[d] = np.sum(-2.0 * unit * freq * np.sin(2.0 * np.pi * (freq * d % points) / points)) / points
    return values[lag]


def exchange_part(density, hartree, grad_x, grad_y, grad_z):
    cube_root = jnp.cbrt(density)
    four_thirds = density * cube_root
    grad_square = grad_x * grad_x + grad_y * grad_y + grad_z * grad_z
    reduced = grad_square / (REDUCED_SCALE * four_thirds * four_thirds)
    denominator = 1.0 + PBE_MU * reduced / PBE_KAPPA
    enhance = 1.0 + PBE_KAPPA - PBE_KAPPA / denominator
    enhance_slope = PBE_MU / (denominator * denominator)
    return hartree - SLATER_COEF * cube_root * (
        4.0 / 3.0 * enhance - 8.0 / 3.0 * reduced * enhance_slope
    )


def share_density(orbitals, occupations, stick_map, px_index):
    bands_here, columns_here, doubled = orbitals.shape
    points = doubled // 2
    rows_px = lax.axis_size("px")
    rows_py = lax.axis_size("py")
    groups = lax.axis_size("band")
    xblock = points // rows_px
    yblock = points // rows_px
    pieces = groups * rows_py
    zshare = points // pieces
    sticks = columns_here * rows_py
    bands = groups * bands_here
    inverse = inverse_table(points)
    z_order = inverse.reshape(2, points, 2, rows_py, groups, zshare).transpose(0, 1, 4, 3, 2, 5)
    z_table = two_halves(z_order.reshape(doubled, pieces, 2 * zshare))
    columns = dot2("bsk,kdw->dbsw", orbitals, z_table).astype(BF)
    columns = lax.all_to_all(columns, ("band", "py"), split_axis=0, concat_axis=0, tiled=True)
    columns = lax.all_gather(columns, "px", axis=0, tiled=False)
    columns = columns.reshape(rows_px, groups, rows_py, bands_here, columns_here, 2, zshare)
    columns = columns.transpose(0, 2, 4, 5, 1, 3, 6).reshape(rows_px, sticks, 2, bands * zshare)
    places = lax.all_gather(stick_map, "px", axis=0, tiled=False)
    loads = (orbitals.astype(F32) ** 2).sum((1, 2))
    first = (px_index == 0) & (lax.axis_index("py") == 0)
    own = jnp.where(jnp.arange(groups)[:, None] == lax.axis_index("band"), occupations[None, :], 0.0).reshape(bands)
    totals = jnp.concatenate([jnp.where(first, own, 0.0), (occupations * loads).sum()[None]])
    totals = lax.psum(totals, ("band", "px", "py"))
    weights, mean = totals[:bands], totals[bands]
    y_hot = (places[:, 1, :, None] == jnp.arange(points, dtype=jnp.int32)).astype(BF)
    x_local = places[:, 0] - jnp.arange(rows_px, dtype=jnp.int32)[:, None] * xblock
    x_hot = x_local[:, :, None] == jnp.arange(xblock, dtype=jnp.int32)
    by_y = inverse.reshape(2, points, 2, rows_px, yblock).transpose(3, 1, 0, 4, 2)
    picked = [
        jnp.einsum(
            "psy,yiwo->psiwo",
            y_hot,
            lax.dynamic_index_in_dim(jnp.asarray(half), px_index, 0, keepdims=False),
            preferred_element_type=F32,
        ).astype(BF)
        for half in two_halves(by_y)
    ]
    x_table = two_halves(inverse.reshape(2, rows_px, xblock, 2, points).transpose(1, 0, 2, 3, 4))
    spread = jnp.where(x_hot[:, :, None, :, None], columns[:, :, :, None, :], jnp.zeros((), BF))
    plane = jnp.einsum("psiwo,psixz->pwoxz", picked[0], spread, preferred_element_type=F32)
    plane = plane + jnp.einsum("psiwo,psixz->pwoxz", picked[1], spread, preferred_element_type=F32)
    values = dot2("pwoxz,poxtk->wztk", plane.astype(BF), x_table)
    values = values.reshape(yblock, bands, zshare, 2, points)
    square = values[:, :, :, 0] * values[:, :, :, 0] + values[:, :, :, 1] * values[:, :, :, 1]
    return (weights[None, :, None, None] * square).sum(1), mean


def gathered(field):
    field = with_layout_constraint(field.astype(BF), Layout((0, 1, 2)))
    return lax.all_gather(field, "band", axis=0, tiled=True)


LANES = 128
HALF = 64


def halves_stack(table, axis):
    return jnp.asarray(np.concatenate([np.asarray(h) for h in two_halves(table)], axis))


def packed_lane(parity, mode):
    return np.where(mode < LANES, parity * LANES + mode, 2 * LANES + parity * HALF + mode - LANES)


def chain_tables(points, rows_px, rows_py, groups):
    basis, freq = real_basis(points)
    derive = derivative_matrix(points)
    xblock = points // rows_px
    zshare = points // (rows_py * groups)
    modes = np.arange(points)
    forward = np.zeros((2, points, 3 * LANES + rows_px * LANES))
    spread = np.zeros((rows_px, LANES, 3 * LANES))
    for parity in range(2):
        forward[parity][:, packed_lane(parity, modes)] = basis
        lane = modes // xblock * LANES + parity * HALF + modes % xblock
        forward[parity][:, 3 * LANES + lane] = basis
        spread[modes // xblock, parity * HALF + modes % xblock, packed_lane(parity, modes)] = 1.0
    source = np.arange(points // 2)
    device, within = source // (zshare // 2), source % (zshare // 2)
    even = device % rows_py * (points // rows_py) + device // rows_py * zshare + 2 * within
    to_modes = np.concatenate([basis[even].T, basis[even + 1].T], 0)
    from_modes = np.concatenate([basis[even], basis[even + 1]], 0)
    return dict(
        forward=jnp.stack([jnp.asarray(h) for h in two_halves(forward)]),
        y_in=halves_stack(basis.T, 0),
        y_out=halves_stack(basis, 0),
        y_slope=halves_stack(derive.T, 0),
        z_in=halves_stack(to_modes, 1),
        z_out=halves_stack(from_modes, 0),
        spread=jnp.asarray(spread.astype(np.float32).astype(BF)),
    )


def slope_tables(points, rows_py, groups):
    derive = derivative_matrix(points)
    pairs = np.arange(points // 2)
    zblock = points // rows_py
    own = []
    for py in range(rows_py):
        order = np.concatenate([np.arange(zblock) + q * zblock for q in [py] + [q for q in range(rows_py) if q != py]])
        mine = np.arange(zblock) + py * zblock
        parts = []
        for out_parity in range(2):
            for in_parity in range(2):
                parts.append(derive[np.ix_(order[in_parity::2], mine[out_parity::2])].T)
        own.append(np.concatenate(parts, 0))
    stacked = np.stack(own)
    return np.concatenate([np.asarray(h) for h in two_halves(stacked)], 2)


def final_tables(points):
    basis, _ = real_basis(points)
    derive = derivative_matrix(points)
    out = np.zeros((2, 2 * LANES, 2, 2 * LANES))
    for parity in range(2):
        modes = np.arange(points)
        row = np.where(modes < LANES, modes, parity * HALF + modes)
        out[parity, row, 0, :points] = basis.T
        out[parity, row, 1, :points] = basis.T @ derive
    high, low = two_halves(out)
    both = np.stack([np.asarray(high), np.asarray(low)], 0)
    return jnp.asarray(both.transpose(1, 3, 0, 2, 4))


def dotf(left, right):
    return jnp.dot(left, right, preferred_element_type=F32)


def split(value):
    high = value.astype(BF)
    return high, (value - high.astype(F32)).astype(BF)


def chain_kernel(
    dims, summed, rho, forward, y_in, y_out, y_slope, z_in, z_out, spread, slope,
    xs, gy, gz, h,
    others, c1s, c1, c2s, c2, c3s, c3, c4s, c4, gin, gs, wide, deep, sends, recvs, g_sends, g_recvs, b_sends, b_recvs,
):
    points, rows_px, rows_py, groups = dims
    yblock = points // rows_px
    zpairs = points // (rows_py * groups) // 2
    pieces = groups * rows_py
    kyblock = points // pieces
    rows = zpairs * yblock
    short = zpairs * kyblock
    band, px, py = lax.axis_index("band"), lax.axis_index("px"), lax.axis_index("py")
    me = band * rows_py + py
    px_peers = [lax.rem(px + s, rows_px) for s in range(1, rows_px)]
    zy_peers = [
        (lax.rem(band + b, groups), lax.rem(py + q, rows_py))
        for b in range(groups) for q in range(rows_py) if b or q
    ]
    used = []

    def send(src, dst, device):
        copy = pltpu.make_async_remote_copy(
            src_ref=src, dst_ref=dst, send_sem=sends.at[len(used)], recv_sem=recvs.at[len(used)],
            device_id=device, device_id_type=pl.DeviceIdType.MESH,
        )
        used.append(copy)
        copy.start()
        return copy

    def to_px(src, dst, cut):
        dst[px, cut] = src[px, cut]
        return [send(src.at[peer, cut], dst.at[px, cut], (band, peer, py)) for peer in px_peers]

    def to_zy(src, dst, cut):
        dst[me, cut] = src[me, cut]
        return [send(src.at[b * rows_py + q, cut], dst.at[me, cut], (b, px, q)) for b, q in zy_peers]

    def arrived(copies):
        for copy in copies:
            copy.wait_recv()

    right, left = lax.rem(band + 1, groups), lax.rem(band + groups - 1, groups)

    def to_band(field, slot, target, cut=pl.ds(0, rows)):
        return send(field.at[slot, cut], field.at[slot, cut], (target, px, py))

    def to_other(slot):
        return send(xs.at[slot], others.at[slot], (band, px, lax.rem(py + 1, rows_py)))

    step = zpairs // CHUNKS
    lined = [pl.ds(c * step * yblock, step * yblock) for c in range(CHUNKS)]
    short_cuts = [pl.ds(c * step * kyblock, step * kyblock) for c in range(CHUNKS)]
    first, second, third, fourth, ring_right = [], [], [], [], []
    h_right, h_left, h_far = [], [], []

    def to_modes_x(c):
        summed(c * step, (c + 1) * step)
        at = lined[c]
        out = None
        for parity in range(2):
            high, low = split(rho[parity, at, :])
            part = dotf(high, forward[0, parity]) + dotf(low, forward[0, parity]) + dotf(high, forward[1, parity])
            out = part if out is None else out + part
        xs[band, at, :] = out[:, : 3 * LANES].astype(BF)
        for p in range(rows_px):
            c1s[p, at, :] = out[:, (3 + p) * LANES : (4 + p) * LANES].astype(BF)
        first.append(to_px(c1s, c1, at))
        ring_right.append(to_band(xs, band, right, at))

    def to_modes_y(c):
        arrived(first[c])

        @pl.loop(c * step // 2, (c + 1) * step // 2)
        def _(i):
            found = []
            for k in range(2):
                at = pl.ds(pl.multiple_of((2 * i + k) * yblock, yblock), yblock)
                out = dotf(y_in[...], jnp.concatenate([c1[p, at, :] for p in range(rows_px)], 0))
                found.append(out[:points] + out[points:])
            at = pl.ds(pl.multiple_of(i * 2 * kyblock, 2 * kyblock), 2 * kyblock)
            for d in range(pieces):
                cut = slice(d * kyblock, (d + 1) * kyblock)
                c2s[d, at, :] = jnp.concatenate([f[cut] for f in found], 0).astype(BF)

        second.append(to_zy(c2s, c2, short_cuts[c]))

    for c in range(CHUNKS):
        to_modes_x(c)
        if c:
            to_modes_y(c - 1)
    to_modes_y(CHUNKS - 1)
    far = lax.rem(band + 2, groups)
    slots = [band, left, right, far]
    across = [to_other(band)]

    def outward(k, source):
        return pltpu.make_async_remote_copy(
            src_ref=xs.at[slots[k]], dst_ref=gin.at[source], send_sem=g_sends.at[k], recv_sem=g_recvs.at[source],
            device_id=(band, k, py), device_id_type=pl.DeviceIdType.MESH,
        )

    def spread_out(k):
        @pl.when(px != k)
        def _():
            outward(k, px).start()

        @pl.when(px == k)
        def _():
            gin[k] = xs[slots[k]]

    def slot_of(p):
        return jnp.where(p == 0, band, jnp.where(p == 1, left, jnp.where(p == 2, right, far)))

    def homeward(k, peer, owner):
        return pltpu.make_async_remote_copy(
            src_ref=gs.at[peer], dst_ref=gy.at[slot_of(owner)], send_sem=b_sends.at[k], recv_sem=b_recvs.at[owner],
            device_id=(band, peer, py), device_id_type=pl.DeviceIdType.MESH,
        )

    def slopes_along_y():
        for peer in px_peers:
            outward(0, peer).wait_recv()

        @pl.loop(0, zpairs)
        def _(i):
            at = pl.ds(pl.multiple_of(i * yblock, yblock), yblock)
            out = dotf(y_slope[...], jnp.concatenate([gin[p, at, :] for p in range(rows_px)], 0))
            out = out[:points] + out[points:]
            for p in range(rows_px):
                gs[p, at, :] = out[p * yblock : (p + 1) * yblock].astype(BF)

        for k, peer in enumerate(px_peers):
            homeward(k, peer, px).start()
        gy[slot_of(px)] = gs[px]

    spread_out(0)
    ring_left = to_band(xs, band, left)
    arrived(ring_right)
    across.append(to_other(left))
    spread_out(1)
    for copies in second:
        arrived(copies)
    for d in range(pieces):
        wide[pl.ds(d * short, short), :] = c2[d].astype(F32)
    lane = lax.broadcasted_iota(jnp.int32, (points, 2 * LANES), 1) % LANES
    column = pieces * zpairs
    unit = 2.0 * math.pi / (points * SPACING)

    def frequency(index):
        return jnp.where(index > points // 2, index - points // 2, index)

    level = frequency(lax.broadcasted_iota(jnp.int32, (points, 2 * LANES), 0))
    across_x = frequency(lane + px * yblock)
    flat = (level * level + across_x * across_x).astype(F32)
    second_half = lax.broadcasted_iota(jnp.int32, (points, 2 * LANES), 1) >= LANES

    def swapped(value):
        return jnp.concatenate([pltpu.roll(value[:, k * LANES : (k + 1) * LANES], HALF, 1) for k in range(2)], 1)

    @pl.loop(0, kyblock // 2)
    def _(i):
        at = [pl.ds(2 * i + k, column, stride=kyblock) for k in range(2)]
        data = jnp.concatenate([wide[a, :] for a in at], 1).astype(BF)
        out = dotf(z_in[...], jnp.concatenate([data, data], 0))
        here = [frequency(me * kyblock + 2 * i + k) for k in range(2)]
        here = [(f * f).astype(F32) for f in here]
        squared = unit**2 * (flat + jnp.where(second_half, here[1], here[0]))
        factor = jnp.where(squared > 0, 4.0 * math.pi / jnp.where(squared > 0, squared, 1.0), 0.0)
        spectrum = (out[:points] + swapped(out[points:])) * factor
        spectrum = jnp.where(lane < HALF, spectrum, swapped(spectrum))
        high, low = split(spectrum)
        back = dotf(z_out[:points, :], high) + dotf(z_out[points:, :], high) + dotf(z_out[:points, :], low)
        back = jnp.where(lane[:column] < HALF, back[:column], back[column:])
        for k in range(2):
            wide[at[k], :] = back[:, k * LANES : (k + 1) * LANES]

    for d in range(pieces):
        c3s[d] = wide[pl.ds(d * short, short), :].astype(BF)
    for c in range(CHUNKS):
        third.append(to_zy(c3s, c3, short_cuts[c]))
    ring_far = to_band(xs, left, right)
    ring_left.wait_recv()
    across.append(to_other(right))
    spread_out(2)
    pl.when(px < 2)(slopes_along_y)

    def from_modes_y(c):
        arrived(third[c])
        for d in range(pieces):
            wide[pl.ds(d * short + c * step * kyblock, step * kyblock), :] = c3[d, short_cuts[c], :].astype(F32)

        @pl.loop(c * step, (c + 1) * step)
        def _(i):
            data = jnp.concatenate(
                [wide[pl.ds(pl.multiple_of(d * short + i * kyblock, 8), kyblock), :] for d in range(pieces)], 0
            ).astype(BF)
            out = dotf(y_out[...], data)
            out = out[:points] + out[points:]
            at = pl.ds(pl.multiple_of(i * yblock, yblock), yblock)
            for p in range(rows_px):
                c4s[p, at, :] = out[p * yblock : (p + 1) * yblock].astype(BF)

        fourth.append(to_px(c4s, c4, lined[c]))

    def gathered_modes(c):
        arrived(fourth[c])
        at = lined[c]
        out = None
        for p in range(rows_px):
            part = dotf(c4[p, at, :], spread[p])
            out = part if out is None else out + part
        h[band, at, :] = out.astype(BF)
        h_right.append(to_band(h, band, right, at))
        h_left.append(to_band(h, band, left, at))

    for c in range(CHUNKS):
        from_modes_y(c)
        if c:
            gathered_modes(c - 1)
    gathered_modes(CHUNKS - 1)
    ring_far.wait_recv()
    across.append(to_other(far))
    spread_out(3)
    pl.when(px >= 2)(slopes_along_y)
    for c in range(CHUNKS):
        h_right[c].wait_recv()
        h_far.append(to_band(h, left, right, lined[c]))
    arrived(across)
    own_rows = groups * rows
    for b in range(groups):
        for t in range(3):
            cut = pl.ds(t * LANES, LANES)
            deep[t, pl.ds(b * rows, rows), :] = xs[b, :, cut].astype(F32)
            deep[t, pl.ds(own_rows + b * rows, rows), :] = others[b, :, cut].astype(F32)
    zlines = groups * zpairs
    tail = lax.broadcasted_iota(jnp.int32, (zlines, LANES), 1) < HALF

    @pl.loop(0, yblock // 2)
    def _(i):
        data = jnp.concatenate(
            [
                deep[t, pl.ds(2 * i + k, rows_py * zlines, stride=yblock), :]
                for k in range(2) for t in range(3)
            ],
            1,
        ).astype(BF)
        out = dotf(slope[py], jnp.concatenate([data, data], 0))
        parts = [out[q * zlines : (q + 1) * zlines] for q in range(4)]
        for k in range(2):
            first, middle, last = (slice((3 * k + t) * LANES, (3 * k + t + 1) * LANES) for t in range(3))
            at = pl.ds(2 * i + k, zlines, stride=yblock)
            even = parts[0][:, last] + pltpu.roll(parts[1][:, last], HALF, 1)
            odd = pltpu.roll(parts[2][:, last], HALF, 1) + parts[3][:, last]
            deep[0, at, :] = parts[0][:, first] + parts[1][:, middle]
            deep[1, at, :] = parts[2][:, first] + parts[3][:, middle]
            deep[2, at, :] = jnp.where(tail, even, odd)

    for b in range(groups):
        for t in range(3):
            gz[b, :, pl.ds(t * LANES, LANES)] = deep[t, pl.ds(b * rows, rows), :].astype(BF)
    arrived(h_left)
    arrived(h_far)
    for k, peer in enumerate(px_peers):
        homeward(k, px, peer).wait_recv()
        homeward(k, peer, px).wait_send()
    for k in range(rows_px):
        pl.when(px != k)(outward(k, px).wait_send)
    for copy in used:
        copy.wait_send()


def final_kernel(dims, shift, xs, gy, gz, h, table, potential, gradient):
    points, yblock, pairs = dims
    for parity in range(2):
        first = slice(parity * LANES, (parity + 1) * LANES)

        def natural(ref):
            value = ref[...]
            return jnp.concatenate([value[:, first], value[:, 2 * LANES :]], 1)

        def spatial(value, kind):
            out = dotf(value, table[parity, kind, 0]) + dotf(value, table[parity, kind, 1])
            return out[:, :points]

        lines = natural(xs)
        out = spatial(jnp.concatenate([lines, natural(gy), natural(gz), natural(h)], 0), 0)
        grad_x = spatial(lines, 1)
        n = pairs * yblock
        density, grad_y, grad_z, hartree = (out[k * n : (k + 1) * n] for k in range(4))
        density = jnp.maximum(density + shift[0:1, 0:1], CORE_LEAST)
        cube_root = jnp.exp(jnp.log(density) * (1.0 / 3.0))
        power = density * cube_root
        power = power * power
        grad_square = grad_x * grad_x + grad_y * grad_y + grad_z * grad_z
        ratio = power / (power + (PBE_MU / (PBE_KAPPA * REDUCED_SCALE)) * grad_square)
        part = 4.0 / 3.0 * (1.0 + PBE_KAPPA) - PBE_KAPPA * ratio * (4.0 - 8.0 / 3.0 * ratio)
        value = hartree - SLATER_COEF * cube_root * part
        for k in range(pairs):
            cut = slice(k * yblock, (k + 1) * yblock)
            potential[2 * k + parity] = value[cut]
            gradient[0, 2 * k + parity] = grad_x[cut]
            gradient[1, 2 * k + parity] = grad_y[cut]
            gradient[2, 2 * k + parity] = grad_z[cut]


def run_final(xs, gy, gz, h, shift, points, yblock):
    groups, rows, _ = xs.shape
    pairs = PAIRS
    steps = groups * rows // (pairs * yblock)
    zblock = steps * 2 * pairs
    table = final_tables(points)
    flat = pl.BlockSpec((pairs * yblock, 3 * LANES), lambda i: (i, 0))
    return pl.pallas_call(
        functools.partial(final_kernel, (points, yblock, pairs)),
        grid=(steps,),
        out_shape=[
            jax.ShapeDtypeStruct((zblock, yblock, points), F32),
            jax.ShapeDtypeStruct((3, zblock, yblock, points), F32),
        ],
        in_specs=[pl.BlockSpec((8, LANES), lambda i: (0, 0))]
        + [flat] * 4
        + [pl.BlockSpec(table.shape, lambda i: (0, 0, 0, 0, 0))],
        out_specs=[
            pl.BlockSpec((2 * pairs, yblock, points), lambda i: (i, 0, 0)),
            pl.BlockSpec((3, 2 * pairs, yblock, points), lambda i: (0, i, 0, 0)),
        ],
    )(shift, *[f.reshape(groups * rows, 3 * LANES) for f in (xs, gy, gz, h)], table)


def column_tables(points, rows_px, rows_py, groups):
    inverse = inverse_table(points)
    pieces = groups * rows_py
    zshare = points // pieces
    yblock = points // rows_px
    doubled = 2 * points
    z_order = inverse.reshape(2, points, 2, rows_py, groups, zshare).transpose(0, 1, 4, 3, 2, 5)
    by_y = np.zeros((rows_px, 2, points, 2, HALF))
    by_y[:, :, :, :, :yblock] = inverse.reshape(2, points, 2, rows_px, yblock).transpose(3, 0, 1, 2, 4)
    by_y = np.concatenate([np.asarray(h) for h in two_halves(by_y.reshape(rows_px, 2, points, LANES))], 3)
    by_x = np.concatenate([np.asarray(h) for h in two_halves(inverse[0].transpose(1, 2, 0).reshape(doubled, points))], 0)
    z_table = np.stack([np.asarray(h) for h in two_halves(z_order.reshape(doubled, doubled).T)])
    return jnp.asarray(z_table), jnp.asarray(by_y), jnp.asarray(by_x)


def column_kernel(
    dims, occupation, orbitals, z_table, places, sticks, every_place, notes, columns, note, middle, sends, recvs
):
    points, rows_px, rows_py, groups = dims
    band, px, py = lax.axis_index("band"), lax.axis_index("px"), lax.axis_index("py")
    me = band * rows_py + py
    px_peers = [(band, lax.rem(px + s, rows_px), py) for s in range(1, rows_px)]
    zy_peers = [
        (lax.rem(band + b, groups), px, lax.rem(py + q, rows_py))
        for b in range(groups) for q in range(rows_py) if b or q
    ]
    barrier = pltpu.get_barrier_semaphore()
    for peer in px_peers + zy_peers:
        pl.semaphore_signal(barrier, inc=1, device_id=peer, device_id_type=pl.DeviceIdType.MESH)
    coefficients = orbitals[0]
    contract = (((1,), (1,)), ((), ()))
    found = lax.dot_general(z_table[0], coefficients, contract, preferred_element_type=F32)
    found = found + lax.dot_general(z_table[1], coefficients, contract, preferred_element_type=F32)
    share = 2 * points // (groups * rows_py)
    for d in range(groups * rows_py):
        columns[d] = found[d * share : (d + 1) * share].astype(BF)
    wide = coefficients.astype(F32)
    load = occupation[0] * jnp.sum(wide * wide)
    lane = lax.broadcasted_iota(jnp.int32, (8, LANES), 1)
    note[...] = jnp.where(lane == 0, occupation[0], jnp.where(lane == 1, load, 0.0))
    pl.semaphore_wait(barrier, len(px_peers) + len(zy_peers))
    used = []

    def send(src, dst, device):
        copy = pltpu.make_async_remote_copy(
            src_ref=src, dst_ref=dst, send_sem=sends.at[len(used)], recv_sem=recvs.at[len(used)],
            device_id=device, device_id_type=pl.DeviceIdType.MESH,
        )
        used.append(copy)
        copy.start()

    for peer in zy_peers:
        send(columns.at[peer[0] * rows_py + peer[2]], middle.at[me], peer)
    for peer in zy_peers:
        send(note, notes.at[px, me], peer)
    first = len(used)
    for peer in px_peers:
        send(places, every_place.at[px], peer)
    middle[me] = columns[me]
    notes[px, me] = note[...]
    every_place[px] = places[...]
    for copy in used[:first]:
        copy.wait_recv()
    for peer in px_peers:
        send(middle, sticks.at[px], peer)
        send(notes.at[px], notes.at[px], peer)
    sticks[px] = middle[...]

    def settled():
        for copy in used[first:]:
            copy.wait_recv()

    def sent():
        for copy in used:
            copy.wait_send()

    return settled, sent


def density_kernel(dims, settled, notes, sticks, places, by_y, by_x, core, rho, shift, wide, planes, held, sem):
    points, rows_px, rows_py, groups = dims
    xblock = yblock = points // rows_px
    zshare = points // (rows_py * groups)
    band, px = lax.axis_index("band"), lax.axis_index("px")
    fetch = pltpu.make_async_copy(core.at[pl.ds(band * zshare, zshare)], held, sem)
    fetch.start()
    count = COUNT
    lines = groups * zshare
    sticks_px = rows_py * LANES

    def spread_along_y(p):
        wide[...] = sticks[p].astype(F32)
        spots = places[p]
        at_y = lax.broadcasted_iota(jnp.int32, (points, sticks_px), 0) == spots[1:2, :]
        one_hot = at_y.astype(F32).astype(BF)
        table = jnp.concatenate(
            [
                lax.dot_general(one_hot, by_y[px, i], (((0,), (0,)), ((), ())), preferred_element_type=F32)
                for i in range(2)
            ],
            0,
        ).astype(BF)
        at_x = lax.broadcasted_iota(jnp.int32, (xblock, sticks_px), 0) == spots[0:1, :] - p * xblock
        mask = at_x.astype(F32)

        @pl.loop(0, lines // count)
        def _(c):
            b = c // (zshare // count)
            z = (c % (zshare // count)) * count
            blocks = []
            for k in range(count):
                tiles = [
                    mask[:, q * LANES : (q + 1) * LANES]
                    * wide[b * rows_py + q, pl.ds(i * zshare + z + k, 1), :]
                    for i in range(2) for q in range(rows_py)
                ]
                blocks.append(jnp.concatenate(tiles, 1))
            out = dotf(jnp.concatenate(blocks, 0).astype(BF), table)
            out = (out[:, :LANES] + out[:, LANES:]).astype(BF)
            for k in range(count):
                planes[c * count + k, pl.ds(pl.multiple_of(p * xblock, xblock), xblock), :] = out[
                    k * xblock : (k + 1) * xblock
                ]

    spread_along_y(px)
    settled()

    @pl.loop(1, rows_px)
    def _(s):
        spread_along_y(lax.rem(px + s, rows_px))

    mean = CORE_TYPICAL
    for p in range(rows_px):
        for d in range(groups * rows_py):
            mean = mean + notes[p, d, :, 1:2]
    shift[...] = jnp.broadcast_to(mean, (8, LANES))
    mean = mean[0:1]
    weights = [notes[0, b * rows_py, 0:1, 0:1] for b in range(groups)]
    fetch.wait()
    lane = lax.broadcasted_iota(jnp.int32, (points, LANES), 1)
    sign = jnp.where(lane < HALF, -1.0, 1.0)

    def summed(start, stop):
        @pl.loop(start, stop)
        def _(i):
            total = [None, None]
            for b in range(groups):
                both = jnp.concatenate([planes[b * zshare + 2 * i + k] for k in range(2)], 1)
                out = dotf(by_x[...], both)
                out = out[: 2 * points] + out[2 * points :]
                cosine, sine = out[:points], out[points:]
                for k in range(2):
                    cut = slice(k * LANES, (k + 1) * LANES)
                    value = cosine[:, cut] + sign * pltpu.roll(sine[:, cut], HALF, 1)
                    value = weights[b] * (value * value)
                    total[k] = value if b == 0 else total[k] + value
            for k in range(2):
                density = total[k] + pltpu.roll(total[k], HALF, 1)
                rho[k, pl.ds(pl.multiple_of(i * yblock, yblock), yblock), :] = (
                    density.T[:yblock] + (held[2 * i + k] - mean)
                )

    return summed


COLUMN_INPUTS, DENSITY_INPUTS, CHAIN_INPUTS = 4, 3, 8


def whole_kernel(dims, counts, *refs):
    groups = [COLUMN_INPUTS, DENSITY_INPUTS, CHAIN_INPUTS, 5] + counts
    parts, at = [], 0
    for count in groups:
        parts.append(refs[at : at + count])
        at += count
    column_in, density_in, chain_in, out, shared, column_own, density_own, chain_own = parts
    sticks, places, notes, rho = shared
    fields, shift = out[:4], out[4]
    settled, sent = column_kernel(dims, *column_in, sticks, places, notes, *column_own)
    summed = density_kernel(dims, settled, notes, sticks, places, *density_in, rho, shift, *density_own)
    chain_kernel(dims, summed, rho, *chain_in, *fields, *chain_own)
    sent()


def run_whole(occupations, orbitals, stick_map, core, dims):
    points, rows_px, rows_py, groups = dims
    xblock = yblock = points // rows_px
    pieces = groups * rows_py
    kyblock = zshare = points // pieces
    zpairs = zshare // 2
    rows, short = zpairs * yblock, zpairs * kyblock
    z_table, by_y, by_x = column_tables(points, rows_px, rows_py, groups)
    tables = chain_tables(points, rows_px, rows_py, groups)
    names = ("forward", "y_in", "y_out", "y_slope", "z_in", "z_out", "spread")
    slope = jnp.asarray(slope_tables(points, rows_py, groups))
    share = (pieces, 2 * zshare, LANES)
    field = jax.ShapeDtypeStruct((groups, rows, 3 * LANES), BF)
    vmem = pl.BlockSpec(memory_space=pltpu.VMEM)
    lined = pltpu.VMEM((rows_px, rows, LANES), BF)
    cut = pltpu.VMEM((pieces, short, LANES), BF)
    dma = pltpu.SemaphoreType.DMA
    column_copies = 2 * (pieces - 1) + 3 * (rows_px - 1)
    chain_copies = CHUNKS * (2 * (rows_px - 1) + 2 * (pieces - 1) + 1 + 3) + 2 + groups
    shared = [
        pltpu.VMEM((rows_px,) + share, BF),
        pltpu.VMEM((rows_px,) + stick_map.shape, jnp.int32),
        pltpu.VMEM((rows_px, pieces, 8, LANES), F32),
        pltpu.VMEM((2, rows, points), F32),
    ]
    column_own = [
        pltpu.VMEM(share, BF),
        pltpu.VMEM((8, LANES), F32),
        pltpu.VMEM(share, BF),
        dma((column_copies,)),
        dma((column_copies,)),
    ]
    density_own = [
        pltpu.VMEM(share, F32),
        pltpu.VMEM((groups * zshare, points, LANES), BF),
        pltpu.VMEM((zshare, yblock, points), F32),
        dma,
    ]
    chain_own = [
        pltpu.VMEM((groups, rows, 3 * LANES), BF),
        lined, lined, cut, cut, cut, cut, lined, lined,
        pltpu.VMEM((rows_px, rows, 3 * LANES), BF),
        pltpu.VMEM((rows_px, rows, 3 * LANES), BF),
        pltpu.VMEM((pieces * short, LANES), F32),
        pltpu.VMEM((3, rows_py * groups * rows, LANES), F32),
        dma((chain_copies,)),
        dma((chain_copies,)),
        dma((rows_px,)),
        dma((rows_px,)),
        dma((rows_px - 1,)),
        dma((rows_px,)),
    ]
    counts = [len(part) for part in (shared, column_own, density_own, chain_own)]
    return pl.pallas_call(
        functools.partial(whole_kernel, dims, counts),
        out_shape=[field] * 4 + [jax.ShapeDtypeStruct((8, LANES), F32)],
        in_specs=[pl.BlockSpec(memory_space=pltpu.SMEM)]
        + [vmem] * 5
        + [pl.BlockSpec(memory_space=pl.ANY)]
        + [vmem] * 8,
        out_specs=[vmem] * 5,
        scratch_shapes=shared + column_own + density_own + chain_own,
        compiler_params=pltpu.CompilerParams(collective_id=1, has_side_effects=True, vmem_limit_bytes=60 << 20),
    )(occupations, orbitals, z_table, stick_map, by_y, by_x, core, *[tables[n] for n in names], slope)


def fast_body(orbitals, occupations, stick_map, core_density):
    points = orbitals.shape[2] // 2
    rows_px, rows_py, groups = lax.axis_size("px"), lax.axis_size("py"), lax.axis_size("band")
    dims = (points, rows_px, rows_py, groups)
    yblock = points // rows_px
    xs, gy, gz, h, shift = run_whole(occupations, orbitals, stick_map, core_density, dims)
    return tuple(run_final(xs, gy, gz, h, shift, points, yblock))


def body(orbitals, occupations, stick_map, core_density):
    points = orbitals.shape[2] // 2
    rows_px = lax.axis_size("px")
    rows_py = lax.axis_size("py")
    groups = lax.axis_size("band")
    px_index = lax.axis_index("px")
    py_index = lax.axis_index("py")
    band_index = lax.axis_index("band")
    yblock = points // rows_px
    xblock = points // rows_px
    zblock = points // rows_py
    zshare = zblock // groups
    pieces = groups * rows_py
    kyblock = points // pieces

    density, _ = share_density(orbitals, occupations, stick_map, px_index)
    core = lax.dynamic_slice_in_dim(core_density, band_index * zshare, zshare, 0)
    rho = density + core.transpose(1, 0, 2)

    basis, freq = real_basis(points)
    derive = derivative_matrix(points).astype(np.float32)
    basis32 = basis.astype(np.float32)
    data = jnp.einsum("yzx,xpk->pyzk", rho, basis32.reshape(points, rows_px, xblock), precision=HIGH)
    grad_x = jnp.einsum("yzx,xw->zyw", rho, derive, precision=HIGH)
    data, grad_x_sent = lax.optimization_barrier((data, grad_x.astype(BF)))
    every_x = gathered(grad_x_sent)
    data = lax.all_to_all(data, "px", split_axis=0, concat_axis=0, tiled=True)
    data = data.reshape(points, zshare, xblock)
    high_basis, low_basis = two_halves(basis)
    x_basis = (high_basis.reshape(points, rows_px, xblock), low_basis.reshape(points, rows_px, xblock))
    lines_y = jnp.einsum("yzk,yw->wzk", data, derive, precision=HIGH).astype(BF)
    lines_y = lines_y.reshape(rows_px, yblock, zshare, xblock)
    lines_y = lax.all_to_all(lines_y, "px", split_axis=0, concat_axis=0, tiled=True)
    grad_y = dot2("pyzk,xpk->zyx", lines_y, x_basis)
    grad_y_sent = grad_y.astype(BF)
    modes = jnp.einsum("yzk,yj->jzk", data, basis32, precision=HIGH)
    modes = modes.reshape(pieces, kyblock, zshare, xblock)
    modes = lax.all_to_all(modes, ("band", "py"), split_axis=0, concat_axis=0, tiled=True)
    source = np.arange(points)
    device, within = source // zshare, source % zshare
    z_order = device % rows_py * zblock + device // rows_py * zshare + within
    z_basis = basis32[z_order].reshape(pieces, zshare, points)
    z_derive = derive[z_order][:, z_order].reshape(pieces, zshare, pieces, zshare)
    spectrum = jnp.einsum("djzk,dzm->mjk", modes, z_basis, precision=HIGH)
    unit = 2.0 * math.pi / (points * SPACING)
    all_q = jnp.asarray((freq * freq).astype(np.float32))
    q_col = lax.dynamic_slice_in_dim(all_q, (band_index * rows_py + py_index) * kyblock, kyblock)
    q_row = lax.dynamic_slice_in_dim(all_q, px_index * xblock, xblock)
    squared = unit**2 * (all_q[:, None, None] + q_col[None, :, None] + q_row[None, None, :])
    factor = jnp.where(squared > 0, 4.0 * math.pi / jnp.where(squared > 0, squared, 1.0), 0.0)
    spectrum = spectrum * factor
    back = jnp.stack(
        [
            jnp.einsum("mjk,dzm->djzk", spectrum, z_basis, precision=HIGH).astype(BF),
            jnp.einsum("ejwk,ewdz->djzk", modes, z_derive, precision=HIGH).astype(BF),
        ],
        1,
    )
    back, every_y, every_x = lax.optimization_barrier((back, grad_y_sent, every_x))
    every_y = gathered(every_y)
    back = lax.all_to_all(back, ("band", "py"), split_axis=0, concat_axis=0, tiled=True)
    y_basis = (high_basis.reshape(points, pieces, kyblock), low_basis.reshape(points, pieces, kyblock))
    lines = dot2("dfjzk,ydj->fyzk", back, y_basis)
    lines = lines.astype(BF).reshape(2, rows_px, yblock, zshare, xblock)
    lines = lax.all_to_all(lines, "px", split_axis=1, concat_axis=1, tiled=True)
    fields = dot2("fpyzk,xpk->fzyx", lines, x_basis)
    every_z = gathered(fields[1])
    potential = exchange_part(rho.transpose(1, 0, 2), fields[0], grad_x, grad_y, fields[1])
    every_potential = gathered(potential)
    gradient = jnp.stack([every_x.astype(F32), every_y.astype(F32), every_z.astype(F32)])
    return (every_potential.astype(F32), gradient)


def solution(mesh):
    def step(orbitals, occupations, stick_map, core_density):
        points = orbitals.shape[2] // 2
        block = points // mesh.shape["px"]
        share = points // (mesh.shape["py"] * mesh.shape["band"])
        fits = (
            points == LANES + HALF and block <= HALF and block % 16 == 0 and share % 8 == 0
            and orbitals.shape[:2] == (1, LANES)
            and mesh.shape["py"] == 2 and mesh.shape["band"] == 4 and mesh.shape["px"] == 4
        )
        return (fast_body if fits else body)(orbitals, occupations, stick_map, core_density)

    return jax.shard_map(
        step,
        mesh=mesh,
        in_specs=(P("band", ("px", "py"), None), P("band"), P(None, "px"), P("py", "px", None)),
        out_specs=(P("py", "px", None), P(None, "py", "px", None)),
        check_vma=False,
    )
```

```python
import functools
import math

import jax
import jax.numpy as jnp
import numpy as np
from jax import lax
from jax.experimental import pallas as pl
from jax.experimental.pallas import tpu as pltpu
from jax.experimental.layout import Layout, with_layout_constraint
from jax.sharding import PartitionSpec as P

SPACING = 0.25
PBE_KAPPA = 0.804
PBE_MU = 0.2195
SLATER_COEF = 0.75 * (3.0 / math.pi) ** (1.0 / 3.0)
REDUCED_SCALE = 4.0 * (3.0 * math.pi**2) ** (2.0 / 3.0)
BF = jnp.bfloat16
F32 = jnp.float32
HIGH = lax.Precision.HIGH
CORE_LEAST = 0.05
CORE_TYPICAL = 0.2
PAIRS = 12
COUNT = 24
CHUNKS = 3


def inverse_table(points):
    k = np.arange(points)
    angles = 2.0 * np.pi / points * (k[:, None] * k[None, :] % points)
    cosine, sine = np.cos(angles), np.sin(angles)
    return np.stack([np.stack([cosine, sine], 1), np.stack([-sine, cosine], 1)], 0)


def two_halves(table):
    high = table.astype(np.float32).astype(BF)
    low = (table - high.astype(np.float64)).astype(np.float32).astype(BF)
    return high, low


def dot2(spec, data, table):
    high, low = table
    first = jnp.einsum(spec, data, high, preferred_element_type=F32)
    return first + jnp.einsum(spec, data, low, preferred_element_type=F32)


def real_basis(points):
    pos = np.arange(points)
    freq = np.concatenate([np.arange(points // 2 + 1), np.arange(1, points // 2)])
    angle = 2.0 * np.pi / points * (pos[:, None] * freq[None, :] % points)
    basis = np.where(np.arange(points)[None, :] <= points // 2, np.cos(angle), np.sin(angle))
    scale = np.where((freq == 0) | (freq == points // 2), 1.0 / points, 2.0 / points)
    return basis * np.sqrt(scale), freq


def derivative_matrix(points):
    pos = np.arange(points)
    freq = np.arange(1, points // 2)
    unit = 2.0 * np.pi / (points * SPACING)
    lag = (pos[None, :] - pos[:, None]) % points
    values = np.zeros(points)
    for d in range(points):
        values[d] = np.sum(-2.0 * unit * freq * np.sin(2.0 * np.pi * (freq * d % points) / points)) / points
    return values[lag]


def exchange_part(density, hartree, grad_x, grad_y, grad_z):
    cube_root = jnp.cbrt(density)
    four_thirds = density * cube_root
    grad_square = grad_x * grad_x + grad_y * grad_y + grad_z * grad_z
    reduced = grad_square / (REDUCED_SCALE * four_thirds * four_thirds)
    denominator = 1.0 + PBE_MU * reduced / PBE_KAPPA
    enhance = 1.0 + PBE_KAPPA - PBE_KAPPA / denominator
    enhance_slope = PBE_MU / (denominator * denominator)
    return hartree - SLATER_COEF * cube_root * (
        4.0 / 3.0 * enhance - 8.0 / 3.0 * reduced * enhance_slope
    )


def share_density(orbitals, occupations, stick_map, px_index):
    bands_here, columns_here, doubled = orbitals.shape
    points = doubled // 2
    rows_px = lax.axis_size("px")
    rows_py = lax.axis_size("py")
    groups = lax.axis_size("band")
    xblock = points // rows_px
    yblock = points // rows_px
    pieces = groups * rows_py
    zshare = points // pieces
    sticks = columns_here * rows_py
    bands = groups * bands_here
    inverse = inverse_table(points)
    z_order = inverse.reshape(2, points, 2, rows_py, groups, zshare).transpose(0, 1, 4, 3, 2, 5)
    z_table = two_halves(z_order.reshape(doubled, pieces, 2 * zshare))
    columns = dot2("bsk,kdw->dbsw", orbitals, z_table).astype(BF)
    columns = lax.all_to_all(columns, ("band", "py"), split_axis=0, concat_axis=0, tiled=True)
    columns = lax.all_gather(columns, "px", axis=0, tiled=False)
    columns = columns.reshape(rows_px, groups, rows_py, bands_here, columns_here, 2, zshare)
    columns = columns.transpose(0, 2, 4, 5, 1, 3, 6).reshape(rows_px, sticks, 2, bands * zshare)
    places = lax.all_gather(stick_map, "px", axis=0, tiled=False)
    loads = (orbitals.astype(F32) ** 2).sum((1, 2))
    first = (px_index == 0) & (lax.axis_index("py") == 0)
    own = jnp.where(jnp.arange(groups)[:, None] == lax.axis_index("band"), occupations[None, :], 0.0).reshape(bands)
    totals = jnp.concatenate([jnp.where(first, own, 0.0), (occupations * loads).sum()[None]])
    totals = lax.psum(totals, ("band", "px", "py"))
    weights, mean = totals[:bands], totals[bands]
    y_hot = (places[:, 1, :, None] == jnp.arange(points, dtype=jnp.int32)).astype(BF)
    x_local = places[:, 0] - jnp.arange(rows_px, dtype=jnp.int32)[:, None] * xblock
    x_hot = x_local[:, :, None] == jnp.arange(xblock, dtype=jnp.int32)
    by_y = inverse.reshape(2, points, 2, rows_px, yblock).transpose(3, 1, 0, 4, 2)
    picked = [
        jnp.einsum(
            "psy,yiwo->psiwo",
            y_hot,
            lax.dynamic_index_in_dim(jnp.asarray(half), px_index, 0, keepdims=False),
            preferred_element_type=F32,
        ).astype(BF)
        for half in two_halves(by_y)
    ]
    x_table = two_halves(inverse.reshape(2, rows_px, xblock, 2, points).transpose(1, 0, 2, 3, 4))
    spread = jnp.where(x_hot[:, :, None, :, None], columns[:, :, :, None, :], jnp.zeros((), BF))
    plane = jnp.einsum("psiwo,psixz->pwoxz", picked[0], spread, preferred_element_type=F32)
    plane = plane + jnp.einsum("psiwo,psixz->pwoxz", picked[1], spread, preferred_element_type=F32)
    values = dot2("pwoxz,poxtk->wztk", plane.astype(BF), x_table)
    values = values.reshape(yblock, bands, zshare, 2, points)
    square = values[:, :, :, 0] * values[:, :, :, 0] + values[:, :, :, 1] * values[:, :, :, 1]
    return (weights[None, :, None, None] * square).sum(1), mean


def gathered(field):
    field = with_layout_constraint(field.astype(BF), Layout((0, 1, 2)))
    return lax.all_gather(field, "band", axis=0, tiled=True)


LANES = 128
HALF = 64


def halves_stack(table, axis):
    return jnp.asarray(np.concatenate([np.asarray(h) for h in two_halves(table)], axis))


def packed_lane(parity, mode):
    return np.where(mode < LANES, parity * LANES + mode, 2 * LANES + parity * HALF + mode - LANES)


def chain_tables(points, rows_px, rows_py, groups):
    basis, freq = real_basis(points)
    derive = derivative_matrix(points)
    xblock = points // rows_px
    zshare = points // (rows_py * groups)
    modes = np.arange(points)
    forward = np.zeros((2, points, 3 * LANES + rows_px * LANES))
    spread = np.zeros((rows_px, LANES, 3 * LANES))
    for parity in range(2):
        forward[parity][:, packed_lane(parity, modes)] = basis
        lane = modes // xblock * LANES + parity * HALF + modes % xblock
        forward[parity][:, 3 * LANES + lane] = basis
        spread[modes // xblock, parity * HALF + modes % xblock, packed_lane(parity, modes)] = 1.0
    source = np.arange(points // 2)
    device, within = source // (zshare // 2), source % (zshare // 2)
    even = device % rows_py * (points // rows_py) + device // rows_py * zshare + 2 * within
    to_modes = np.concatenate([basis[even].T, basis[even + 1].T], 0)
    from_modes = np.concatenate([basis[even], basis[even + 1]], 0)
    return dict(
        forward=jnp.stack([jnp.asarray(h) for h in two_halves(forward)]),
        y_in=halves_stack(basis.T, 0),
        y_out=halves_stack(basis, 0),
        y_slope=halves_stack(derive.T, 0),
        z_in=halves_stack(to_modes, 1),
        z_out=halves_stack(from_modes, 0),
        spread=jnp.asarray(spread.astype(np.float32).astype(BF)),
    )


def slope_tables(points, rows_py, groups):
    derive = derivative_matrix(points)
    pairs = np.arange(points // 2)
    zblock = points // rows_py
    own = []
    for py in range(rows_py):
        order = np.concatenate([np.arange(zblock) + q * zblock for q in [py] + [q for q in range(rows_py) if q != py]])
        mine = np.arange(zblock) + py * zblock
        parts = []
        for out_parity in range(2):
            for in_parity in range(2):
                parts.append(derive[np.ix_(order[in_parity::2], mine[out_parity::2])].T)
        own.append(np.concatenate(parts, 0))
    stacked = np.stack(own)
    return np.concatenate([np.asarray(h) for h in two_halves(stacked)], 2)


def final_tables(points):
    basis, _ = real_basis(points)
    derive = derivative_matrix(points)
    out = np.zeros((2, 2 * LANES, 2, 2 * LANES))
    for parity in range(2):
        modes = np.arange(points)
        row = np.where(modes < LANES, modes, parity * HALF + modes)
        out[parity, row, 0, :points] = basis.T
        out[parity, row, 1, :points] = basis.T @ derive
    high, low = two_halves(out)
    both = np.stack([np.asarray(high), np.asarray(low)], 0)
    return jnp.asarray(both.transpose(1, 3, 0, 2, 4))


def dotf(left, right):
    return jnp.dot(left, right, preferred_element_type=F32)


def split(value):
    high = value.astype(BF)
    return high, (value - high.astype(F32)).astype(BF)


def chain_kernel(
    dims, summed, rho, forward, y_in, y_out, y_slope, z_in, z_out, spread, slope,
    xs, gy, gz, h,
    others, c1s, c1, c2s, c2, c3s, c3, c4s, c4, gin, gs, wide, deep, sends, recvs, g_sends, g_recvs, b_sends, b_recvs,
    o_sends, o_recvs, x_sends, x_recvs, h_sends, h_recvs,
):
    points, rows_px, rows_py, groups = dims
    yblock = points // rows_px
    zpairs = points // (rows_py * groups) // 2
    pieces = groups * rows_py
    kyblock = points // pieces
    rows = zpairs * yblock
    short = zpairs * kyblock
    band, px, py = lax.axis_index("band"), lax.axis_index("px"), lax.axis_index("py")
    me = band * rows_py + py
    px_peers = [lax.rem(px + s, rows_px) for s in range(1, rows_px)]
    zy_peers = [
        (lax.rem(band + b, groups), lax.rem(py + q, rows_py))
        for b in range(groups) for q in range(rows_py) if b or q
    ]
    used = []

    def send(src, dst, device):
        copy = pltpu.make_async_remote_copy(
            src_ref=src, dst_ref=dst, send_sem=sends.at[len(used)], recv_sem=recvs.at[len(used)],
            device_id=device, device_id_type=pl.DeviceIdType.MESH,
        )
        used.append(copy)
        copy.start()
        return copy

    def to_px(src, dst, cut):
        dst[px, cut] = src[px, cut]
        return [send(src.at[peer, cut], dst.at[px, cut], (band, peer, py)) for peer in px_peers]

    def to_zy(src, dst, cut):
        dst[me, cut] = src[me, cut]
        return [send(src.at[b * rows_py + q, cut], dst.at[me, cut], (b, px, q)) for b, q in zy_peers]

    def arrived(copies):
        for copy in copies:
            copy.wait_recv()

    def hop(field, out_sems, in_sems, sign, phase, c):
        slot = jnp.clip(band - sign * phase, 0, groups - 1)
        target = jnp.clip(band + sign, 0, groups - 1)
        return pltpu.make_async_remote_copy(
            src_ref=field.at[slot, lined[c]], dst_ref=field.at[slot, lined[c]],
            send_sem=out_sems.at[phase * 2 + (sign > 0), c], recv_sem=in_sems.at[slot, c],
            device_id=(target, px, py), device_id_type=pl.DeviceIdType.MESH,
        )

    def hops(phase):
        return [
            (1, (band >= phase) & (band < groups - 1)),
            (-1, (band + phase < groups) & (band > 0)),
        ]

    def launch(fields, phase, c):
        for sign, runs in hops(phase):
            pl.when(runs)(hop(*fields, sign, phase, c).start)

    def landed(fields, distance, c):
        for sign in (1, -1):
            slot = band - sign * distance

            @pl.when((slot >= 0) & (slot < groups))
            def _():
                pltpu.make_async_remote_copy(
                    src_ref=fields[0].at[0, lined[c]], dst_ref=fields[0].at[jnp.clip(slot, 0, groups - 1), lined[c]],
                    send_sem=fields[1].at[0, c], recv_sem=fields[2].at[jnp.clip(slot, 0, groups - 1), c],
                    device_id=(band, px, py), device_id_type=pl.DeviceIdType.MESH,
                ).wait_recv()

    def to_other(slot):
        return pltpu.make_async_remote_copy(
            src_ref=xs.at[slot], dst_ref=others.at[slot], send_sem=o_sends.at[slot], recv_sem=o_recvs.at[slot],
            device_id=(band, px, lax.rem(py + 1, rows_py)), device_id_type=pl.DeviceIdType.MESH,
        )

    x_line = (xs, x_sends, x_recvs)
    h_line = (h, h_sends, h_recvs)
    step = zpairs // CHUNKS
    lined = [pl.ds(c * step * yblock, step * yblock) for c in range(CHUNKS)]
    short_cuts = [pl.ds(c * step * kyblock, step * kyblock) for c in range(CHUNKS)]
    first, second, third, fourth = [], [], [], []

    def to_modes_x(c):
        summed(c * step, (c + 1) * step)
        at = lined[c]
        out = None
        for parity in range(2):
            high, low = split(rho[parity, at, :])
            part = dotf(high, forward[0, parity]) + dotf(low, forward[0, parity]) + dotf(high, forward[1, parity])
            out = part if out is None else out + part
        xs[band, at, :] = out[:, : 3 * LANES].astype(BF)
        for p in range(rows_px):
            c1s[p, at, :] = out[:, (3 + p) * LANES : (4 + p) * LANES].astype(BF)
        first.append(to_px(c1s, c1, at))
        launch(x_line, 0, c)

    def to_modes_y(c):
        arrived(first[c])

        @pl.loop(c * step // 2, (c + 1) * step // 2)
        def _(i):
            found = []
            for k in range(2):
                at = pl.ds(pl.multiple_of((2 * i + k) * yblock, yblock), yblock)
                out = dotf(y_in[...], jnp.concatenate([c1[p, at, :] for p in range(rows_px)], 0))
                found.append(out[:points] + out[points:])
            at = pl.ds(pl.multiple_of(i * 2 * kyblock, 2 * kyblock), 2 * kyblock)
            for d in range(pieces):
                cut = slice(d * kyblock, (d + 1) * kyblock)
                c2s[d, at, :] = jnp.concatenate([f[cut] for f in found], 0).astype(BF)

        second.append(to_zy(c2s, c2, short_cuts[c]))

    for c in range(CHUNKS):
        to_modes_x(c)
        if c:
            to_modes_y(c - 1)
    to_modes_y(CHUNKS - 1)

    def outward(slot, source, c):
        return pltpu.make_async_remote_copy(
            src_ref=xs.at[slot, lined[c]], dst_ref=gin.at[source, lined[c]],
            send_sem=g_sends.at[slot, c], recv_sem=g_recvs.at[source, c],
            device_id=(band, slot, py), device_id_type=pl.DeviceIdType.MESH,
        )

    def pass_on(slot, c):
        pl.when(px != slot)(lambda: outward(slot, px, c).start())

        @pl.when(px == slot)
        def _():
            gin[px, lined[c]] = xs[slot, lined[c]]

    def at_distance(distance, act):
        for sign in (1, -1):
            slot = band - sign * distance
            pl.when((slot >= 0) & (slot < groups))(lambda: act(jnp.clip(slot, 0, groups - 1)))

    def cross_over(slot):
        to_other(slot).start()

    def homeward(k, peer, owner, c):
        return pltpu.make_async_remote_copy(
            src_ref=gs.at[peer, lined[c]], dst_ref=gy.at[owner, lined[c]],
            send_sem=b_sends.at[k, c], recv_sem=b_recvs.at[owner, c],
            device_id=(band, peer, py), device_id_type=pl.DeviceIdType.MESH,
        )

    def slopes_along_y():
        for c in range(CHUNKS):
            for peer in px_peers:
                outward(0, peer, c).wait_recv()

            @pl.loop(c * step, (c + 1) * step)
            def _(i):
                at = pl.ds(pl.multiple_of(i * yblock, yblock), yblock)
                out = dotf(y_slope[...], jnp.concatenate([gin[p, at, :] for p in range(rows_px)], 0))
                out = out[:points] + out[points:]
                for p in range(rows_px):
                    gs[p, at, :] = out[p * yblock : (p + 1) * yblock].astype(BF)

            for k, peer in enumerate(px_peers):
                homeward(k, peer, px, c).start()
            gy[px, lined[c]] = gs[px, lined[c]]

    near = (px - band <= 1) & (band - px <= 1)
    for c in range(CHUNKS):
        pass_on(band, c)
    for c in range(CHUNKS):
        landed(x_line, 1, c)
        launch(x_line, 1, c)
        at_distance(1, functools.partial(pass_on, c=c))
    for copies in second:
        arrived(copies)
    for d in range(pieces):
        wide[pl.ds(d * short, short), :] = c2[d].astype(F32)
    lane = lax.broadcasted_iota(jnp.int32, (points, 2 * LANES), 1) % LANES
    column = pieces * zpairs
    unit = 2.0 * math.pi / (points * SPACING)

    def frequency(index):
        return jnp.where(index > points // 2, index - points // 2, index)

    level = frequency(lax.broadcasted_iota(jnp.int32, (points, 2 * LANES), 0))
    across_x = frequency(lane + px * yblock)
    flat = (level * level + across_x * across_x).astype(F32)
    second_half = lax.broadcasted_iota(jnp.int32, (points, 2 * LANES), 1) >= LANES

    def swapped(value):
        return jnp.concatenate([pltpu.roll(value[:, k * LANES : (k + 1) * LANES], HALF, 1) for k in range(2)], 1)

    @pl.loop(0, kyblock // 2)
    def _(i):
        at = [pl.ds(2 * i + k, column, stride=kyblock) for k in range(2)]
        data = jnp.concatenate([wide[a, :] for a in at], 1).astype(BF)
        out = dotf(z_in[...], jnp.concatenate([data, data], 0))
        here = [frequency(me * kyblock + 2 * i + k) for k in range(2)]
        here = [(f * f).astype(F32) for f in here]
        squared = unit**2 * (flat + jnp.where(second_half, here[1], here[0]))
        factor = jnp.where(squared > 0, 4.0 * math.pi / jnp.where(squared > 0, squared, 1.0), 0.0)
        spectrum = (out[:points] + swapped(out[points:])) * factor
        spectrum = jnp.where(lane < HALF, spectrum, swapped(spectrum))
        high, low = split(spectrum)
        back = dotf(z_out[:points, :], high) + dotf(z_out[points:, :], high) + dotf(z_out[:points, :], low)
        back = jnp.where(lane[:column] < HALF, back[:column], back[column:])
        for k in range(2):
            wide[at[k], :] = back[:, k * LANES : (k + 1) * LANES]

    for d in range(pieces):
        c3s[d] = wide[pl.ds(d * short, short), :].astype(BF)
    for c in range(CHUNKS):
        third.append(to_zy(c3s, c3, short_cuts[c]))
    for c in range(CHUNKS):
        landed(x_line, 2, c)
        launch(x_line, 2, c)
        at_distance(2, functools.partial(pass_on, c=c))
    cross_over(band)
    at_distance(1, cross_over)
    at_distance(2, cross_over)
    pl.when(near)(slopes_along_y)

    def from_modes_y(c):
        arrived(third[c])
        for d in range(pieces):
            wide[pl.ds(d * short + c * step * kyblock, step * kyblock), :] = c3[d, short_cuts[c], :].astype(F32)

        @pl.loop(c * step, (c + 1) * step)
        def _(i):
            data = jnp.concatenate(
                [wide[pl.ds(pl.multiple_of(d * short + i * kyblock, 8), kyblock), :] for d in range(pieces)], 0
            ).astype(BF)
            out = dotf(y_out[...], data)
            out = out[:points] + out[points:]
            at = pl.ds(pl.multiple_of(i * yblock, yblock), yblock)
            for p in range(rows_px):
                c4s[p, at, :] = out[p * yblock : (p + 1) * yblock].astype(BF)

        fourth.append(to_px(c4s, c4, lined[c]))

    def gathered_modes(c):
        arrived(fourth[c])
        at = lined[c]
        out = None
        for p in range(rows_px):
            part = dotf(c4[p, at, :], spread[p])
            out = part if out is None else out + part
        h[band, at, :] = out.astype(BF)
        launch(h_line, 0, c)

    for c in range(CHUNKS):
        from_modes_y(c)
        if c:
            gathered_modes(c - 1)
    gathered_modes(CHUNKS - 1)
    for c in range(CHUNKS):
        landed(h_line, 1, c)
        launch(h_line, 1, c)
    for c in range(CHUNKS):
        landed(x_line, 3, c)
        at_distance(3, functools.partial(pass_on, c=c))
    at_distance(3, cross_over)
    pl.when(jnp.logical_not(near))(slopes_along_y)
    for c in range(CHUNKS):
        landed(h_line, 2, c)
        launch(h_line, 2, c)
    for slot in range(groups):
        to_other(slot).wait_recv()
    own_rows = groups * rows
    for b in range(groups):
        for t in range(3):
            cut = pl.ds(t * LANES, LANES)
            deep[t, pl.ds(b * rows, rows), :] = xs[b, :, cut].astype(F32)
            deep[t, pl.ds(own_rows + b * rows, rows), :] = others[b, :, cut].astype(F32)
    zlines = groups * zpairs
    tail = lax.broadcasted_iota(jnp.int32, (zlines, LANES), 1) < HALF

    @pl.loop(0, yblock // 2)
    def _(i):
        data = jnp.concatenate(
            [
                deep[t, pl.ds(2 * i + k, rows_py * zlines, stride=yblock), :]
                for k in range(2) for t in range(3)
            ],
            1,
        ).astype(BF)
        out = dotf(slope[py], jnp.concatenate([data, data], 0))
        parts = [out[q * zlines : (q + 1) * zlines] for q in range(4)]
        for k in range(2):
            first, middle, last = (slice((3 * k + t) * LANES, (3 * k + t + 1) * LANES) for t in range(3))
            at = pl.ds(2 * i + k, zlines, stride=yblock)
            even = parts[0][:, last] + pltpu.roll(parts[1][:, last], HALF, 1)
            odd = pltpu.roll(parts[2][:, last], HALF, 1) + parts[3][:, last]
            deep[0, at, :] = parts[0][:, first] + parts[1][:, middle]
            deep[1, at, :] = parts[2][:, first] + parts[3][:, middle]
            deep[2, at, :] = jnp.where(tail, even, odd)

    for b in range(groups):
        for t in range(3):
            gz[b, :, pl.ds(t * LANES, LANES)] = deep[t, pl.ds(b * rows, rows), :].astype(BF)
    for c in range(CHUNKS):
        landed(h_line, 3, c)
    for k, peer in enumerate(px_peers):
        for c in range(CHUNKS):
            homeward(k, px, peer, c).wait_recv()
            homeward(k, peer, px, c).wait_send()
    for slot in range(groups):
        to_other(slot).wait_send()
        for c in range(CHUNKS):
            pl.when(px != slot)(outward(slot, px, c).wait_send)
    for line in (x_line, h_line):
        for phase in range(groups - 1):
            for sign, runs in hops(phase):
                for c in range(CHUNKS):
                    pl.when(runs)(hop(*line, sign, phase, c).wait_send)
    for copy in used:
        copy.wait_send()


def final_kernel(dims, shift, xs, gy, gz, h, table, potential, gradient):
    points, yblock, pairs = dims
    for parity in range(2):
        first = slice(parity * LANES, (parity + 1) * LANES)

        def natural(ref):
            value = ref[...]
            return jnp.concatenate([value[:, first], value[:, 2 * LANES :]], 1)

        def spatial(value, kind):
            out = dotf(value, table[parity, kind, 0]) + dotf(value, table[parity, kind, 1])
            return out[:, :points]

        lines = natural(xs)
        out = spatial(jnp.concatenate([lines, natural(gy), natural(gz), natural(h)], 0), 0)
        grad_x = spatial(lines, 1)
        n = pairs * yblock
        density, grad_y, grad_z, hartree = (out[k * n : (k + 1) * n] for k in range(4))
        density = jnp.maximum(density + shift[0:1, 0:1], CORE_LEAST)
        cube_root = jnp.exp(jnp.log(density) * (1.0 / 3.0))
        power = density * cube_root
        power = power * power
        grad_square = grad_x * grad_x + grad_y * grad_y + grad_z * grad_z
        ratio = power / (power + (PBE_MU / (PBE_KAPPA * REDUCED_SCALE)) * grad_square)
        part = 4.0 / 3.0 * (1.0 + PBE_KAPPA) - PBE_KAPPA * ratio * (4.0 - 8.0 / 3.0 * ratio)
        value = hartree - SLATER_COEF * cube_root * part
        for k in range(pairs):
            cut = slice(k * yblock, (k + 1) * yblock)
            potential[2 * k + parity] = value[cut]
            gradient[0, 2 * k + parity] = grad_x[cut]
            gradient[1, 2 * k + parity] = grad_y[cut]
            gradient[2, 2 * k + parity] = grad_z[cut]


def run_final(xs, gy, gz, h, shift, points, yblock):
    groups, rows, _ = xs.shape
    pairs = PAIRS
    steps = groups * rows // (pairs * yblock)
    zblock = steps * 2 * pairs
    table = final_tables(points)
    flat = pl.BlockSpec((pairs * yblock, 3 * LANES), lambda i: (i, 0))
    return pl.pallas_call(
        functools.partial(final_kernel, (points, yblock, pairs)),
        grid=(steps,),
        out_shape=[
            jax.ShapeDtypeStruct((zblock, yblock, points), F32),
            jax.ShapeDtypeStruct((3, zblock, yblock, points), F32),
        ],
        in_specs=[pl.BlockSpec((8, LANES), lambda i: (0, 0))]
        + [flat] * 4
        + [pl.BlockSpec(table.shape, lambda i: (0, 0, 0, 0, 0))],
        out_specs=[
            pl.BlockSpec((2 * pairs, yblock, points), lambda i: (i, 0, 0)),
            pl.BlockSpec((3, 2 * pairs, yblock, points), lambda i: (0, i, 0, 0)),
        ],
    )(shift, *[f.reshape(groups * rows, 3 * LANES) for f in (xs, gy, gz, h)], table)


def column_tables(points, rows_px, rows_py, groups):
    inverse = inverse_table(points)
    pieces = groups * rows_py
    zshare = points // pieces
    yblock = points // rows_px
    doubled = 2 * points
    z_order = inverse.reshape(2, points, 2, rows_py, groups, zshare).transpose(0, 1, 4, 3, 2, 5)
    by_y = np.zeros((rows_px, 2, points, 2, HALF))
    by_y[:, :, :, :, :yblock] = inverse.reshape(2, points, 2, rows_px, yblock).transpose(3, 0, 1, 2, 4)
    by_y = np.concatenate([np.asarray(h) for h in two_halves(by_y.reshape(rows_px, 2, points, LANES))], 3)
    by_x = np.concatenate([np.asarray(h) for h in two_halves(inverse[0].transpose(1, 2, 0).reshape(doubled, points))], 0)
    z_table = np.stack([np.asarray(h) for h in two_halves(z_order.reshape(doubled, doubled).T)])
    return jnp.asarray(z_table), jnp.asarray(by_y), jnp.asarray(by_x)


def column_kernel(
    dims, occupation, orbitals, z_table, places, sticks, every_place, notes, columns, note, middle, sends, recvs
):
    points, rows_px, rows_py, groups = dims
    band, px, py = lax.axis_index("band"), lax.axis_index("px"), lax.axis_index("py")
    me = band * rows_py + py
    px_peers = [(band, lax.rem(px + s, rows_px), py) for s in range(1, rows_px)]
    zy_peers = [
        (lax.rem(band + b, groups), px, lax.rem(py + q, rows_py))
        for b in range(groups) for q in range(rows_py) if b or q
    ]
    barrier = pltpu.get_barrier_semaphore()
    for peer in px_peers + zy_peers:
        pl.semaphore_signal(barrier, inc=1, device_id=peer, device_id_type=pl.DeviceIdType.MESH)
    coefficients = orbitals[0]
    contract = (((1,), (1,)), ((), ()))
    found = lax.dot_general(z_table[0], coefficients, contract, preferred_element_type=F32)
    found = found + lax.dot_general(z_table[1], coefficients, contract, preferred_element_type=F32)
    share = 2 * points // (groups * rows_py)
    for d in range(groups * rows_py):
        columns[d] = found[d * share : (d + 1) * share].astype(BF)
    wide = coefficients.astype(F32)
    load = occupation[0] * jnp.sum(wide * wide)
    lane = lax.broadcasted_iota(jnp.int32, (8, LANES), 1)
    note[...] = jnp.where(lane == 0, occupation[0], jnp.where(lane == 1, load, 0.0))
    pl.semaphore_wait(barrier, len(px_peers) + len(zy_peers))
    used = []

    def send(src, dst, device):
        copy = pltpu.make_async_remote_copy(
            src_ref=src, dst_ref=dst, send_sem=sends.at[len(used)], recv_sem=recvs.at[len(used)],
            device_id=device, device_id_type=pl.DeviceIdType.MESH,
        )
        used.append(copy)
        copy.start()

    for peer in zy_peers:
        send(columns.at[peer[0] * rows_py + peer[2]], middle.at[me], peer)
    for peer in zy_peers:
        send(note, notes.at[px, me], peer)
    first = len(used)
    for peer in px_peers:
        send(places, every_place.at[px], peer)
    middle[me] = columns[me]
    notes[px, me] = note[...]
    every_place[px] = places[...]
    for copy in used[:first]:
        copy.wait_recv()
    for peer in px_peers:
        send(middle, sticks.at[px], peer)
        send(notes.at[px], notes.at[px], peer)
    sticks[px] = middle[...]

    def settled():
        for copy in used[first:]:
            copy.wait_recv()

    def sent():
        for copy in used:
            copy.wait_send()

    return settled, sent


def density_kernel(dims, settled, notes, sticks, places, by_y, by_x, core, rho, shift, wide, planes, held, sem):
    points, rows_px, rows_py, groups = dims
    xblock = yblock = points // rows_px
    zshare = points // (rows_py * groups)
    band, px = lax.axis_index("band"), lax.axis_index("px")
    fetch = pltpu.make_async_copy(core.at[pl.ds(band * zshare, zshare)], held, sem)
    fetch.start()
    count = COUNT
    lines = groups * zshare
    sticks_px = rows_py * LANES

    def spread_along_y(p):
        wide[...] = sticks[p].astype(F32)
        spots = places[p]
        at_y = lax.broadcasted_iota(jnp.int32, (points, sticks_px), 0) == spots[1:2, :]
        one_hot = at_y.astype(F32).astype(BF)
        table = jnp.concatenate(
            [
                lax.dot_general(one_hot, by_y[px, i], (((0,), (0,)), ((), ())), preferred_element_type=F32)
                for i in range(2)
            ],
            0,
        ).astype(BF)
        at_x = lax.broadcasted_iota(jnp.int32, (xblock, sticks_px), 0) == spots[0:1, :] - p * xblock
        mask = at_x.astype(F32)

        @pl.loop(0, lines // count)
        def _(c):
            b = c // (zshare // count)
            z = (c % (zshare // count)) * count
            blocks = []
            for k in range(count):
                tiles = [
                    mask[:, q * LANES : (q + 1) * LANES]
                    * wide[b * rows_py + q, pl.ds(i * zshare + z + k, 1), :]
                    for i in range(2) for q in range(rows_py)
                ]
                blocks.append(jnp.concatenate(tiles, 1))
            out = dotf(jnp.concatenate(blocks, 0).astype(BF), table)
            out = (out[:, :LANES] + out[:, LANES:]).astype(BF)
            for k in range(count):
                planes[c * count + k, pl.ds(pl.multiple_of(p * xblock, xblock), xblock), :] = out[
                    k * xblock : (k + 1) * xblock
                ]

    spread_along_y(px)
    settled()

    @pl.loop(1, rows_px)
    def _(s):
        spread_along_y(lax.rem(px + s, rows_px))

    mean = CORE_TYPICAL
    for p in range(rows_px):
        for d in range(groups * rows_py):
            mean = mean + notes[p, d, :, 1:2]
    shift[...] = jnp.broadcast_to(mean, (8, LANES))
    mean = mean[0:1]
    weights = [notes[0, b * rows_py, 0:1, 0:1] for b in range(groups)]
    fetch.wait()
    lane = lax.broadcasted_iota(jnp.int32, (points, LANES), 1)
    sign = jnp.where(lane < HALF, -1.0, 1.0)

    def summed(start, stop):
        @pl.loop(start, stop)
        def _(i):
            total = [None, None]
            for b in range(groups):
                both = jnp.concatenate([planes[b * zshare + 2 * i + k] for k in range(2)], 1)
                out = dotf(by_x[...], both)
                out = out[: 2 * points] + out[2 * points :]
                cosine, sine = out[:points], out[points:]
                for k in range(2):
                    cut = slice(k * LANES, (k + 1) * LANES)
                    value = cosine[:, cut] + sign * pltpu.roll(sine[:, cut], HALF, 1)
                    value = weights[b] * (value * value)
                    total[k] = value if b == 0 else total[k] + value
            for k in range(2):
                density = total[k] + pltpu.roll(total[k], HALF, 1)
                rho[k, pl.ds(pl.multiple_of(i * yblock, yblock), yblock), :] = (
                    density.T[:yblock] + (held[2 * i + k] - mean)
                )

    return summed


COLUMN_INPUTS, DENSITY_INPUTS, CHAIN_INPUTS = 4, 3, 8


def whole_kernel(dims, counts, *refs):
    groups = [COLUMN_INPUTS, DENSITY_INPUTS, CHAIN_INPUTS, 5] + counts
    parts, at = [], 0
    for count in groups:
        parts.append(refs[at : at + count])
        at += count
    column_in, density_in, chain_in, out, shared, column_own, density_own, chain_own = parts
    sticks, places, notes, rho = shared
    fields, shift = out[:4], out[4]
    settled, sent = column_kernel(dims, *column_in, sticks, places, notes, *column_own)
    summed = density_kernel(dims, settled, notes, sticks, places, *density_in, rho, shift, *density_own)
    chain_kernel(dims, summed, rho, *chain_in, *fields, *chain_own)
    sent()


def run_whole(occupations, orbitals, stick_map, core, dims):
    points, rows_px, rows_py, groups = dims
    xblock = yblock = points // rows_px
    pieces = groups * rows_py
    kyblock = zshare = points // pieces
    zpairs = zshare // 2
    rows, short = zpairs * yblock, zpairs * kyblock
    z_table, by_y, by_x = column_tables(points, rows_px, rows_py, groups)
    tables = chain_tables(points, rows_px, rows_py, groups)
    names = ("forward", "y_in", "y_out", "y_slope", "z_in", "z_out", "spread")
    slope = jnp.asarray(slope_tables(points, rows_py, groups))
    share = (pieces, 2 * zshare, LANES)
    field = jax.ShapeDtypeStruct((groups, rows, 3 * LANES), BF)
    vmem = pl.BlockSpec(memory_space=pltpu.VMEM)
    lined = pltpu.VMEM((rows_px, rows, LANES), BF)
    cut = pltpu.VMEM((pieces, short, LANES), BF)
    dma = pltpu.SemaphoreType.DMA
    column_copies = 2 * (pieces - 1) + 3 * (rows_px - 1)
    chain_copies = CHUNKS * (2 * (rows_px - 1) + 2 * (pieces - 1))
    shared = [
        pltpu.VMEM((rows_px,) + share, BF),
        pltpu.VMEM((rows_px,) + stick_map.shape, jnp.int32),
        pltpu.VMEM((rows_px, pieces, 8, LANES), F32),
        pltpu.VMEM((2, rows, points), F32),
    ]
    column_own = [
        pltpu.VMEM(share, BF),
        pltpu.VMEM((8, LANES), F32),
        pltpu.VMEM(share, BF),
        dma((column_copies,)),
        dma((column_copies,)),
    ]
    density_own = [
        pltpu.VMEM(share, F32),
        pltpu.VMEM((groups * zshare, points, LANES), BF),
        pltpu.VMEM((zshare, yblock, points), F32),
        dma,
    ]
    chain_own = [
        pltpu.VMEM((groups, rows, 3 * LANES), BF),
        lined, lined, cut, cut, cut, cut, lined, lined,
        pltpu.VMEM((rows_px, rows, 3 * LANES), BF),
        pltpu.VMEM((rows_px, rows, 3 * LANES), BF),
        pltpu.VMEM((pieces * short, LANES), F32),
        pltpu.VMEM((3, rows_py * groups * rows, LANES), F32),
        dma((chain_copies,)),
        dma((chain_copies,)),
        dma((rows_px, CHUNKS)),
        dma((rows_px, CHUNKS)),
        dma((rows_px - 1, CHUNKS)),
        dma((rows_px, CHUNKS)),
        dma((groups,)),
        dma((groups,)),
    ] + [dma((2 * (groups - 1), CHUNKS)), dma((groups, CHUNKS))] * 2
    counts = [len(part) for part in (shared, column_own, density_own, chain_own)]
    return pl.pallas_call(
        functools.partial(whole_kernel, dims, counts),
        out_shape=[field] * 4 + [jax.ShapeDtypeStruct((8, LANES), F32)],
        in_specs=[pl.BlockSpec(memory_space=pltpu.SMEM)]
        + [vmem] * 5
        + [pl.BlockSpec(memory_space=pl.ANY)]
        + [vmem] * 8,
        out_specs=[vmem] * 5,
        scratch_shapes=shared + column_own + density_own + chain_own,
        compiler_params=pltpu.CompilerParams(collective_id=1, has_side_effects=True, vmem_limit_bytes=60 << 20),
    )(occupations, orbitals, z_table, stick_map, by_y, by_x, core, *[tables[n] for n in names], slope)


def fast_body(orbitals, occupations, stick_map, core_density):
    points = orbitals.shape[2] // 2
    rows_px, rows_py, groups = lax.axis_size("px"), lax.axis_size("py"), lax.axis_size("band")
    dims = (points, rows_px, rows_py, groups)
    yblock = points // rows_px
    xs, gy, gz, h, shift = run_whole(occupations, orbitals, stick_map, core_density, dims)
    return tuple(run_final(xs, gy, gz, h, shift, points, yblock))


def body(orbitals, occupations, stick_map, core_density):
    points = orbitals.shape[2] // 2
    rows_px = lax.axis_size("px")
    rows_py = lax.axis_size("py")
    groups = lax.axis_size("band")
    px_index = lax.axis_index("px")
    py_index = lax.axis_index("py")
    band_index = lax.axis_index("band")
    yblock = points // rows_px
    xblock = points // rows_px
    zblock = points // rows_py
    zshare = zblock // groups
    pieces = groups * rows_py
    kyblock = points // pieces

    density, _ = share_density(orbitals, occupations, stick_map, px_index)
    core = lax.dynamic_slice_in_dim(core_density, band_index * zshare, zshare, 0)
    rho = density + core.transpose(1, 0, 2)

    basis, freq = real_basis(points)
    derive = derivative_matrix(points).astype(np.float32)
    basis32 = basis.astype(np.float32)
    data = jnp.einsum("yzx,xpk->pyzk", rho, basis32.reshape(points, rows_px, xblock), precision=HIGH)
    grad_x = jnp.einsum("yzx,xw->zyw", rho, derive, precision=HIGH)
    data, grad_x_sent = lax.optimization_barrier((data, grad_x.astype(BF)))
    every_x = gathered(grad_x_sent)
    data = lax.all_to_all(data, "px", split_axis=0, concat_axis=0, tiled=True)
    data = data.reshape(points, zshare, xblock)
    high_basis, low_basis = two_halves(basis)
    x_basis = (high_basis.reshape(points, rows_px, xblock), low_basis.reshape(points, rows_px, xblock))
    lines_y = jnp.einsum("yzk,yw->wzk", data, derive, precision=HIGH).astype(BF)
    lines_y = lines_y.reshape(rows_px, yblock, zshare, xblock)
    lines_y = lax.all_to_all(lines_y, "px", split_axis=0, concat_axis=0, tiled=True)
    grad_y = dot2("pyzk,xpk->zyx", lines_y, x_basis)
    grad_y_sent = grad_y.astype(BF)
    modes = jnp.einsum("yzk,yj->jzk", data, basis32, precision=HIGH)
    modes = modes.reshape(pieces, kyblock, zshare, xblock)
    modes = lax.all_to_all(modes, ("band", "py"), split_axis=0, concat_axis=0, tiled=True)
    source = np.arange(points)
    device, within = source // zshare, source % zshare
    z_order = device % rows_py * zblock + device // rows_py * zshare + within
    z_basis = basis32[z_order].reshape(pieces, zshare, points)
    z_derive = derive[z_order][:, z_order].reshape(pieces, zshare, pieces, zshare)
    spectrum = jnp.einsum("djzk,dzm->mjk", modes, z_basis, precision=HIGH)
    unit = 2.0 * math.pi / (points * SPACING)
    all_q = jnp.asarray((freq * freq).astype(np.float32))
    q_col = lax.dynamic_slice_in_dim(all_q, (band_index * rows_py + py_index) * kyblock, kyblock)
    q_row = lax.dynamic_slice_in_dim(all_q, px_index * xblock, xblock)
    squared = unit**2 * (all_q[:, None, None] + q_col[None, :, None] + q_row[None, None, :])
    factor = jnp.where(squared > 0, 4.0 * math.pi / jnp.where(squared > 0, squared, 1.0), 0.0)
    spectrum = spectrum * factor
    back = jnp.stack(
        [
            jnp.einsum("mjk,dzm->djzk", spectrum, z_basis, precision=HIGH).astype(BF),
            jnp.einsum("ejwk,ewdz->djzk", modes, z_derive, precision=HIGH).astype(BF),
        ],
        1,
    )
    back, every_y, every_x = lax.optimization_barrier((back, grad_y_sent, every_x))
    every_y = gathered(every_y)
    back = lax.all_to_all(back, ("band", "py"), split_axis=0, concat_axis=0, tiled=True)
    y_basis = (high_basis.reshape(points, pieces, kyblock), low_basis.reshape(points, pieces, kyblock))
    lines = dot2("dfjzk,ydj->fyzk", back, y_basis)
    lines = lines.astype(BF).reshape(2, rows_px, yblock, zshare, xblock)
    lines = lax.all_to_all(lines, "px", split_axis=1, concat_axis=1, tiled=True)
    fields = dot2("fpyzk,xpk->fzyx", lines, x_basis)
    every_z = gathered(fields[1])
    potential = exchange_part(rho.transpose(1, 0, 2), fields[0], grad_x, grad_y, fields[1])
    every_potential = gathered(potential)
    gradient = jnp.stack([every_x.astype(F32), every_y.astype(F32), every_z.astype(F32)])
    return (every_potential.astype(F32), gradient)


def solution(mesh):
    def step(orbitals, occupations, stick_map, core_density):
        points = orbitals.shape[2] // 2
        block = points // mesh.shape["px"]
        share = points // (mesh.shape["py"] * mesh.shape["band"])
        fits = (
            points == LANES + HALF and block <= HALF and block % 16 == 0 and share % 8 == 0
            and orbitals.shape[:2] == (1, LANES)
            and mesh.shape["py"] == 2 and mesh.shape["band"] == 4 and mesh.shape["px"] == 4
        )
        return (fast_body if fits else body)(orbitals, occupations, stick_map, core_density)

    return jax.shard_map(
        step,
        mesh=mesh,
        in_specs=(P("band", ("px", "py"), None), P("band"), P(None, "px"), P("py", "px", None)),
        out_specs=(P("py", "px", None), P(None, "py", "px", None)),
        check_vma=False,
    )
```

```python
import functools
import math

import jax
import jax.numpy as jnp
import numpy as np
from jax import lax
from jax.experimental import pallas as pl
from jax.experimental.pallas import tpu as pltpu
from jax.experimental.layout import Layout, with_layout_constraint
from jax.sharding import PartitionSpec as P

SPACING = 0.25
PBE_KAPPA = 0.804
PBE_MU = 0.2195
SLATER_COEF = 0.75 * (3.0 / math.pi) ** (1.0 / 3.0)
REDUCED_SCALE = 4.0 * (3.0 * math.pi**2) ** (2.0 / 3.0)
BF = jnp.bfloat16
F32 = jnp.float32
HIGH = lax.Precision.HIGH
CORE_LEAST = 0.05
CORE_TYPICAL = 0.2
PAIRS = 12
COUNT = 24
CHUNKS = 3


def inverse_table(points):
    k = np.arange(points)
    angles = 2.0 * np.pi / points * (k[:, None] * k[None, :] % points)
    cosine, sine = np.cos(angles), np.sin(angles)
    return np.stack([np.stack([cosine, sine], 1), np.stack([-sine, cosine], 1)], 0)


def two_halves(table):
    high = table.astype(np.float32).astype(BF)
    low = (table - high.astype(np.float64)).astype(np.float32).astype(BF)
    return high, low


def dot2(spec, data, table):
    high, low = table
    first = jnp.einsum(spec, data, high, preferred_element_type=F32)
    return first + jnp.einsum(spec, data, low, preferred_element_type=F32)


def real_basis(points):
    pos = np.arange(points)
    freq = np.concatenate([np.arange(points // 2 + 1), np.arange(1, points // 2)])
    angle = 2.0 * np.pi / points * (pos[:, None] * freq[None, :] % points)
    basis = np.where(np.arange(points)[None, :] <= points // 2, np.cos(angle), np.sin(angle))
    scale = np.where((freq == 0) | (freq == points // 2), 1.0 / points, 2.0 / points)
    return basis * np.sqrt(scale), freq


def derivative_matrix(points):
    pos = np.arange(points)
    freq = np.arange(1, points // 2)
    unit = 2.0 * np.pi / (points * SPACING)
    lag = (pos[None, :] - pos[:, None]) % points
    values = np.zeros(points)
    for d in range(points):
        values[d] = np.sum(-2.0 * unit * freq * np.sin(2.0 * np.pi * (freq * d % points) / points)) / points
    return values[lag]


def exchange_part(density, hartree, grad_x, grad_y, grad_z):
    cube_root = jnp.cbrt(density)
    four_thirds = density * cube_root
    grad_square = grad_x * grad_x + grad_y * grad_y + grad_z * grad_z
    reduced = grad_square / (REDUCED_SCALE * four_thirds * four_thirds)
    denominator = 1.0 + PBE_MU * reduced / PBE_KAPPA
    enhance = 1.0 + PBE_KAPPA - PBE_KAPPA / denominator
    enhance_slope = PBE_MU / (denominator * denominator)
    return hartree - SLATER_COEF * cube_root * (
        4.0 / 3.0 * enhance - 8.0 / 3.0 * reduced * enhance_slope
    )


def share_density(orbitals, occupations, stick_map, px_index):
    bands_here, columns_here, doubled = orbitals.shape
    points = doubled // 2
    rows_px = lax.axis_size("px")
    rows_py = lax.axis_size("py")
    groups = lax.axis_size("band")
    xblock = points // rows_px
    yblock = points // rows_px
    pieces = groups * rows_py
    zshare = points // pieces
    sticks = columns_here * rows_py
    bands = groups * bands_here
    inverse = inverse_table(points)
    z_order = inverse.reshape(2, points, 2, rows_py, groups, zshare).transpose(0, 1, 4, 3, 2, 5)
    z_table = two_halves(z_order.reshape(doubled, pieces, 2 * zshare))
    columns = dot2("bsk,kdw->dbsw", orbitals, z_table).astype(BF)
    columns = lax.all_to_all(columns, ("band", "py"), split_axis=0, concat_axis=0, tiled=True)
    columns = lax.all_gather(columns, "px", axis=0, tiled=False)
    columns = columns.reshape(rows_px, groups, rows_py, bands_here, columns_here, 2, zshare)
    columns = columns.transpose(0, 2, 4, 5, 1, 3, 6).reshape(rows_px, sticks, 2, bands * zshare)
    places = lax.all_gather(stick_map, "px", axis=0, tiled=False)
    loads = (orbitals.astype(F32) ** 2).sum((1, 2))
    first = (px_index == 0) & (lax.axis_index("py") == 0)
    own = jnp.where(jnp.arange(groups)[:, None] == lax.axis_index("band"), occupations[None, :], 0.0).reshape(bands)
    totals = jnp.concatenate([jnp.where(first, own, 0.0), (occupations * loads).sum()[None]])
    totals = lax.psum(totals, ("band", "px", "py"))
    weights, mean = totals[:bands], totals[bands]
    y_hot = (places[:, 1, :, None] == jnp.arange(points, dtype=jnp.int32)).astype(BF)
    x_local = places[:, 0] - jnp.arange(rows_px, dtype=jnp.int32)[:, None] * xblock
    x_hot = x_local[:, :, None] == jnp.arange(xblock, dtype=jnp.int32)
    by_y = inverse.reshape(2, points, 2, rows_px, yblock).transpose(3, 1, 0, 4, 2)
    picked = [
        jnp.einsum(
            "psy,yiwo->psiwo",
            y_hot,
            lax.dynamic_index_in_dim(jnp.asarray(half), px_index, 0, keepdims=False),
            preferred_element_type=F32,
        ).astype(BF)
        for half in two_halves(by_y)
    ]
    x_table = two_halves(inverse.reshape(2, rows_px, xblock, 2, points).transpose(1, 0, 2, 3, 4))
    spread = jnp.where(x_hot[:, :, None, :, None], columns[:, :, :, None, :], jnp.zeros((), BF))
    plane = jnp.einsum("psiwo,psixz->pwoxz", picked[0], spread, preferred_element_type=F32)
    plane = plane + jnp.einsum("psiwo,psixz->pwoxz", picked[1], spread, preferred_element_type=F32)
    values = dot2("pwoxz,poxtk->wztk", plane.astype(BF), x_table)
    values = values.reshape(yblock, bands, zshare, 2, points)
    square = values[:, :, :, 0] * values[:, :, :, 0] + values[:, :, :, 1] * values[:, :, :, 1]
    return (weights[None, :, None, None] * square).sum(1), mean


def gathered(field):
    field = with_layout_constraint(field.astype(BF), Layout((0, 1, 2)))
    return lax.all_gather(field, "band", axis=0, tiled=True)


LANES = 128
HALF = 64


def halves_stack(table, axis):
    return jnp.asarray(np.concatenate([np.asarray(h) for h in two_halves(table)], axis))


def packed_lane(parity, mode):
    return np.where(mode < LANES, parity * LANES + mode, 2 * LANES + parity * HALF + mode - LANES)


def chain_tables(points, rows_px, rows_py, groups):
    basis, freq = real_basis(points)
    derive = derivative_matrix(points)
    xblock = points // rows_px
    zshare = points // (rows_py * groups)
    modes = np.arange(points)
    forward = np.zeros((2, points, 3 * LANES + rows_px * LANES))
    spread = np.zeros((rows_px, LANES, 3 * LANES))
    for parity in range(2):
        forward[parity][:, packed_lane(parity, modes)] = basis
        lane = modes // xblock * LANES + parity * HALF + modes % xblock
        forward[parity][:, 3 * LANES + lane] = basis
        spread[modes // xblock, parity * HALF + modes % xblock, packed_lane(parity, modes)] = 1.0
    source = np.arange(points // 2)
    device, within = source // (zshare // 2), source % (zshare // 2)
    even = device % rows_py * (points // rows_py) + device // rows_py * zshare + 2 * within
    to_modes = np.concatenate([basis[even].T, basis[even + 1].T], 0)
    from_modes = np.concatenate([basis[even], basis[even + 1]], 0)
    return dict(
        forward=jnp.stack([jnp.asarray(h) for h in two_halves(forward)]),
        y_in=halves_stack(basis.T, 0),
        y_out=halves_stack(basis, 0),
        y_slope=halves_stack(derive.T, 0),
        z_in=halves_stack(to_modes, 1),
        z_out=halves_stack(from_modes, 0),
        spread=jnp.asarray(spread.astype(np.float32).astype(BF)),
    )


def slope_tables(points, rows_py, groups):
    derive = derivative_matrix(points)
    pairs = np.arange(points // 2)
    zblock = points // rows_py
    own = []
    for py in range(rows_py):
        order = np.concatenate([np.arange(zblock) + q * zblock for q in [py] + [q for q in range(rows_py) if q != py]])
        mine = np.arange(zblock) + py * zblock
        parts = []
        for out_parity in range(2):
            for in_parity in range(2):
                parts.append(derive[np.ix_(order[in_parity::2], mine[out_parity::2])].T)
        own.append(np.concatenate(parts, 0))
    stacked = np.stack(own)
    return np.concatenate([np.asarray(h) for h in two_halves(stacked)], 2)


def final_tables(points):
    basis, _ = real_basis(points)
    derive = derivative_matrix(points)
    out = np.zeros((2, 2 * LANES, 2, 2 * LANES))
    for parity in range(2):
        modes = np.arange(points)
        row = np.where(modes < LANES, modes, parity * HALF + modes)
        out[parity, row, 0, :points] = basis.T
        out[parity, row, 1, :points] = basis.T @ derive
    high, low = two_halves(out)
    both = np.stack([np.asarray(high), np.asarray(low)], 0)
    return jnp.asarray(both.transpose(1, 3, 0, 2, 4))


def dotf(left, right):
    return jnp.dot(left, right, preferred_element_type=F32)


def split(value):
    high = value.astype(BF)
    return high, (value - high.astype(F32)).astype(BF)


def chain_kernel(
    dims, summed, rho, forward, y_in, y_out, y_slope, z_in, z_out, spread, slope,
    xs, gy, gz, h,
    others, c1s, c1, c2s, c2, c3s, c3, c4s, c4, gin, gs, wide, deep, sends, recvs, g_sends, g_recvs, b_sends, b_recvs,
    o_sends, o_recvs, x_sends, x_recvs, h_sends, h_recvs,
):
    points, rows_px, rows_py, groups = dims
    yblock = points // rows_px
    zpairs = points // (rows_py * groups) // 2
    pieces = groups * rows_py
    kyblock = points // pieces
    rows = zpairs * yblock
    short = zpairs * kyblock
    band, px, py = lax.axis_index("band"), lax.axis_index("px"), lax.axis_index("py")
    me = band * rows_py + py
    px_peers = [lax.rem(px + s, rows_px) for s in range(1, rows_px)]
    zy_peers = [
        (lax.rem(band + b, groups), lax.rem(py + q, rows_py))
        for b in range(groups) for q in range(rows_py) if b or q
    ]
    used = []

    def send(src, dst, device):
        copy = pltpu.make_async_remote_copy(
            src_ref=src, dst_ref=dst, send_sem=sends.at[len(used)], recv_sem=recvs.at[len(used)],
            device_id=device, device_id_type=pl.DeviceIdType.MESH,
        )
        used.append(copy)
        copy.start()
        return copy

    def to_px(src, dst, cut):
        dst[px, cut] = src[px, cut]
        return [send(src.at[peer, cut], dst.at[px, cut], (band, peer, py)) for peer in px_peers]

    def to_zy(src, dst, cut):
        dst[me, cut] = src[me, cut]
        return [send(src.at[b * rows_py + q, cut], dst.at[me, cut], (b, px, q)) for b, q in zy_peers]

    def arrived(copies):
        for copy in copies:
            copy.wait_recv()

    def hop(field, out_sems, in_sems, sign, phase, c):
        slot = jnp.clip(band - sign * phase, 0, groups - 1)
        target = jnp.clip(band + sign, 0, groups - 1)
        return pltpu.make_async_remote_copy(
            src_ref=field.at[slot, lined[c]], dst_ref=field.at[slot, lined[c]],
            send_sem=out_sems.at[phase * 2 + (sign > 0), c], recv_sem=in_sems.at[slot, c],
            device_id=(target, px, py), device_id_type=pl.DeviceIdType.MESH,
        )

    def hops(phase):
        return [
            (1, (band >= phase) & (band < groups - 1)),
            (-1, (band + phase < groups) & (band > 0)),
        ]

    def launch(fields, phase, c):
        for sign, runs in hops(phase):
            pl.when(runs)(hop(*fields, sign, phase, c).start)

    def landed(fields, distance, c):
        for sign in (1, -1):
            slot = band - sign * distance

            @pl.when((slot >= 0) & (slot < groups))
            def _():
                pltpu.make_async_remote_copy(
                    src_ref=fields[0].at[0, lined[c]], dst_ref=fields[0].at[jnp.clip(slot, 0, groups - 1), lined[c]],
                    send_sem=fields[1].at[0, c], recv_sem=fields[2].at[jnp.clip(slot, 0, groups - 1), c],
                    device_id=(band, px, py), device_id_type=pl.DeviceIdType.MESH,
                ).wait_recv()

    def to_other(slot):
        return pltpu.make_async_remote_copy(
            src_ref=xs.at[slot], dst_ref=others.at[slot], send_sem=o_sends.at[slot], recv_sem=o_recvs.at[slot],
            device_id=(band, px, lax.rem(py + 1, rows_py)), device_id_type=pl.DeviceIdType.MESH,
        )

    x_line = (xs, x_sends, x_recvs)
    h_line = (h, h_sends, h_recvs)
    step = zpairs // CHUNKS
    lined = [pl.ds(c * step * yblock, step * yblock) for c in range(CHUNKS)]
    short_cuts = [pl.ds(c * step * kyblock, step * kyblock) for c in range(CHUNKS)]
    first, second, third, fourth = [], [], [], []

    def to_modes_x(c):
        summed(c * step, (c + 1) * step)
        at = lined[c]
        out = None
        for parity in range(2):
            high, low = split(rho[parity, at, :])
            part = dotf(high, forward[0, parity]) + dotf(low, forward[0, parity]) + dotf(high, forward[1, parity])
            out = part if out is None else out + part
        xs[band, at, :] = out[:, : 3 * LANES].astype(BF)
        for p in range(rows_px):
            c1s[p, at, :] = out[:, (3 + p) * LANES : (4 + p) * LANES].astype(BF)
        first.append(to_px(c1s, c1, at))
        launch(x_line, 0, c)

    def to_modes_y(c):
        arrived(first[c])

        @pl.loop(c * step // 2, (c + 1) * step // 2)
        def _(i):
            found = []
            for k in range(2):
                at = pl.ds(pl.multiple_of((2 * i + k) * yblock, yblock), yblock)
                out = dotf(y_in[...], jnp.concatenate([c1[p, at, :] for p in range(rows_px)], 0))
                found.append(out[:points] + out[points:])
            at = pl.ds(pl.multiple_of(i * 2 * kyblock, 2 * kyblock), 2 * kyblock)
            for d in range(pieces):
                cut = slice(d * kyblock, (d + 1) * kyblock)
                c2s[d, at, :] = jnp.concatenate([f[cut] for f in found], 0).astype(BF)

        second.append(to_zy(c2s, c2, short_cuts[c]))

    for c in range(CHUNKS):
        to_modes_x(c)
        if c:
            to_modes_y(c - 1)
    to_modes_y(CHUNKS - 1)

    def outward(slot, source, c):
        return pltpu.make_async_remote_copy(
            src_ref=xs.at[slot, lined[c]], dst_ref=gin.at[source, lined[c]],
            send_sem=g_sends.at[slot, c], recv_sem=g_recvs.at[source, c],
            device_id=(band, slot, py), device_id_type=pl.DeviceIdType.MESH,
        )

    def pass_on(slot, c):
        pl.when(px != slot)(lambda: outward(slot, px, c).start())

        @pl.when(px == slot)
        def _():
            gin[px, lined[c]] = xs[slot, lined[c]]

    def at_distance(distance, act):
        for sign in (1, -1):
            slot = band - sign * distance
            pl.when((slot >= 0) & (slot < groups))(lambda: act(jnp.clip(slot, 0, groups - 1)))

    def cross_over(slot):
        to_other(slot).start()

    def homeward(k, peer, owner, c):
        return pltpu.make_async_remote_copy(
            src_ref=gs.at[peer, lined[c]], dst_ref=gy.at[owner, lined[c]],
            send_sem=b_sends.at[k, c], recv_sem=b_recvs.at[owner, c],
            device_id=(band, peer, py), device_id_type=pl.DeviceIdType.MESH,
        )

    def slopes_along_y():
        for c in range(CHUNKS):
            for peer in px_peers:
                outward(0, peer, c).wait_recv()

            @pl.loop(c * step, (c + 1) * step)
            def _(i):
                at = pl.ds(pl.multiple_of(i * yblock, yblock), yblock)
                out = dotf(y_slope[...], jnp.concatenate([gin[p, at, :] for p in range(rows_px)], 0))
                out = out[:points] + out[points:]
                for p in range(rows_px):
                    gs[p, at, :] = out[p * yblock : (p + 1) * yblock].astype(BF)

            for k, peer in enumerate(px_peers):
                homeward(k, peer, px, c).start()
            gy[px, lined[c]] = gs[px, lined[c]]

    near = (px - band <= 1) & (band - px <= 1)
    for c in range(CHUNKS):
        pass_on(band, c)
    for c in range(CHUNKS):
        landed(x_line, 1, c)
        launch(x_line, 1, c)
        at_distance(1, functools.partial(pass_on, c=c))
    for copies in second:
        arrived(copies)
    for d in range(pieces):
        wide[pl.ds(d * short, short), :] = c2[d].astype(F32)
    lane = lax.broadcasted_iota(jnp.int32, (points, 2 * LANES), 1) % LANES
    column = pieces * zpairs
    unit = 2.0 * math.pi / (points * SPACING)

    def frequency(index):
        return jnp.where(index > points // 2, index - points // 2, index)

    level = frequency(lax.broadcasted_iota(jnp.int32, (points, 2 * LANES), 0))
    across_x = frequency(lane + px * yblock)
    flat = (level * level + across_x * across_x).astype(F32)
    second_half = lax.broadcasted_iota(jnp.int32, (points, 2 * LANES), 1) >= LANES

    def swapped(value):
        return jnp.concatenate([pltpu.roll(value[:, k * LANES : (k + 1) * LANES], HALF, 1) for k in range(2)], 1)

    @pl.loop(0, kyblock // 2)
    def _(i):
        at = [pl.ds(2 * i + k, column, stride=kyblock) for k in range(2)]
        data = jnp.concatenate([wide[a, :] for a in at], 1).astype(BF)
        out = dotf(z_in[...], jnp.concatenate([data, data], 0))
        here = [frequency(me * kyblock + 2 * i + k) for k in range(2)]
        here = [(f * f).astype(F32) for f in here]
        squared = unit**2 * (flat + jnp.where(second_half, here[1], here[0]))
        factor = jnp.where(squared > 0, 4.0 * math.pi / jnp.where(squared > 0, squared, 1.0), 0.0)
        spectrum = (out[:points] + swapped(out[points:])) * factor
        spectrum = jnp.where(lane < HALF, spectrum, swapped(spectrum))
        high, low = split(spectrum)
        back = dotf(z_out[:points, :], high) + dotf(z_out[points:, :], high) + dotf(z_out[:points, :], low)
        back = jnp.where(lane[:column] < HALF, back[:column], back[column:])
        for k in range(2):
            wide[at[k], :] = back[:, k * LANES : (k + 1) * LANES]

    for d in range(pieces):
        c3s[d] = wide[pl.ds(d * short, short), :].astype(BF)
    for c in range(CHUNKS):
        landed(x_line, 2, c)
        launch(x_line, 2, c)
        at_distance(2, functools.partial(pass_on, c=c))
    for c in range(CHUNKS):
        third.append(to_zy(c3s, c3, short_cuts[c]))
    cross_over(band)
    at_distance(1, cross_over)
    at_distance(2, cross_over)
    pl.when(near)(slopes_along_y)

    def from_modes_y(c):
        arrived(third[c])
        for d in range(pieces):
            wide[pl.ds(d * short + c * step * kyblock, step * kyblock), :] = c3[d, short_cuts[c], :].astype(F32)

        @pl.loop(c * step, (c + 1) * step)
        def _(i):
            data = jnp.concatenate(
                [wide[pl.ds(pl.multiple_of(d * short + i * kyblock, 8), kyblock), :] for d in range(pieces)], 0
            ).astype(BF)
            out = dotf(y_out[...], data)
            out = out[:points] + out[points:]
            at = pl.ds(pl.multiple_of(i * yblock, yblock), yblock)
            for p in range(rows_px):
                c4s[p, at, :] = out[p * yblock : (p + 1) * yblock].astype(BF)

        fourth.append(to_px(c4s, c4, lined[c]))

    def gathered_modes(c):
        arrived(fourth[c])
        at = lined[c]
        out = None
        for p in range(rows_px):
            part = dotf(c4[p, at, :], spread[p])
            out = part if out is None else out + part
        h[band, at, :] = out.astype(BF)
        launch(h_line, 0, c)

    for c in range(CHUNKS):
        from_modes_y(c)
        if c:
            gathered_modes(c - 1)
    gathered_modes(CHUNKS - 1)
    for c in range(CHUNKS):
        landed(h_line, 1, c)
        launch(h_line, 1, c)
    for c in range(CHUNKS):
        landed(x_line, 3, c)
        at_distance(3, functools.partial(pass_on, c=c))
    at_distance(3, cross_over)
    pl.when(jnp.logical_not(near))(slopes_along_y)
    for c in range(CHUNKS):
        landed(h_line, 2, c)
        launch(h_line, 2, c)
    for slot in range(groups):
        to_other(slot).wait_recv()
    own_rows = groups * rows
    for b in range(groups):
        for t in range(3):
            cut = pl.ds(t * LANES, LANES)
            deep[t, pl.ds(b * rows, rows), :] = xs[b, :, cut].astype(F32)
            deep[t, pl.ds(own_rows + b * rows, rows), :] = others[b, :, cut].astype(F32)
    zlines = groups * zpairs
    tail = lax.broadcasted_iota(jnp.int32, (zlines, LANES), 1) < HALF

    @pl.loop(0, yblock // 2)
    def _(i):
        data = jnp.concatenate(
            [
                deep[t, pl.ds(2 * i + k, rows_py * zlines, stride=yblock), :]
                for k in range(2) for t in range(3)
            ],
            1,
        ).astype(BF)
        out = dotf(slope[py], jnp.concatenate([data, data], 0))
        parts = [out[q * zlines : (q + 1) * zlines] for q in range(4)]
        for k in range(2):
            first, middle, last = (slice((3 * k + t) * LANES, (3 * k + t + 1) * LANES) for t in range(3))
            at = pl.ds(2 * i + k, zlines, stride=yblock)
            even = parts[0][:, last] + pltpu.roll(parts[1][:, last], HALF, 1)
            odd = pltpu.roll(parts[2][:, last], HALF, 1) + parts[3][:, last]
            deep[0, at, :] = parts[0][:, first] + parts[1][:, middle]
            deep[1, at, :] = parts[2][:, first] + parts[3][:, middle]
            deep[2, at, :] = jnp.where(tail, even, odd)

    for b in range(groups):
        for t in range(3):
            gz[b, :, pl.ds(t * LANES, LANES)] = deep[t, pl.ds(b * rows, rows), :].astype(BF)
    for c in range(CHUNKS):
        landed(h_line, 3, c)
    for k, peer in enumerate(px_peers):
        for c in range(CHUNKS):
            homeward(k, px, peer, c).wait_recv()
            homeward(k, peer, px, c).wait_send()
    for slot in range(groups):
        to_other(slot).wait_send()
        for c in range(CHUNKS):
            pl.when(px != slot)(outward(slot, px, c).wait_send)
    for line in (x_line, h_line):
        for phase in range(groups - 1):
            for sign, runs in hops(phase):
                for c in range(CHUNKS):
                    pl.when(runs)(hop(*line, sign, phase, c).wait_send)
    for copy in used:
        copy.wait_send()


def final_kernel(dims, shift, xs, gy, gz, h, table, potential, gradient):
    points, yblock, pairs = dims
    for parity in range(2):
        first = slice(parity * LANES, (parity + 1) * LANES)

        def natural(ref):
            value = ref[...]
            return jnp.concatenate([value[:, first], value[:, 2 * LANES :]], 1)

        def spatial(value, kind):
            out = dotf(value, table[parity, kind, 0]) + dotf(value, table[parity, kind, 1])
            return out[:, :points]

        lines = natural(xs)
        out = spatial(jnp.concatenate([lines, natural(gy), natural(gz), natural(h)], 0), 0)
        grad_x = spatial(lines, 1)
        n = pairs * yblock
        density, grad_y, grad_z, hartree = (out[k * n : (k + 1) * n] for k in range(4))
        density = jnp.maximum(density + shift[0:1, 0:1], CORE_LEAST)
        cube_root = jnp.exp(jnp.log(density) * (1.0 / 3.0))
        power = density * cube_root
        power = power * power
        grad_square = grad_x * grad_x + grad_y * grad_y + grad_z * grad_z
        ratio = power / (power + (PBE_MU / (PBE_KAPPA * REDUCED_SCALE)) * grad_square)
        part = 4.0 / 3.0 * (1.0 + PBE_KAPPA) - PBE_KAPPA * ratio * (4.0 - 8.0 / 3.0 * ratio)
        value = hartree - SLATER_COEF * cube_root * part
        for k in range(pairs):
            cut = slice(k * yblock, (k + 1) * yblock)
            potential[2 * k + parity] = value[cut]
            gradient[0, 2 * k + parity] = grad_x[cut]
            gradient[1, 2 * k + parity] = grad_y[cut]
            gradient[2, 2 * k + parity] = grad_z[cut]


def run_final(xs, gy, gz, h, shift, points, yblock):
    groups, rows, _ = xs.shape
    pairs = PAIRS
    steps = groups * rows // (pairs * yblock)
    zblock = steps * 2 * pairs
    table = final_tables(points)
    flat = pl.BlockSpec((pairs * yblock, 3 * LANES), lambda i: (i, 0))
    return pl.pallas_call(
        functools.partial(final_kernel, (points, yblock, pairs)),
        grid=(steps,),
        out_shape=[
            jax.ShapeDtypeStruct((zblock, yblock, points), F32),
            jax.ShapeDtypeStruct((3, zblock, yblock, points), F32),
        ],
        in_specs=[pl.BlockSpec((8, LANES), lambda i: (0, 0))]
        + [flat] * 4
        + [pl.BlockSpec(table.shape, lambda i: (0, 0, 0, 0, 0))],
        out_specs=[
            pl.BlockSpec((2 * pairs, yblock, points), lambda i: (i, 0, 0)),
            pl.BlockSpec((3, 2 * pairs, yblock, points), lambda i: (0, i, 0, 0)),
        ],
    )(shift, *[f.reshape(groups * rows, 3 * LANES) for f in (xs, gy, gz, h)], table)


def column_tables(points, rows_px, rows_py, groups):
    inverse = inverse_table(points)
    pieces = groups * rows_py
    zshare = points // pieces
    yblock = points // rows_px
    doubled = 2 * points
    z_order = inverse.reshape(2, points, 2, rows_py, groups, zshare).transpose(0, 1, 4, 3, 2, 5)
    by_y = np.zeros((rows_px, 2, points, 2, HALF))
    by_y[:, :, :, :, :yblock] = inverse.reshape(2, points, 2, rows_px, yblock).transpose(3, 0, 1, 2, 4)
    by_y = np.concatenate([np.asarray(h) for h in two_halves(by_y.reshape(rows_px, 2, points, LANES))], 3)
    by_x = np.concatenate([np.asarray(h) for h in two_halves(inverse[0].transpose(1, 2, 0).reshape(doubled, points))], 0)
    z_table = np.stack([np.asarray(h) for h in two_halves(z_order.reshape(doubled, doubled).T)])
    return jnp.asarray(z_table), jnp.asarray(by_y), jnp.asarray(by_x)


def column_kernel(
    dims, occupation, orbitals, z_table, places, sticks, every_place, notes, columns, note, middle, sends, recvs
):
    points, rows_px, rows_py, groups = dims
    band, px, py = lax.axis_index("band"), lax.axis_index("px"), lax.axis_index("py")
    me = band * rows_py + py
    px_peers = [(band, lax.rem(px + s, rows_px), py) for s in range(1, rows_px)]
    zy_peers = [
        (lax.rem(band + b, groups), px, lax.rem(py + q, rows_py))
        for b in range(groups) for q in range(rows_py) if b or q
    ]
    barrier = pltpu.get_barrier_semaphore()
    for peer in px_peers + zy_peers:
        pl.semaphore_signal(barrier, inc=1, device_id=peer, device_id_type=pl.DeviceIdType.MESH)
    coefficients = orbitals[0]
    contract = (((1,), (1,)), ((), ()))
    found = lax.dot_general(z_table[0], coefficients, contract, preferred_element_type=F32)
    found = found + lax.dot_general(z_table[1], coefficients, contract, preferred_element_type=F32)
    share = 2 * points // (groups * rows_py)
    for d in range(groups * rows_py):
        columns[d] = found[d * share : (d + 1) * share].astype(BF)
    wide = coefficients.astype(F32)
    load = occupation[0] * jnp.sum(wide * wide)
    lane = lax.broadcasted_iota(jnp.int32, (8, LANES), 1)
    note[...] = jnp.where(lane == 0, occupation[0], jnp.where(lane == 1, load, 0.0))
    pl.semaphore_wait(barrier, len(px_peers) + len(zy_peers))
    used = []

    def send(src, dst, device):
        copy = pltpu.make_async_remote_copy(
            src_ref=src, dst_ref=dst, send_sem=sends.at[len(used)], recv_sem=recvs.at[len(used)],
            device_id=device, device_id_type=pl.DeviceIdType.MESH,
        )
        used.append(copy)
        copy.start()

    for peer in zy_peers:
        send(columns.at[peer[0] * rows_py + peer[2]], middle.at[me], peer)
    for peer in zy_peers:
        send(note, notes.at[px, me], peer)
    first = len(used)
    for peer in px_peers:
        send(places, every_place.at[px], peer)
    middle[me] = columns[me]
    notes[px, me] = note[...]
    every_place[px] = places[...]
    for copy in used[:first]:
        copy.wait_recv()
    for peer in px_peers:
        send(middle, sticks.at[px], peer)
        send(notes.at[px], notes.at[px], peer)
    sticks[px] = middle[...]

    def settled():
        for copy in used[first:]:
            copy.wait_recv()

    def sent():
        for copy in used:
            copy.wait_send()

    return settled, sent


def density_kernel(dims, settled, notes, sticks, places, by_y, by_x, core, rho, shift, wide, planes, held, sem):
    points, rows_px, rows_py, groups = dims
    xblock = yblock = points // rows_px
    zshare = points // (rows_py * groups)
    band, px = lax.axis_index("band"), lax.axis_index("px")
    fetch = pltpu.make_async_copy(core.at[pl.ds(band * zshare, zshare)], held, sem)
    fetch.start()
    count = COUNT
    lines = groups * zshare
    sticks_px = rows_py * LANES

    def spread_along_y(p):
        wide[...] = sticks[p].astype(F32)
        spots = places[p]
        at_y = lax.broadcasted_iota(jnp.int32, (points, sticks_px), 0) == spots[1:2, :]
        one_hot = at_y.astype(F32).astype(BF)
        table = jnp.concatenate(
            [
                lax.dot_general(one_hot, by_y[px, i], (((0,), (0,)), ((), ())), preferred_element_type=F32)
                for i in range(2)
            ],
            0,
        ).astype(BF)
        at_x = lax.broadcasted_iota(jnp.int32, (xblock, sticks_px), 0) == spots[0:1, :] - p * xblock
        mask = at_x.astype(F32)

        @pl.loop(0, lines // count)
        def _(c):
            b = c // (zshare // count)
            z = (c % (zshare // count)) * count
            blocks = []
            for k in range(count):
                tiles = [
                    mask[:, q * LANES : (q + 1) * LANES]
                    * wide[b * rows_py + q, pl.ds(i * zshare + z + k, 1), :]
                    for i in range(2) for q in range(rows_py)
                ]
                blocks.append(jnp.concatenate(tiles, 1))
            out = dotf(jnp.concatenate(blocks, 0).astype(BF), table)
            out = (out[:, :LANES] + out[:, LANES:]).astype(BF)
            for k in range(count):
                planes[c * count + k, pl.ds(pl.multiple_of(p * xblock, xblock), xblock), :] = out[
                    k * xblock : (k + 1) * xblock
                ]

    spread_along_y(px)
    settled()

    @pl.loop(1, rows_px)
    def _(s):
        spread_along_y(lax.rem(px + s, rows_px))

    mean = CORE_TYPICAL
    for p in range(rows_px):
        for d in range(groups * rows_py):
            mean = mean + notes[p, d, :, 1:2]
    shift[...] = jnp.broadcast_to(mean, (8, LANES))
    mean = mean[0:1]
    weights = [notes[0, b * rows_py, 0:1, 0:1] for b in range(groups)]
    fetch.wait()
    lane = lax.broadcasted_iota(jnp.int32, (points, LANES), 1)
    sign = jnp.where(lane < HALF, -1.0, 1.0)

    def summed(start, stop):
        @pl.loop(start, stop)
        def _(i):
            total = [None, None]
            for b in range(groups):
                both = jnp.concatenate([planes[b * zshare + 2 * i + k] for k in range(2)], 1)
                out = dotf(by_x[...], both)
                out = out[: 2 * points] + out[2 * points :]
                cosine, sine = out[:points], out[points:]
                for k in range(2):
                    cut = slice(k * LANES, (k + 1) * LANES)
                    value = cosine[:, cut] + sign * pltpu.roll(sine[:, cut], HALF, 1)
                    value = weights[b] * (value * value)
                    total[k] = value if b == 0 else total[k] + value
            for k in range(2):
                density = total[k] + pltpu.roll(total[k], HALF, 1)
                rho[k, pl.ds(pl.multiple_of(i * yblock, yblock), yblock), :] = (
                    density.T[:yblock] + (held[2 * i + k] - mean)
                )

    return summed


COLUMN_INPUTS, DENSITY_INPUTS, CHAIN_INPUTS = 4, 3, 8


def whole_kernel(dims, counts, *refs):
    groups = [COLUMN_INPUTS, DENSITY_INPUTS, CHAIN_INPUTS, 5] + counts
    parts, at = [], 0
    for count in groups:
        parts.append(refs[at : at + count])
        at += count
    column_in, density_in, chain_in, out, shared, column_own, density_own, chain_own = parts
    sticks, places, notes, rho = shared
    fields, shift = out[:4], out[4]
    settled, sent = column_kernel(dims, *column_in, sticks, places, notes, *column_own)
    summed = density_kernel(dims, settled, notes, sticks, places, *density_in, rho, shift, *density_own)
    chain_kernel(dims, summed, rho, *chain_in, *fields, *chain_own)
    sent()


def run_whole(occupations, orbitals, stick_map, core, dims):
    points, rows_px, rows_py, groups = dims
    xblock = yblock = points // rows_px
    pieces = groups * rows_py
    kyblock = zshare = points // pieces
    zpairs = zshare // 2
    rows, short = zpairs * yblock, zpairs * kyblock
    z_table, by_y, by_x = column_tables(points, rows_px, rows_py, groups)
    tables = chain_tables(points, rows_px, rows_py, groups)
    names = ("forward", "y_in", "y_out", "y_slope", "z_in", "z_out", "spread")
    slope = jnp.asarray(slope_tables(points, rows_py, groups))
    share = (pieces, 2 * zshare, LANES)
    field = jax.ShapeDtypeStruct((groups, rows, 3 * LANES), BF)
    vmem = pl.BlockSpec(memory_space=pltpu.VMEM)
    lined = pltpu.VMEM((rows_px, rows, LANES), BF)
    cut = pltpu.VMEM((pieces, short, LANES), BF)
    dma = pltpu.SemaphoreType.DMA
    column_copies = 2 * (pieces - 1) + 3 * (rows_px - 1)
    chain_copies = CHUNKS * (2 * (rows_px - 1) + 2 * (pieces - 1))
    shared = [
        pltpu.VMEM((rows_px,) + share, BF),
        pltpu.VMEM((rows_px,) + stick_map.shape, jnp.int32),
        pltpu.VMEM((rows_px, pieces, 8, LANES), F32),
        pltpu.VMEM((2, rows, points), F32),
    ]
    column_own = [
        pltpu.VMEM(share, BF),
        pltpu.VMEM((8, LANES), F32),
        pltpu.VMEM(share, BF),
        dma((column_copies,)),
        dma((column_copies,)),
    ]
    density_own = [
        pltpu.VMEM(share, F32),
        pltpu.VMEM((groups * zshare, points, LANES), BF),
        pltpu.VMEM((zshare, yblock, points), F32),
        dma,
    ]
    chain_own = [
        pltpu.VMEM((groups, rows, 3 * LANES), BF),
        lined, lined, cut, cut, cut, cut, lined, lined,
        pltpu.VMEM((rows_px, rows, 3 * LANES), BF),
        pltpu.VMEM((rows_px, rows, 3 * LANES), BF),
        pltpu.VMEM((pieces * short, LANES), F32),
        pltpu.VMEM((3, rows_py * groups * rows, LANES), F32),
        dma((chain_copies,)),
        dma((chain_copies,)),
        dma((rows_px, CHUNKS)),
        dma((rows_px, CHUNKS)),
        dma((rows_px - 1, CHUNKS)),
        dma((rows_px, CHUNKS)),
        dma((groups,)),
        dma((groups,)),
    ] + [dma((2 * (groups - 1), CHUNKS)), dma((groups, CHUNKS))] * 2
    counts = [len(part) for part in (shared, column_own, density_own, chain_own)]
    return pl.pallas_call(
        functools.partial(whole_kernel, dims, counts),
        out_shape=[field] * 4 + [jax.ShapeDtypeStruct((8, LANES), F32)],
        in_specs=[pl.BlockSpec(memory_space=pltpu.SMEM)]
        + [vmem] * 5
        + [pl.BlockSpec(memory_space=pl.ANY)]
        + [vmem] * 8,
        out_specs=[vmem] * 5,
        scratch_shapes=shared + column_own + density_own + chain_own,
        compiler_params=pltpu.CompilerParams(collective_id=1, has_side_effects=True, vmem_limit_bytes=60 << 20),
    )(occupations, orbitals, z_table, stick_map, by_y, by_x, core, *[tables[n] for n in names], slope)


def fast_body(orbitals, occupations, stick_map, core_density):
    points = orbitals.shape[2] // 2
    rows_px, rows_py, groups = lax.axis_size("px"), lax.axis_size("py"), lax.axis_size("band")
    dims = (points, rows_px, rows_py, groups)
    yblock = points // rows_px
    xs, gy, gz, h, shift = run_whole(occupations, orbitals, stick_map, core_density, dims)
    return tuple(run_final(xs, gy, gz, h, shift, points, yblock))


def body(orbitals, occupations, stick_map, core_density):
    points = orbitals.shape[2] // 2
    rows_px = lax.axis_size("px")
    rows_py = lax.axis_size("py")
    groups = lax.axis_size("band")
    px_index = lax.axis_index("px")
    py_index = lax.axis_index("py")
    band_index = lax.axis_index("band")
    yblock = points // rows_px
    xblock = points // rows_px
    zblock = points // rows_py
    zshare = zblock // groups
    pieces = groups * rows_py
    kyblock = points // pieces

    density, _ = share_density(orbitals, occupations, stick_map, px_index)
    core = lax.dynamic_slice_in_dim(core_density, band_index * zshare, zshare, 0)
    rho = density + core.transpose(1, 0, 2)

    basis, freq = real_basis(points)
    derive = derivative_matrix(points).astype(np.float32)
    basis32 = basis.astype(np.float32)
    data = jnp.einsum("yzx,xpk->pyzk", rho, basis32.reshape(points, rows_px, xblock), precision=HIGH)
    grad_x = jnp.einsum("yzx,xw->zyw", rho, derive, precision=HIGH)
    data, grad_x_sent = lax.optimization_barrier((data, grad_x.astype(BF)))
    every_x = gathered(grad_x_sent)
    data = lax.all_to_all(data, "px", split_axis=0, concat_axis=0, tiled=True)
    data = data.reshape(points, zshare, xblock)
    high_basis, low_basis = two_halves(basis)
    x_basis = (high_basis.reshape(points, rows_px, xblock), low_basis.reshape(points, rows_px, xblock))
    lines_y = jnp.einsum("yzk,yw->wzk", data, derive, precision=HIGH).astype(BF)
    lines_y = lines_y.reshape(rows_px, yblock, zshare, xblock)
    lines_y = lax.all_to_all(lines_y, "px", split_axis=0, concat_axis=0, tiled=True)
    grad_y = dot2("pyzk,xpk->zyx", lines_y, x_basis)
    grad_y_sent = grad_y.astype(BF)
    modes = jnp.einsum("yzk,yj->jzk", data, basis32, precision=HIGH)
    modes = modes.reshape(pieces, kyblock, zshare, xblock)
    modes = lax.all_to_all(modes, ("band", "py"), split_axis=0, concat_axis=0, tiled=True)
    source = np.arange(points)
    device, within = source // zshare, source % zshare
    z_order = device % rows_py * zblock + device // rows_py * zshare + within
    z_basis = basis32[z_order].reshape(pieces, zshare, points)
    z_derive = derive[z_order][:, z_order].reshape(pieces, zshare, pieces, zshare)
    spectrum = jnp.einsum("djzk,dzm->mjk", modes, z_basis, precision=HIGH)
    unit = 2.0 * math.pi / (points * SPACING)
    all_q = jnp.asarray((freq * freq).astype(np.float32))
    q_col = lax.dynamic_slice_in_dim(all_q, (band_index * rows_py + py_index) * kyblock, kyblock)
    q_row = lax.dynamic_slice_in_dim(all_q, px_index * xblock, xblock)
    squared = unit**2 * (all_q[:, None, None] + q_col[None, :, None] + q_row[None, None, :])
    factor = jnp.where(squared > 0, 4.0 * math.pi / jnp.where(squared > 0, squared, 1.0), 0.0)
    spectrum = spectrum * factor
    back = jnp.stack(
        [
            jnp.einsum("mjk,dzm->djzk", spectrum, z_basis, precision=HIGH).astype(BF),
            jnp.einsum("ejwk,ewdz->djzk", modes, z_derive, precision=HIGH).astype(BF),
        ],
        1,
    )
    back, every_y, every_x = lax.optimization_barrier((back, grad_y_sent, every_x))
    every_y = gathered(every_y)
    back = lax.all_to_all(back, ("band", "py"), split_axis=0, concat_axis=0, tiled=True)
    y_basis = (high_basis.reshape(points, pieces, kyblock), low_basis.reshape(points, pieces, kyblock))
    lines = dot2("dfjzk,ydj->fyzk", back, y_basis)
    lines = lines.astype(BF).reshape(2, rows_px, yblock, zshare, xblock)
    lines = lax.all_to_all(lines, "px", split_axis=1, concat_axis=1, tiled=True)
    fields = dot2("fpyzk,xpk->fzyx", lines, x_basis)
    every_z = gathered(fields[1])
    potential = exchange_part(rho.transpose(1, 0, 2), fields[0], grad_x, grad_y, fields[1])
    every_potential = gathered(potential)
    gradient = jnp.stack([every_x.astype(F32), every_y.astype(F32), every_z.astype(F32)])
    return (every_potential.astype(F32), gradient)


def solution(mesh):
    def step(orbitals, occupations, stick_map, core_density):
        points = orbitals.shape[2] // 2
        block = points // mesh.shape["px"]
        share = points // (mesh.shape["py"] * mesh.shape["band"])
        fits = (
            points == LANES + HALF and block <= HALF and block % 16 == 0 and share % 8 == 0
            and orbitals.shape[:2] == (1, LANES)
            and mesh.shape["py"] == 2 and mesh.shape["band"] == 4 and mesh.shape["px"] == 4
        )
        return (fast_body if fits else body)(orbitals, occupations, stick_map, core_density)

    return jax.shard_map(
        step,
        mesh=mesh,
        in_specs=(P("band", ("px", "py"), None), P("band"), P(None, "px"), P("py", "px", None)),
        out_specs=(P("py", "px", None), P(None, "py", "px", None)),
        check_vma=False,
    )
```
